8 devices in a mesh: dp: 2 (over z, y), sp: 4 (over x, core).
Axes of the slice: x: 2, y: 2, z: 1, core: 2. Of those that a mesh axis runs over, the one named last changes fastest.
Arguments:
- hidden: bfloat16 [8192, 1536], P(('dp', 'sp')), parts along dimension 0
- positions: int32 [8192], P(('dp', 'sp')), parts along dimension 0
- attn_gain: bfloat16 [1536], replicated
- w_query: bfloat16 [1536, 1536], replicated
- w_key: bfloat16 [1536, 256], replicated
- w_value: bfloat16 [1536, 256], replicated
- w_out: bfloat16 [1536, 1536], replicated
- mlp_gain: bfloat16 [1536], replicated
- w_gate: bfloat16 [1536, 8960], replicated
- w_up: bfloat16 [1536, 8960], replicated
- w_down: bfloat16 [8960, 1536], replicated
Outputs:
- output 1: bfloat16 [8192, 1536], P(('dp', 'sp')), parts along dimension 0
- output 2: bfloat16 [8192, 4, 128], P('dp', 'sp'), parts along dimension 0
- output 3: bfloat16 [8192, 4, 128], P('dp', 'sp'), parts along dimension 0
There are 2 independent parts. The reference program is written for one: setup_inputs(seed, part) draws one part's arguments, and reference() takes and returns one part's arrays. A program takes and returns all parts, laid end to end along the dimension named above; an argument that names none is the same for every part.
All inputs are finite; a program needn't handle non-finite values.
Results may differ from the reference program's by a relative error of at most 0.00947955.
Values are sent between devices in bfloat16 or wider.
A program may use at most 1 GiB of HBM per device.

```python
import jax
import jax.numpy as jnp
from jax import lax

SEQ_LEN = 4096
MODEL_DIM = 1536
HEADS = 12
KV_HEADS = 2
HEAD_DIM = 128
FFN_DIM = 8960
CACHE_SLOTS = 4
PAD_MAX = 512
QUERY_BLOCK = 64
ROPE_THETA = 500000
NORM_EPS = 1e-5
GROUP_REP = HEADS // KV_HEADS


def setup_inputs(seed: int = 0, part: int = 0) -> dict:
    base_key = jax.random.key(seed)
    weight_keys = jax.random.split(base_key, 9)
    part_keys = jax.random.split(jax.random.fold_in(base_key, part), 2)
    hidden = jax.random.normal(part_keys[0], (SEQ_LEN, MODEL_DIM), jnp.float32)
    pad_len = jax.random.randint(part_keys[1], (), 0, PAD_MAX)
    token_idx = jnp.arange(SEQ_LEN, dtype=jnp.int32) - pad_len
    positions = jnp.where(token_idx < 0, -1, token_idx).astype(jnp.int32)
    att_width = HEADS * HEAD_DIM
    out_scale = att_width ** -0.5 * SEQ_LEN ** 0.5 / 8

    def normal_mat(key_in, mat_shape, mat_scale):
        return (jax.random.normal(key_in, mat_shape, jnp.float32) * mat_scale).astype(jnp.bfloat16)

    def make_gain(key_in):
        return (1.0 + 0.3 * jax.random.normal(key_in, (MODEL_DIM,), jnp.float32)).astype(jnp.bfloat16)

    return {
        "hidden": hidden.astype(jnp.bfloat16),
        "positions": positions,
        "attn_gain": make_gain(weight_keys[0]),
        "w_query": normal_mat(weight_keys[1], (MODEL_DIM, att_width), MODEL_DIM ** -0.5),
        "w_key": normal_mat(weight_keys[2], (MODEL_DIM, KV_HEADS * HEAD_DIM), MODEL_DIM ** -0.5),
        "w_value": normal_mat(weight_keys[3], (MODEL_DIM, KV_HEADS * HEAD_DIM), MODEL_DIM ** -0.5),
        "w_out": normal_mat(weight_keys[4], (att_width, MODEL_DIM), out_scale),
        "mlp_gain": make_gain(weight_keys[5]),
        "w_gate": normal_mat(weight_keys[6], (MODEL_DIM, FFN_DIM), MODEL_DIM ** -0.5),
        "w_up": normal_mat(weight_keys[7], (MODEL_DIM, FFN_DIM), MODEL_DIM ** -0.5),
        "w_down": normal_mat(weight_keys[8], (FFN_DIM, MODEL_DIM), FFN_DIM ** -0.5),
    }


def rms_norm(acts_in, gain_vec):
    rows_f32 = acts_in.astype(jnp.float32)
    mean_sq = jnp.mean(rows_f32 * rows_f32, axis=-1, keepdims=True)
    return (rows_f32 * lax.rsqrt(mean_sq + NORM_EPS) * gain_vec.astype(jnp.float32)).astype(jnp.bfloat16)


def rotary(heads_in, positions):
    half_dim = HEAD_DIM // 2
    inv_freq = 1.0 / (ROPE_THETA ** (jnp.arange(0, HEAD_DIM, 2, dtype=jnp.float32) / HEAD_DIM))
    angles = positions.astype(jnp.float32)[:, None] * inv_freq[None, :]
    cos_part = jnp.cos(angles)[:, None, :]
    sin_part = jnp.sin(angles)[:, None, :]
    first_half = heads_in[..., :half_dim]
    second_half = heads_in[..., half_dim:]
    return jnp.concatenate([first_half * cos_part - second_half * sin_part, second_half * cos_part + first_half * sin_part], axis=-1)


def reference(hidden, positions, attn_gain, w_query, w_key, w_value, w_out, mlp_gain, w_gate, w_up, w_down):
    h_norm = rms_norm(hidden, attn_gain)
    q_rot = rotary(jnp.dot(h_norm, w_query, preferred_element_type=jnp.float32).reshape(SEQ_LEN, HEADS, HEAD_DIM), positions).astype(jnp.bfloat16)
    k_rot = rotary(jnp.dot(h_norm, w_key, preferred_element_type=jnp.float32).reshape(SEQ_LEN, KV_HEADS, HEAD_DIM), positions).astype(jnp.bfloat16)
    v_proj = jnp.dot(h_norm, w_value, preferred_element_type=jnp.float32).astype(jnp.bfloat16).reshape(SEQ_LEN, KV_HEADS, HEAD_DIM)
    key_ok = positions >= 0
    key_idx = jnp.arange(SEQ_LEN)
    k_wide = k_rot.astype(jnp.float32)
    v_wide = v_proj.astype(jnp.float32)
    num_blocks = SEQ_LEN // QUERY_BLOCK
    q_blocks = q_rot.reshape(num_blocks, QUERY_BLOCK, KV_HEADS, GROUP_REP, HEAD_DIM)

    def attend(block_args):
        q_blk, block_idx = block_args
        q_idx = block_idx * QUERY_BLOCK + jnp.arange(QUERY_BLOCK)
        scores = jnp.einsum("qgrd,kgd->qgrk", q_blk.astype(jnp.float32), k_wide) * HEAD_DIM ** -0.5
        allowed = (key_idx[None, :] <= q_idx[:, None]) & key_ok[None, :]
        scores = jnp.where(allowed[:, None, None, :], scores, -jnp.inf)
        row_max = jnp.max(scores, axis=-1, keepdims=True)
        row_max = jnp.where(jnp.isfinite(row_max), row_max, 0.0)
        weights = jnp.exp(scores - row_max)
        row_sum = jnp.sum(weights, axis=-1, keepdims=True)
        weights = weights / jnp.where(row_sum > 0, row_sum, 1.0)
        return jnp.einsum("qgrk,kgd->qgrd", weights, v_wide).astype(jnp.bfloat16)

    attn_out = lax.map(attend, (q_blocks, jnp.arange(num_blocks))).reshape(SEQ_LEN, HEADS * HEAD_DIM)
    x_mid = (hidden.astype(jnp.float32) + jnp.dot(attn_out, w_out, preferred_element_type=jnp.float32)).astype(jnp.bfloat16)
    g_norm = rms_norm(x_mid, mlp_gain)
    gate_proj = jnp.dot(g_norm, w_gate, preferred_element_type=jnp.float32)
    up_proj = jnp.dot(g_norm, w_up, preferred_element_type=jnp.float32)
    act_mix = (jax.nn.silu(gate_proj) * up_proj).astype(jnp.bfloat16)
    hidden_out = (x_mid.astype(jnp.float32) + jnp.dot(act_mix, w_down, preferred_element_type=jnp.float32)).astype(jnp.bfloat16)
    k_cache = jnp.repeat(k_rot, CACHE_SLOTS // KV_HEADS, axis=1)
    v_cache = jnp.repeat(v_proj, CACHE_SLOTS // KV_HEADS, axis=1)
    return (hidden_out, k_cache, v_cache)
```

```python
import functools
import jax
import jax.numpy as jnp
from jax import lax
from jax.experimental import pallas as pl
from jax.experimental.pallas import tpu as pltpu

from jax.sharding import PartitionSpec as P

HEAD_DIM = 128
ROPE_THETA = 500000
BLOCK_LEN = 512
ROWS = 1024
DIM = 1536
FFN = 8960
NORM_EPS = 1e-5


def mlp_kernel(fb, rt, o_ref, x_ref, wout_ref, gain_ref, wg_hbm, wu_hbm, wd_hbm, out_ref, acc, g_buf, m_buf, wg, wu, wd, sems):
    steps = FFN // fb

    def copies(j, slot):
        off = pl.multiple_of(j * fb, 128)
        return (
            pltpu.make_async_copy(wg_hbm.at[:, pl.ds(off, fb)], wg.at[slot], sems.at[slot, 0]),
            pltpu.make_async_copy(wu_hbm.at[:, pl.ds(off, fb)], wu.at[slot], sems.at[slot, 1]),
            pltpu.make_async_copy(wd_hbm.at[pl.ds(off, fb), :], wd.at[slot], sems.at[slot, 2]),
        )

    for c in copies(0, 0):
        c.start()

    gain = gain_ref[...].astype(jnp.float32)

    def proj(r, _):
        rows = pl.ds(pl.multiple_of(r * 256, 256), 256)
        y = x_ref[rows, :].astype(jnp.float32) + jnp.dot(o_ref[rows, :], wout_ref[...], preferred_element_type=jnp.float32)
        y = y.astype(jnp.bfloat16).astype(jnp.float32)
        acc[rows, :] = y
        ms = jnp.mean(y * y, axis=-1, keepdims=True)
        g_buf[rows, :] = (y * lax.rsqrt(ms + NORM_EPS) * gain).astype(jnp.bfloat16)
        return 0

    lax.fori_loop(0, ROWS // 256, proj, 0)

    def step(j, _):
        slot = lax.rem(j, 2)
        for c in copies(j, slot):
            c.wait()

        @pl.when(j + 1 < steps)
        def _():
            for c in copies(j + 1, 1 - slot):
                c.start()

        def tile(r, _):
            rows = pl.ds(pl.multiple_of(r * rt, rt), rt)
            for c0 in range(0, fb, 256):
                cols = pl.ds(c0, 256)
                gate = jnp.dot(g_buf[rows, :], wg[slot, :, cols], preferred_element_type=jnp.float32)
                up = jnp.dot(g_buf[rows, :], wu[slot, :, cols], preferred_element_type=jnp.float32)
                m_buf[:, cols] = (gate / (1.0 + jnp.exp(-gate)) * up).astype(jnp.bfloat16)
            acc[rows, :] += jnp.dot(m_buf[...], wd[slot], preferred_element_type=jnp.float32)
            return 0

        lax.fori_loop(0, ROWS // rt, tile, 0)
        return 0

    lax.fori_loop(0, steps, step, 0)

    def fin(r, _):
        rows = pl.ds(pl.multiple_of(r * 128, 128), 128)
        out_ref[rows, :] = acc[rows, :].astype(jnp.bfloat16)
        return 0

    lax.fori_loop(0, ROWS // 128, fin, 0)


def mlp_call(o, x, w_out, gain, wg, wu, wd, fb=1280, rt=512):
    vm = pl.BlockSpec(memory_space=pltpu.VMEM)
    hbm = pl.BlockSpec(memory_space=pl.ANY)
    flops = 2 * ROWS * DIM * (DIM + 3 * FFN)
    return pl.pallas_call(
        functools.partial(mlp_kernel, fb, rt),
        out_shape=jax.ShapeDtypeStruct((ROWS, DIM), jnp.bfloat16),
        in_specs=[vm, vm, vm, vm, hbm, hbm, hbm],
        out_specs=vm,
        scratch_shapes=[
            pltpu.VMEM((ROWS, DIM), jnp.float32),
            pltpu.VMEM((ROWS, DIM), jnp.bfloat16),
            pltpu.VMEM((rt, fb), jnp.bfloat16),
            pltpu.VMEM((2, DIM, fb), jnp.bfloat16),
            pltpu.VMEM((2, DIM, fb), jnp.bfloat16),
            pltpu.VMEM((2, fb, DIM), jnp.bfloat16),
            pltpu.SemaphoreType.DMA((2, 3)),
        ],
        compiler_params=pltpu.CompilerParams(vmem_limit_bytes=60 << 20),
        cost_estimate=pl.CostEstimate(flops=flops, bytes_accessed=3 * DIM * FFN * 2, transcendentals=ROWS * FFN),
        name="mlp_block",
    )(o, x, w_out, gain.reshape(1, DIM), wg, wu, wd)


def rms_norm(acts_in, gain_vec):
    rows_f32 = acts_in.astype(jnp.float32)
    mean_sq = jnp.mean(rows_f32 * rows_f32, axis=-1, keepdims=True)
    return (rows_f32 * lax.rsqrt(mean_sq + NORM_EPS) * gain_vec.astype(jnp.float32)).astype(jnp.bfloat16)


def rotary(heads_in, positions):
    half_dim = HEAD_DIM // 2
    inv_freq = 1.0 / (ROPE_THETA ** (jnp.arange(0, HEAD_DIM, 2, dtype=jnp.float32) / HEAD_DIM))
    angles = positions.astype(jnp.float32)[:, None] * inv_freq[None, :]
    cos_part = jnp.cos(angles)[:, None, :]
    sin_part = jnp.sin(angles)[:, None, :]
    first_half = heads_in[..., :half_dim]
    second_half = heads_in[..., half_dim:]
    return jnp.concatenate([first_half * cos_part - second_half * sin_part, second_half * cos_part + first_half * sin_part], axis=-1)


def causal_attention(q_grp, k_all, v_all, key_ok, q_base):
    q_len, kv_local, group_rep, head_dim = q_grp.shape
    block_len = min(BLOCK_LEN, q_len)
    num_qblocks = q_len // block_len
    score_scale = head_dim ** -0.5
    q_blocks = q_grp.reshape(num_qblocks, block_len, kv_local, group_rep, head_dim)
    offsets = jnp.arange(block_len)

    def one_block(block_args):
        q_blk, block_idx = block_args
        q_start = q_base + block_idx * block_len
        q_idx = q_start + offsets

        def kv_step(kv_idx, run_state):
            run_max, run_sum, acc_pv = run_state
            k_start = kv_idx * block_len
            k_blk = lax.dynamic_slice_in_dim(k_all, k_start, block_len, 0)
            v_blk = lax.dynamic_slice_in_dim(v_all, k_start, block_len, 0)
            ok_blk = lax.dynamic_slice_in_dim(key_ok, k_start, block_len, 0)
            k_idx = k_start + offsets
            allowed = (k_idx[None, :] <= q_idx[:, None]) & ok_blk[None, :]
            scores = jnp.einsum("qgrd,kgd->qgrk", q_blk, k_blk, preferred_element_type=jnp.float32) * score_scale
            scores = jnp.where(allowed[:, None, None, :], scores, -jnp.inf)
            new_max = jnp.maximum(run_max, jnp.max(scores, axis=-1))
            safe_max = jnp.where(jnp.isfinite(new_max), new_max, 0.0)
            weights = jnp.exp(scores - safe_max[..., None])
            decay_fac = jnp.exp(run_max - safe_max)
            run_sum = run_sum * decay_fac + jnp.sum(weights, axis=-1)
            acc_pv = acc_pv * decay_fac[..., None] + jnp.einsum("qgrk,kgd->qgrd", weights.astype(jnp.bfloat16), v_blk, preferred_element_type=jnp.float32)
            return new_max, run_sum, acc_pv

        init_state = (jnp.full((block_len, kv_local, group_rep), -jnp.inf, jnp.float32), jnp.zeros((block_len, kv_local, group_rep), jnp.float32), jnp.zeros((block_len, kv_local, group_rep, head_dim), jnp.float32))
        num_steps = q_start // block_len + 1
        final_max, final_sum, final_acc = lax.fori_loop(0, num_steps, kv_step, init_state)
        return (final_acc / jnp.where(final_sum > 0, final_sum, 1.0)[..., None]).astype(jnp.bfloat16)

    attn_blocks = lax.map(one_block, (q_blocks, jnp.arange(num_qblocks)))
    return attn_blocks.reshape(q_len, kv_local, group_rep, head_dim)


def solution(mesh):
    groups = mesh.shape["sp"]

    def layer_shard(hidden, positions, attn_gain, w_query, w_key, w_value, w_out, mlp_gain, w_gate, w_up, w_down):
        tok_rows = hidden.shape[0]
        heads = w_query.shape[1] // HEAD_DIM
        kv_heads = w_key.shape[1] // HEAD_DIM
        cache_slots = max(kv_heads, groups)
        kv_local = cache_slots // groups
        copies = cache_slots // kv_heads
        heads_local = heads // groups
        h_norm = rms_norm(hidden, attn_gain)
        q_rot = rotary(jnp.dot(h_norm, w_query, preferred_element_type=jnp.float32).reshape(tok_rows, heads, HEAD_DIM), positions).astype(jnp.bfloat16)
        k_rot = rotary(jnp.dot(h_norm, w_key, preferred_element_type=jnp.float32).reshape(tok_rows, kv_heads, HEAD_DIM), positions).astype(jnp.bfloat16)
        v_proj = jnp.dot(h_norm, w_value, preferred_element_type=jnp.float32).astype(jnp.bfloat16).reshape(tok_rows, kv_heads, HEAD_DIM)
        slot_shape = (tok_rows, kv_heads, copies, HEAD_DIM)
        k_slots = jnp.broadcast_to(k_rot[:, :, None, :], slot_shape).reshape(tok_rows, cache_slots, HEAD_DIM)
        v_slots = jnp.broadcast_to(v_proj[:, :, None, :], slot_shape).reshape(tok_rows, cache_slots, HEAD_DIM)
        q_heads = lax.all_to_all(q_rot, "sp", 1, 0, tiled=True)
        k_heads = lax.all_to_all(k_slots, "sp", 1, 0, tiled=True)
        v_heads = lax.all_to_all(v_slots, "sp", 1, 0, tiled=True)
        pos_all = lax.all_gather(positions, "sp", axis=0, tiled=True)
        seq_len = q_heads.shape[0]
        q_grp = q_heads.reshape(seq_len, kv_local, heads_local // kv_local, HEAD_DIM)
        attn_heads = causal_attention(q_grp, k_heads, v_heads, pos_all >= 0, 0).reshape(seq_len, heads_local, HEAD_DIM)
        attn_tok = lax.all_to_all(attn_heads, "sp", 0, 1, tiled=True).reshape(tok_rows, heads * HEAD_DIM)
        hidden_out = mlp_call(attn_tok, hidden, w_out, mlp_gain, w_gate, w_up, w_down)
        return hidden_out, k_heads, v_heads

    row_spec = P(("dp", "sp"), None)
    cache_spec = P("dp", "sp", None)
    return jax.shard_map(layer_shard, mesh=mesh, in_specs=(row_spec, P(("dp", "sp")), P(), P(), P(), P(), P(), P(), P(), P(), P()), out_specs=(row_spec, cache_spec, cache_spec), check_vma=False)
```

```python
import functools
import jax
import jax.numpy as jnp
from jax import lax
from jax.experimental import pallas as pl
from jax.experimental.pallas import tpu as pltpu
from jax.sharding import PartitionSpec as P

ROWS = 1024
DIM = 1536
FFN = 8960
NORM_EPS = 1e-5


def mlp_kernel(fb, rt, o_ref, x_ref, wout_ref, gain_ref, wg_hbm, wu_hbm, wd_hbm, out_ref, acc, g_buf, m_buf, wg, wu, wd, sems):
    steps = FFN // fb

    def copies(j, slot):
        off = pl.multiple_of(j * fb, 128)
        return (
            pltpu.make_async_copy(wg_hbm.at[:, pl.ds(off, fb)], wg.at[slot], sems.at[slot, 0]),
            pltpu.make_async_copy(wu_hbm.at[:, pl.ds(off, fb)], wu.at[slot], sems.at[slot, 1]),
            pltpu.make_async_copy(wd_hbm.at[pl.ds(off, fb), :], wd.at[slot], sems.at[slot, 2]),
        )

    for c in copies(0, 0):
        c.start()

    gain = gain_ref[...].astype(jnp.float32)

    def proj(r, _):
        rows = pl.ds(pl.multiple_of(r * 256, 256), 256)
        y = x_ref[rows, :].astype(jnp.float32) + jnp.dot(o_ref[rows, :], wout_ref[...], preferred_element_type=jnp.float32)
        y = y.astype(jnp.bfloat16).astype(jnp.float32)
        acc[rows, :] = y
        ms = jnp.mean(y * y, axis=-1, keepdims=True)
        g_buf[rows, :] = (y * lax.rsqrt(ms + NORM_EPS) * gain).astype(jnp.bfloat16)
        return 0

    lax.fori_loop(0, ROWS // 256, proj, 0)

    def step(j, _):
        slot = lax.rem(j, 2)
        for c in copies(j, slot):
            c.wait()

        @pl.when(j + 1 < steps)
        def _():
            for c in copies(j + 1, 1 - slot):
                c.start()

        def tile(r, _):
            rows = pl.ds(pl.multiple_of(r * rt, rt), rt)
            for c0 in range(0, fb, 256):
                cols = pl.ds(c0, 256)
                gate = jnp.dot(g_buf[rows, :], wg[slot, :, cols], preferred_element_type=jnp.float32)
                up = jnp.dot(g_buf[rows, :], wu[slot, :, cols], preferred_element_type=jnp.float32)
                m_buf[:, cols] = (gate / (1.0 + jnp.exp(-gate)) * up).astype(jnp.bfloat16)
            acc[rows, :] += jnp.dot(m_buf[...], wd[slot], preferred_element_type=jnp.float32)
            return 0

        lax.fori_loop(0, ROWS // rt, tile, 0)
        return 0

    lax.fori_loop(0, steps, step, 0)

    def fin(r, _):
        rows = pl.ds(pl.multiple_of(r * 128, 128), 128)
        out_ref[rows, :] = acc[rows, :].astype(jnp.bfloat16)
        return 0

    lax.fori_loop(0, ROWS // 128, fin, 0)


def mlp_call(o, x, w_out, gain, wg, wu, wd, fb=1280, rt=512):
    vm = pl.BlockSpec(memory_space=pltpu.VMEM)
    hbm = pl.BlockSpec(memory_space=pl.ANY)
    flops = 2 * ROWS * DIM * (DIM + 3 * FFN)
    return pl.pallas_call(
        functools.partial(mlp_kernel, fb, rt),
        out_shape=jax.ShapeDtypeStruct((ROWS, DIM), jnp.bfloat16),
        in_specs=[vm, vm, vm, vm, hbm, hbm, hbm],
        out_specs=vm,
        scratch_shapes=[
            pltpu.VMEM((ROWS, DIM), jnp.float32),
            pltpu.VMEM((ROWS, DIM), jnp.bfloat16),
            pltpu.VMEM((rt, fb), jnp.bfloat16),
            pltpu.VMEM((2, DIM, fb), jnp.bfloat16),
            pltpu.VMEM((2, DIM, fb), jnp.bfloat16),
            pltpu.VMEM((2, fb, DIM), jnp.bfloat16),
            pltpu.SemaphoreType.DMA((2, 3)),
        ],
        compiler_params=pltpu.CompilerParams(vmem_limit_bytes=60 << 20),
        cost_estimate=pl.CostEstimate(flops=flops, bytes_accessed=3 * DIM * FFN * 2, transcendentals=ROWS * FFN),
        name="mlp_block",
    )(o, x, w_out, gain.reshape(1, DIM), wg, wu, wd)


HEAD_DIM = 128
HEADS = 12
GROUP = 6
ROPE_THETA = 500000
SCALE_LOG2E = 1.4426950408889634 * HEAD_DIM ** -0.5
NEG = -2.0e38
QB = 512
MESH = pl.DeviceIdType.MESH


def attend(q_att, kv, vt, acc, m_s, l_s, tb, src, chunk, kv_head, keys, mask_fn):
    q_src, q_off = tb // 2, pl.multiple_of(lax.rem(tb, 2) * QB, QB)
    k_off = pl.multiple_of(chunk * keys, keys)
    for h in range(GROUP):
        k_blk = kv[src, kv_head, 0, pl.ds(k_off, keys), :]
        q_blk = q_att[q_src, h, pl.ds(q_off, QB), :]
        s = lax.dot_general(k_blk, q_blk, (((1,), (1,)), ((), ())), preferred_element_type=jnp.float32)
        if mask_fn is not None:
            s = mask_fn(s)
        m_prev = m_s[tb, h]
        m_new = jnp.maximum(m_prev, jnp.max(s, axis=0, keepdims=True))
        p = jnp.exp2((s - m_new) * SCALE_LOG2E)
        decay = jnp.exp2((m_prev - m_new) * SCALE_LOG2E)
        l_s[tb, h] = l_s[tb, h] * decay + jnp.sum(p, axis=0, keepdims=True)
        pv = jnp.dot(vt[src, :, pl.ds(k_off, keys)], p.astype(jnp.bfloat16), preferred_element_type=jnp.float32)
        acc[tb, h] = acc[tb, h] * decay + pv
        m_s[tb, h] = m_new


def attn_kernel(pad_ref, x_ref, cos_ref, sin_ref, gain_ref, wq_ref, wk_ref, wv_ref, out_ref, kc_ref, vc_ref,
                h_buf, q_att, q_send, kv, vt, acc, m_s, l_s, o_buf, send_sem, recv_sem, osend_sem, orecv_sem, cache_sem, ocopy_sem):
    me = lax.axis_index("sp")
    x = me // 2
    c = lax.rem(me, 2)
    partner = 2 * x + (1 - c)
    cross = 2 * (1 - x) + c
    diag = 2 * (1 - x) + (1 - c)
    pad = pad_ref[0]

    barrier = pltpu.get_barrier_semaphore()
    for peer in (partner, cross):
        pl.semaphore_signal(barrier, inc=1, device_id={"sp": peer}, device_id_type=MESH)
    pl.semaphore_wait(barrier, 2)

    gain = gain_ref[...].astype(jnp.float32)

    def rope(t, rows):
        return (t * cos_ref[rows, :] + pltpu.roll(t, 64, 1) * sin_ref[rows, :]).astype(jnp.bfloat16)

    def kv_rows(r, _):
        rows = pl.ds(pl.multiple_of(r * 256, 256), 256)
        xf = x_ref[rows, :].astype(jnp.float32)
        ms = jnp.mean(xf * xf, axis=-1, keepdims=True)
        h = (xf * lax.rsqrt(ms + NORM_EPS) * gain).astype(jnp.bfloat16)
        h_buf[rows, :] = h
        k = jnp.dot(h, wk_ref[...], preferred_element_type=jnp.float32)
        v = jnp.dot(h, wv_ref[...], preferred_element_type=jnp.float32).astype(jnp.bfloat16)
        for g in range(2):
            kv[me, g, 0, rows, :] = rope(k[:, g * 128:(g + 1) * 128], rows)
            kv[me, g, 1, rows, :] = v[:, g * 128:(g + 1) * 128]
        return 0

    lax.fori_loop(0, ROWS // 256, kv_rows, 0)

    def kv_copy(src, i, peer):
        return pltpu.make_async_remote_copy(src_ref=kv.at[src], dst_ref=kv.at[src], send_sem=send_sem.at[i], recv_sem=recv_sem.at[i],
                                            device_id={"sp": peer}, device_id_type=MESH)

    to_cross = kv_copy(me, 0, cross)
    to_cross.start()
    to_partner = kv_copy(me, 1, partner)
    to_partner.start()

    def q_rows(dst, head_group):
        def body(r, _):
            rows = pl.ds(pl.multiple_of(r * 256, 256), 256)
            col = pl.multiple_of(head_group * 768, 768)
            q = jnp.dot(h_buf[rows, :], wq_ref[:, pl.ds(col, 768)], preferred_element_type=jnp.float32)
            for h in range(GROUP):
                dst[h, rows, :] = rope(q[:, h * 128:(h + 1) * 128], rows)
            return 0

        lax.fori_loop(0, ROWS // 256, body, 0)

    q_rows(q_send, 1 - c)
    q_copy = pltpu.make_async_remote_copy(src_ref=q_send, dst_ref=q_att.at[c], send_sem=send_sem.at[3], recv_sem=recv_sem.at[3],
                                          device_id={"sp": partner}, device_id_type=MESH)
    q_copy.start()
    q_rows(q_att.at[c], c)

    def flip(src):
        vt[src] = kv[src, c, 1].T

    def cache_copy(src, i):
        rows = pl.ds(pl.multiple_of(src * ROWS, ROWS), ROWS)
        return (pltpu.make_async_copy(kv.at[src, x, 0], kc_ref.at[rows, :], cache_sem.at[i, 0]),
                pltpu.make_async_copy(kv.at[src, x, 1], vc_ref.at[rows, :], cache_sem.at[i, 1]))

    for cp in cache_copy(me, 0):
        cp.start()
    flip(me)
    to_partner.wait_recv()
    for cp in cache_copy(partner, 1):
        cp.start()
    flip(partner)
    q_copy.wait_recv()

    m_s[...] = jnp.full_like(m_s, NEG)
    l_s[...] = jnp.zeros_like(l_s)
    acc[...] = jnp.zeros_like(acc)

    def mask_at(k_base, q_base):
        def mask(s):
            k_idx = lax.broadcasted_iota(jnp.int32, s.shape, 0) + k_base
            q_idx = lax.broadcasted_iota(jnp.int32, s.shape, 1) + q_base
            return jnp.where((k_idx <= q_idx) & (k_idx >= pad), s, NEG)
        return mask

    def local_block(tb, kb, masked):
        base = x * 2 * ROWS
        src = 2 * x + kb // 2
        fn = mask_at(base + kb * QB, base + tb * QB) if masked else None
        attend(q_att, kv, vt, acc, m_s, l_s, tb, src, lax.rem(kb, 2), c, QB, fn)

    def local_tb(tb, _):
        first = jnp.minimum(1 - x, tb)

        def masked(i, _):
            local_block(tb, jnp.where(i == 0, tb, 0), True)
            return 0

        lax.fori_loop(0, 1 + first, masked, 0)

        def plain(kb, _):
            local_block(tb, kb, False)
            return 0

        lax.fori_loop(first, tb, plain, 0)
        return 0

    lax.fori_loop(0, 4, local_tb, 0)

    to_cross.wait_recv()
    forward = kv_copy(cross, 2, partner)
    forward.start()
    for cp in cache_copy(cross, 2):
        cp.start()
    flip(cross)
    kv_copy(diag, 2, partner).wait_recv()
    for cp in cache_copy(diag, 3):
        cp.start()
    flip(diag)

    def o_copies(i, tb):
        rows = pl.ds(pl.multiple_of(lax.rem(tb, 2) * QB, QB), QB)
        cols = pl.ds(pl.multiple_of(c * 768, 768), 768)
        return pltpu.make_async_remote_copy(src_ref=o_buf.at[tb], dst_ref=out_ref.at[rows, cols], send_sem=osend_sem.at[i], recv_sem=orecv_sem.at[i],
                                            device_id={"sp": partner}, device_id_type=MESH), pltpu.make_async_copy(o_buf.at[tb], out_ref.at[rows, cols], ocopy_sem.at[i])

    def finish(tb):
        def remote(src, _):
            def pad_mask(s):
                k_idx = lax.broadcasted_iota(jnp.int32, s.shape, 0) + src * ROWS
                return jnp.where(k_idx >= pad, s, NEG)

            attend(q_att, kv, vt, acc, m_s, l_s, tb, src, 0, c, ROWS, pad_mask)
            return 0

        lax.fori_loop(0, 2 * x, remote, 0)
        q_idx = lax.broadcasted_iota(jnp.int32, (1, QB), 1) + (x * 2 * ROWS + tb * QB)
        for h in range(GROUP):
            inv = jnp.where(q_idx >= pad, 1.0 / l_s[tb, h], 0.0)
            o_buf[tb, :, h * 128:(h + 1) * 128] = (acc[tb, h] * inv).T.astype(jnp.bfloat16)

    def partner_tb(i, _):
        tb = 2 * (1 - c) + i
        finish(tb)
        o_copies(i, tb)[0].start()
        return 0

    lax.fori_loop(0, 2, partner_tb, 0)

    def own_tb(i, _):
        tb = 2 * c + i
        finish(tb)
        o_copies(i, tb)[1].start()
        return 0

    lax.fori_loop(0, 2, own_tb, 0)

    to_cross.wait_send()
    to_partner.wait_send()
    forward.wait_send()
    q_copy.wait_send()
    for i, src in enumerate((me, partner, cross, diag)):
        for cp in cache_copy(src, i):
            cp.wait()
    for i in range(2):
        o_copies(i, 2 * (1 - c) + i)[0].wait_send()
        o_copies(i, 2 * c + i)[1].wait()
    for i in range(2):
        rows = pl.ds(i * QB, QB)
        cols = pl.ds(pl.multiple_of((1 - c) * 768, 768), 768)
        pltpu.make_async_remote_copy(src_ref=o_buf.at[i], dst_ref=out_ref.at[rows, cols], send_sem=osend_sem.at[i], recv_sem=orecv_sem.at[i],
                                     device_id={"sp": partner}, device_id_type=MESH).wait_recv()


def attn_call(pad, x, cos, sin, gain, w_query, w_key, w_value):
    vm = pl.BlockSpec(memory_space=pltpu.VMEM)
    hbm = pl.BlockSpec(memory_space=pl.ANY)
    flops = 2 * ROWS * DIM * 2048 + 4 * 128 * 3 * 4096 * 2048
    bf = jnp.bfloat16
    return pl.pallas_call(
        attn_kernel,
        out_shape=(jax.ShapeDtypeStruct((ROWS, DIM), bf), jax.ShapeDtypeStruct((4 * ROWS, 128), bf), jax.ShapeDtypeStruct((4 * ROWS, 128), bf)),
        in_specs=[pl.BlockSpec(memory_space=pltpu.SMEM)] + [vm] * 7,
        out_specs=(hbm, hbm, hbm),
        scratch_shapes=[
            pltpu.VMEM((ROWS, DIM), bf),
            pltpu.VMEM((2, GROUP, ROWS, 128), bf),
            pltpu.VMEM((GROUP, ROWS, 128), bf),
            pltpu.VMEM((4, 2, 2, ROWS, 128), bf),
            pltpu.VMEM((4, 128, ROWS), bf),
            pltpu.VMEM((4, GROUP, 128, QB), jnp.float32),
            pltpu.VMEM((4, GROUP, 1, QB), jnp.float32),
            pltpu.VMEM((4, GROUP, 1, QB), jnp.float32),
            pltpu.VMEM((4, QB, 768), bf),
            pltpu.SemaphoreType.DMA((4,)),
            pltpu.SemaphoreType.DMA((4,)),
            pltpu.SemaphoreType.DMA((2,)),
            pltpu.SemaphoreType.DMA((2,)),
            pltpu.SemaphoreType.DMA((4, 2)),
            pltpu.SemaphoreType.DMA((2,)),
        ],
        compiler_params=pltpu.CompilerParams(vmem_limit_bytes=60 << 20, collective_id=0, has_side_effects=True),
        cost_estimate=pl.CostEstimate(flops=flops, bytes_accessed=20 << 20, transcendentals=3 * 4096 * 2048),
        name="attn_block",
    )(pad, x, cos, sin, gain.reshape(1, DIM), w_query, w_key, w_value)


def solution(mesh):
    def layer_shard(hidden, positions, attn_gain, w_query, w_key, w_value, w_out, mlp_gain, w_gate, w_up, w_down):
        inv_freq = 1.0 / (ROPE_THETA ** (jnp.arange(0, HEAD_DIM, 2, dtype=jnp.float32) / HEAD_DIM))
        angles = positions.astype(jnp.float32)[:, None] * inv_freq[None, :]
        cos, sin = jnp.cos(angles), jnp.sin(angles)
        cos = jnp.concatenate([cos, cos], axis=-1)
        sin = jnp.concatenate([-sin, sin], axis=-1)
        pad = (lax.axis_index("sp") * ROWS + ROWS - 1 - positions[ROWS - 1]).reshape(1)
        attn, k_cache, v_cache = attn_call(pad, hidden, cos, sin, attn_gain, w_query, w_key, w_value)
        hidden_out = mlp_call(attn, hidden, w_out, mlp_gain, w_gate, w_up, w_down)
        return hidden_out, k_cache.reshape(4 * ROWS, 1, 128), v_cache.reshape(4 * ROWS, 1, 128)

    row_spec = P(("dp", "sp"), None)
    cache_spec = P("dp", "sp", None)
    return jax.shard_map(layer_shard, mesh=mesh, in_specs=(row_spec, P(("dp", "sp")), P(), P(), P(), P(), P(), P(), P(), P(), P()), out_specs=(row_spec, cache_spec, cache_spec), check_vma=False)
```

```python
import functools
import itertools
import jax
import jax.numpy as jnp
from jax import lax
from jax.experimental import pallas as pl
from jax.experimental.pallas import tpu as pltpu
from jax.sharding import PartitionSpec as P

ROWS = 1024
DIM = 1536
FFN = 8960
NORM_EPS = 1e-5


def mlp_kernel(fb, rt, o_ref, x_ref, wout_ref, gain_ref, wg_hbm, wu_hbm, wd_hbm, out_ref, acc, g_buf, m_buf, wg, wu, wd, sems):
    steps = FFN // fb

    def copies(j, slot):
        off = pl.multiple_of(j * fb, 128)
        return (
            pltpu.make_async_copy(wg_hbm.at[:, pl.ds(off, fb)], wg.at[slot], sems.at[slot, 0]),
            pltpu.make_async_copy(wu_hbm.at[:, pl.ds(off, fb)], wu.at[slot], sems.at[slot, 1]),
            pltpu.make_async_copy(wd_hbm.at[pl.ds(off, fb), :], wd.at[slot], sems.at[slot, 2]),
        )

    for c in copies(0, 0):
        c.start()

    gain = gain_ref[...].astype(jnp.float32)

    def proj(r, _):
        rows = pl.ds(pl.multiple_of(r * 256, 256), 256)
        y = x_ref[rows, :].astype(jnp.float32) + jnp.dot(o_ref[rows, :], wout_ref[...], preferred_element_type=jnp.float32)
        y = y.astype(jnp.bfloat16).astype(jnp.float32)
        acc[rows, :] = y
        ms = jnp.mean(y * y, axis=-1, keepdims=True)
        g_buf[rows, :] = (y * lax.rsqrt(ms + NORM_EPS) * gain).astype(jnp.bfloat16)
        return 0

    lax.fori_loop(0, ROWS // 256, proj, 0)

    def step(j, _):
        slot = lax.rem(j, 2)
        for c in copies(j, slot):
            c.wait()

        @pl.when(j + 1 < steps)
        def _():
            for c in copies(j + 1, 1 - slot):
                c.start()

        def tile(r, _):
            rows = pl.ds(pl.multiple_of(r * rt, rt), rt)
            for c0 in range(0, fb, 256):
                cols = pl.ds(c0, 256)
                gate = jnp.dot(g_buf[rows, :], wg[slot, :, cols], preferred_element_type=jnp.float32)
                up = jnp.dot(g_buf[rows, :], wu[slot, :, cols], preferred_element_type=jnp.float32)
                m_buf[:, cols] = (gate / (1.0 + jnp.exp(-gate)) * up).astype(jnp.bfloat16)
            acc[rows, :] += jnp.dot(m_buf[...], wd[slot], preferred_element_type=jnp.float32)
            return 0

        lax.fori_loop(0, ROWS // rt, tile, 0)
        return 0

    lax.fori_loop(0, steps, step, 0)

    def fin(r, _):
        rows = pl.ds(pl.multiple_of(r * 128, 128), 128)
        out_ref[rows, :] = acc[rows, :].astype(jnp.bfloat16)
        return 0

    lax.fori_loop(0, ROWS // 128, fin, 0)


def mlp_call(o, x, w_out, gain, wg, wu, wd, fb=1280, rt=512):
    vm = pl.BlockSpec(memory_space=pltpu.VMEM)
    hbm = pl.BlockSpec(memory_space=pl.ANY)
    flops = 2 * ROWS * DIM * (DIM + 3 * FFN)
    return pl.pallas_call(
        functools.partial(mlp_kernel, fb, rt),
        out_shape=jax.ShapeDtypeStruct((ROWS, DIM), jnp.bfloat16),
        in_specs=[vm, vm, vm, vm, hbm, hbm, hbm],
        out_specs=vm,
        scratch_shapes=[
            pltpu.VMEM((ROWS, DIM), jnp.float32),
            pltpu.VMEM((ROWS, DIM), jnp.bfloat16),
            pltpu.VMEM((rt, fb), jnp.bfloat16),
            pltpu.VMEM((2, DIM, fb), jnp.bfloat16),
            pltpu.VMEM((2, DIM, fb), jnp.bfloat16),
            pltpu.VMEM((2, fb, DIM), jnp.bfloat16),
            pltpu.SemaphoreType.DMA((2, 3)),
        ],
        compiler_params=pltpu.CompilerParams(vmem_limit_bytes=60 << 20),
        cost_estimate=pl.CostEstimate(flops=flops, bytes_accessed=3 * DIM * FFN * 2, transcendentals=ROWS * FFN),
        name="mlp_block",
    )(o, x, w_out, gain.reshape(1, DIM), wg, wu, wd)


HEAD_DIM = 128
HEADS = 12
GROUP = 6
ROPE_THETA = 500000
SCALE_LOG2E = 1.4426950408889634 * HEAD_DIM ** -0.5
NEG = -2.0e38
QB = 512
KC = 256
PC = 64
MESH = pl.DeviceIdType.MESH


def flash_run(n, item_fn, head_sel, biased, q_att, kv, vt, acc, m_s, l_s, s_buf, p_buf, top_s, decay_s, bias):
    def scores(i, pair):
        tb, src, chunk, b = item_fn(i)
        q_off = pl.multiple_of(lax.rem(tb, 2) * QB, QB)
        k_off = pl.multiple_of(chunk * QB, QB)
        for u in range(2):
            q_blk = q_att[tb // 2, 2 * pair + u, pl.ds(q_off, QB), :]
            top = jnp.full((8, QB), NEG, jnp.float32)
            for k0 in range(0, QB, KC):
                k_blk = kv[src, head_sel, 0, pl.ds(k_off + k0, KC), :]
                s = lax.dot_general(k_blk, q_blk, (((1,), (1,)), ((), ())), preferred_element_type=jnp.float32)
                if biased:
                    s = s + bias[b, k0:k0 + KC, :]
                s_buf[pair, u, k0:k0 + KC, :] = s
                top = jnp.maximum(top, jnp.max(s.reshape(KC // 8, 8, QB), axis=0))
                yield
            top_s[pair, u] = top

    def weights(i, pair):
        tb = item_fn(i)[0]
        for u in range(2):
            h = 2 * pair + u
            m_prev = m_s[tb, h]
            m_new = jnp.maximum(m_prev, jnp.max(top_s[pair, u], axis=0, keepdims=True))
            m8 = jnp.broadcast_to(m_new, (8, QB))
            total = jnp.zeros((8, QB), jnp.float32)
            for k0 in range(0, QB, PC):
                s = s_buf[pair, u, k0:k0 + PC, :].reshape(PC // 8, 8, QB)
                p = jnp.exp2((s - m8[None]) * SCALE_LOG2E)
                total = total + jnp.sum(p, axis=0)
                p_buf[pair, u, k0:k0 + PC, :] = p.reshape(PC, QB).astype(jnp.bfloat16)
                if (k0 + PC) % KC == 0:
                    yield
            decay = jnp.exp2((m_prev - m_new) * SCALE_LOG2E)
            decay_s[pair, u] = decay
            l_s[tb, h] = l_s[tb, h] * decay + jnp.sum(total, axis=0, keepdims=True)
            m_s[tb, h] = m_new

    def values(i, pair):
        tb, src, chunk, _ = item_fn(i)
        k_off = pl.multiple_of(chunk * QB, QB)
        for u in range(2):
            h = 2 * pair + u
            pv = jnp.dot(vt[src, :, pl.ds(k_off, QB)], p_buf[pair, u], preferred_element_type=jnp.float32)
            acc[tb, h] = acc[tb, h] * decay_s[pair, u] + pv
            for _ in range(QB // KC):
                yield

    def together(*parts):
        for _ in itertools.zip_longest(*parts):
            pass

    @pl.when(n > 0)
    def _():
        p_buf[2] = jnp.zeros_like(p_buf[2])
        decay_s[2] = jnp.ones_like(decay_s[2])
        together(scores(0, 0))

        def step(i, _):
            nxt = jnp.minimum(i + 1, n - 1)
            together(weights(i, 0), scores(i, 1), values(jnp.maximum(i - 1, 0), 2))
            together(weights(i, 1), scores(i, 2), values(i, 0))
            together(weights(i, 2), scores(nxt, 0), values(i, 1))
            return 0

        lax.fori_loop(0, n, step, 0)
        together(values(n - 1, 2))


def attn_kernel(pad_ref, x_ref, cos_ref, sin_ref, gain_ref, wq_ref, wk_ref, wv_ref, out_ref, kc_ref, vc_ref,
                h_buf, q_att, q_send, kv, vt, acc, m_s, l_s, s_buf, p_buf, top_s, decay_s, bias, o_buf, send_sem, recv_sem, osend_sem, orecv_sem, cache_sem, ocopy_sem):
    me = lax.axis_index("sp")
    x = me // 2
    c = lax.rem(me, 2)
    partner = 2 * x + (1 - c)
    cross = 2 * (1 - x) + c
    diag = 2 * (1 - x) + (1 - c)
    pad = pad_ref[0]

    barrier = pltpu.get_barrier_semaphore()
    for peer in (partner, cross):
        pl.semaphore_signal(barrier, inc=1, device_id={"sp": peer}, device_id_type=MESH)
    pl.semaphore_wait(barrier, 2)

    gain = gain_ref[...].astype(jnp.float32)

    def rope(t, rows):
        return (t * cos_ref[rows, :] + pltpu.roll(t, 64, 1) * sin_ref[rows, :]).astype(jnp.bfloat16)

    def kv_rows(r, _):
        rows = pl.ds(pl.multiple_of(r * 256, 256), 256)
        xf = x_ref[rows, :].astype(jnp.float32)
        ms = jnp.mean(xf * xf, axis=-1, keepdims=True)
        h = (xf * lax.rsqrt(ms + NORM_EPS) * gain).astype(jnp.bfloat16)
        h_buf[rows, :] = h
        k = jnp.dot(h, wk_ref[...], preferred_element_type=jnp.float32)
        v = jnp.dot(h, wv_ref[...], preferred_element_type=jnp.float32).astype(jnp.bfloat16)
        for g in range(2):
            kv[me, g, 0, rows, :] = rope(k[:, g * 128:(g + 1) * 128], rows)
            kv[me, g, 1, rows, :] = v[:, g * 128:(g + 1) * 128]
        return 0

    lax.fori_loop(0, ROWS // 256, kv_rows, 0)

    def kv_copy(src, i, peer):
        return pltpu.make_async_remote_copy(src_ref=kv.at[src], dst_ref=kv.at[src], send_sem=send_sem.at[i], recv_sem=recv_sem.at[i],
                                            device_id={"sp": peer}, device_id_type=MESH)

    to_cross = kv_copy(me, 0, cross)
    to_cross.start()
    to_partner = kv_copy(me, 1, partner)
    to_partner.start()

    def q_rows(dst, head_group):
        def body(r, _):
            rows = pl.ds(pl.multiple_of(r * 256, 256), 256)
            col = pl.multiple_of(head_group * 768, 768)
            q = jnp.dot(h_buf[rows, :], wq_ref[:, pl.ds(col, 768)], preferred_element_type=jnp.float32)
            for h in range(GROUP):
                dst[h, rows, :] = rope(q[:, h * 128:(h + 1) * 128], rows)
            return 0

        lax.fori_loop(0, ROWS // 256, body, 0)

    q_rows(q_send, 1 - c)
    q_copy = pltpu.make_async_remote_copy(src_ref=q_send, dst_ref=q_att.at[c], send_sem=send_sem.at[3], recv_sem=recv_sem.at[3],
                                          device_id={"sp": partner}, device_id_type=MESH)
    q_copy.start()
    q_rows(q_att.at[c], c)

    def flip(src):
        vt[src] = kv[src, c, 1].T

    def cache_copy(src, i):
        rows = pl.ds(pl.multiple_of(src * ROWS, ROWS), ROWS)
        return (pltpu.make_async_copy(kv.at[src, x, 0], kc_ref.at[rows, :], cache_sem.at[i, 0]),
                pltpu.make_async_copy(kv.at[src, x, 1], vc_ref.at[rows, :], cache_sem.at[i, 1]))

    for cp in cache_copy(me, 0):
        cp.start()
    flip(me)
    to_partner.wait_recv()
    for cp in cache_copy(partner, 1):
        cp.start()
    flip(partner)
    q_copy.wait_recv()

    m_s[...] = jnp.full_like(m_s, NEG)
    l_s[...] = jnp.zeros_like(l_s)
    acc[...] = jnp.zeros_like(acc)

    tri = lax.broadcasted_iota(jnp.int32, (QB, QB), 0) <= lax.broadcasted_iota(jnp.int32, (QB, QB), 1)
    real = lax.broadcasted_iota(jnp.int32, (QB, QB), 0) >= pad
    bias[0] = jnp.where(tri, 0.0, NEG)
    bias[1] = jnp.where(real, 0.0, NEG)
    bias[2] = jnp.where(tri & real, 0.0, NEG)

    def flash(n, item_fn, biased):
        flash_run(n, item_fn, c, biased, q_att, kv, vt, acc, m_s, l_s, s_buf, p_buf, top_s, decay_s, bias)

    def local_masked(i):
        tb = jnp.where(i < 4, i, i - 3)
        kb = jnp.where(i < 4, i, 0)
        b = jnp.where(i < 4, jnp.where((i == 0) & (x == 0), 2, 0), 1)
        return tb, 2 * x + kb // 2, lax.rem(kb, 2), b

    def local_plain(i):
        tb = jnp.where(x == 0, 2 + jnp.minimum(i, 1), 1 + jnp.minimum(i, 1) + jnp.where(i >= 3, 1, 0))
        kb = jnp.where(x == 0, 1 + i // 2, i - (tb * (tb - 1)) // 2)
        return tb, 2 * x + kb // 2, lax.rem(kb, 2), 0

    flash(4 + 3 * (1 - x), local_masked, True)
    flash(3 + 3 * x, local_plain, False)

    to_cross.wait_recv()
    forward = kv_copy(cross, 2, partner)
    forward.start()
    for cp in cache_copy(cross, 2):
        cp.start()
    flip(cross)
    kv_copy(diag, 2, partner).wait_recv()
    for cp in cache_copy(diag, 3):
        cp.start()
    flip(diag)

    def o_copies(i, tb):
        rows = pl.ds(pl.multiple_of(lax.rem(tb, 2) * QB, QB), QB)
        cols = pl.ds(pl.multiple_of(c * 768, 768), 768)
        return pltpu.make_async_remote_copy(src_ref=o_buf.at[tb], dst_ref=out_ref.at[rows, cols], send_sem=osend_sem.at[i], recv_sem=orecv_sem.at[i],
                                            device_id={"sp": partner}, device_id_type=MESH), pltpu.make_async_copy(o_buf.at[tb], out_ref.at[rows, cols], ocopy_sem.at[i])

    def remote_masked(i):
        return i, 0, 0, 1

    def remote_plain(i):
        kb = 1 + lax.rem(i, 3)
        return i // 3, kb // 2, lax.rem(kb, 2), 0

    flash(4 * x, remote_masked, True)
    flash(12 * x, remote_plain, False)

    def finish(tb):
        q_idx = lax.broadcasted_iota(jnp.int32, (1, QB), 1) + (x * 2 * ROWS + tb * QB)
        for h in range(GROUP):
            inv = jnp.where(q_idx >= pad, 1.0 / l_s[tb, h], 0.0)
            o_buf[tb, :, h * 128:(h + 1) * 128] = (acc[tb, h] * inv).T.astype(jnp.bfloat16)

    def partner_tb(i, _):
        tb = 2 * (1 - c) + i
        finish(tb)
        o_copies(i, tb)[0].start()
        return 0

    lax.fori_loop(0, 2, partner_tb, 0)

    def own_tb(i, _):
        tb = 2 * c + i
        finish(tb)
        o_copies(i, tb)[1].start()
        return 0

    lax.fori_loop(0, 2, own_tb, 0)

    to_cross.wait_send()
    to_partner.wait_send()
    forward.wait_send()
    q_copy.wait_send()
    for i, src in enumerate((me, partner, cross, diag)):
        for cp in cache_copy(src, i):
            cp.wait()
    for i in range(2):
        o_copies(i, 2 * (1 - c) + i)[0].wait_send()
        o_copies(i, 2 * c + i)[1].wait()
    for i in range(2):
        rows = pl.ds(i * QB, QB)
        cols = pl.ds(pl.multiple_of((1 - c) * 768, 768), 768)
        pltpu.make_async_remote_copy(src_ref=o_buf.at[i], dst_ref=out_ref.at[rows, cols], send_sem=osend_sem.at[i], recv_sem=orecv_sem.at[i],
                                     device_id={"sp": partner}, device_id_type=MESH).wait_recv()


def attn_call(pad, x, cos, sin, gain, w_query, w_key, w_value):
    vm = pl.BlockSpec(memory_space=pltpu.VMEM)
    hbm = pl.BlockSpec(memory_space=pl.ANY)
    flops = 2 * ROWS * DIM * 2048 + 4 * 128 * 3 * 4096 * 2048
    bf = jnp.bfloat16
    return pl.pallas_call(
        attn_kernel,
        out_shape=(jax.ShapeDtypeStruct((ROWS, DIM), bf), jax.ShapeDtypeStruct((4 * ROWS, 128), bf), jax.ShapeDtypeStruct((4 * ROWS, 128), bf)),
        in_specs=[pl.BlockSpec(memory_space=pltpu.SMEM)] + [vm] * 7,
        out_specs=(hbm, hbm, hbm),
        scratch_shapes=[
            pltpu.VMEM((ROWS, DIM), bf),
            pltpu.VMEM((2, GROUP, ROWS, 128), bf),
            pltpu.VMEM((GROUP, ROWS, 128), bf),
            pltpu.VMEM((4, 2, 2, ROWS, 128), bf),
            pltpu.VMEM((4, 128, ROWS), bf),
            pltpu.VMEM((4, GROUP, 128, QB), jnp.float32),
            pltpu.VMEM((4, GROUP, 1, QB), jnp.float32),
            pltpu.VMEM((4, GROUP, 1, QB), jnp.float32),
            pltpu.VMEM((3, 2, QB, QB), jnp.float32),
            pltpu.VMEM((3, 2, QB, QB), bf),
            pltpu.VMEM((3, 2, 8, QB), jnp.float32),
            pltpu.VMEM((3, 2, 1, QB), jnp.float32),
            pltpu.VMEM((3, QB, QB), jnp.float32),
            pltpu.VMEM((4, QB, 768), bf),
            pltpu.SemaphoreType.DMA((4,)),
            pltpu.SemaphoreType.DMA((4,)),
            pltpu.SemaphoreType.DMA((2,)),
            pltpu.SemaphoreType.DMA((2,)),
            pltpu.SemaphoreType.DMA((4, 2)),
            pltpu.SemaphoreType.DMA((2,)),
        ],
        compiler_params=pltpu.CompilerParams(vmem_limit_bytes=60 << 20, collective_id=0, has_side_effects=True),
        cost_estimate=pl.CostEstimate(flops=flops, bytes_accessed=20 << 20, transcendentals=3 * 4096 * 2048),
        name="attn_block",
    )(pad, x, cos, sin, gain.reshape(1, DIM), w_query, w_key, w_value)


def solution(mesh):
    def layer_shard(hidden, positions, attn_gain, w_query, w_key, w_value, w_out, mlp_gain, w_gate, w_up, w_down):
        inv_freq = 1.0 / (ROPE_THETA ** (jnp.arange(0, HEAD_DIM, 2, dtype=jnp.float32) / HEAD_DIM))
        angles = positions.astype(jnp.float32)[:, None] * inv_freq[None, :]
        cos, sin = jnp.cos(angles), jnp.sin(angles)
        cos = jnp.concatenate([cos, cos], axis=-1)
        sin = jnp.concatenate([-sin, sin], axis=-1)
        pad = (lax.axis_index("sp") * ROWS + ROWS - 1 - positions[ROWS - 1]).reshape(1)
        attn, k_cache, v_cache = attn_call(pad, hidden, cos, sin, attn_gain, w_query, w_key, w_value)
        hidden_out = mlp_call(attn, hidden, w_out, mlp_gain, w_gate, w_up, w_down)
        return hidden_out, k_cache.reshape(4 * ROWS, 1, 128), v_cache.reshape(4 * ROWS, 1, 128)

    row_spec = P(("dp", "sp"), None)
    cache_spec = P("dp", "sp", None)
    return jax.shard_map(layer_shard, mesh=mesh, in_specs=(row_spec, P(("dp", "sp")), P(), P(), P(), P(), P(), P(), P(), P(), P()), out_specs=(row_spec, cache_spec, cache_spec), check_vma=False)
```

```python
import functools
import itertools
import jax
import jax.numpy as jnp
import numpy as np
from jax import lax
from jax.experimental import pallas as pl
from jax.experimental.pallas import tpu as pltpu
from jax.sharding import PartitionSpec as P

ROWS = 1024
DIM = 1536
FFN = 8960
NORM_EPS = 1e-5


def mlp_kernel(fb, rt, o_ref, x_ref, wout_ref, gain_ref, wg_hbm, wu_hbm, wd_hbm, k_in, v_in, out_ref, k_out, v_out, acc, g_buf, m_buf, wg, wu, wd, c_buf, sems, c_sems):
    steps = FFN // fb

    def copies(j, slot):
        off = pl.multiple_of(j * fb, 128)
        return (
            pltpu.make_async_copy(wg_hbm.at[:, pl.ds(off, fb)], wg.at[slot], sems.at[slot, 0]),
            pltpu.make_async_copy(wu_hbm.at[:, pl.ds(off, fb)], wu.at[slot], sems.at[slot, 1]),
            pltpu.make_async_copy(wd_hbm.at[pl.ds(off, fb), :], wd.at[slot], sems.at[slot, 2]),
        )

    for c in copies(0, 0):
        c.start()

    cache = ((k_in, k_out), (v_in, v_out))
    for i in range(2):
        pltpu.make_async_copy(cache[i][0], c_buf.at[i], c_sems.at[0, i]).start()
    gain = gain_ref[...].reshape(1, DIM).astype(jnp.float32)

    def proj(r, _):
        rows = pl.ds(pl.multiple_of(r * 256, 256), 256)
        y = x_ref[rows, :].astype(jnp.float32) + jnp.dot(o_ref[rows, :], wout_ref[...], preferred_element_type=jnp.float32)
        y = y.astype(jnp.bfloat16).astype(jnp.float32)
        acc[rows, :] = y
        ms = jnp.mean(y * y, axis=-1, keepdims=True)
        g_buf[rows, :] = (y * lax.rsqrt(ms + NORM_EPS) * gain).astype(jnp.bfloat16)
        return 0

    lax.fori_loop(0, ROWS // 256, proj, 0)
    for i in range(2):
        pltpu.make_async_copy(cache[i][0], c_buf.at[i], c_sems.at[0, i]).wait()
        pltpu.make_async_copy(c_buf.at[i], cache[i][1], c_sems.at[1, i]).start()

    def step(j, _):
        slot = lax.rem(j, 2)
        for c in copies(j, slot):
            c.wait()

        @pl.when(j + 1 < steps)
        def _():
            for c in copies(j + 1, 1 - slot):
                c.start()

        def tile(r, _):
            rows = pl.ds(pl.multiple_of(r * rt, rt), rt)
            for c0 in range(0, fb, 256):
                cols = pl.ds(c0, 256)
                gate = jnp.dot(g_buf[rows, :], wg[slot, :, cols], preferred_element_type=jnp.float32)
                up = jnp.dot(g_buf[rows, :], wu[slot, :, cols], preferred_element_type=jnp.float32)
                m_buf[:, cols] = (gate / (1.0 + jnp.exp(-gate)) * up).astype(jnp.bfloat16)
            acc[rows, :] += jnp.dot(m_buf[...], wd[slot], preferred_element_type=jnp.float32)
            return 0

        lax.fori_loop(0, ROWS // rt, tile, 0)
        return 0

    lax.fori_loop(0, steps, step, 0)

    def fin(r, _):
        rows = pl.ds(pl.multiple_of(r * 128, 128), 128)
        out_ref[rows, :] = acc[rows, :].astype(jnp.bfloat16)
        return 0

    lax.fori_loop(0, ROWS // 128, fin, 0)
    for i in range(2):
        pltpu.make_async_copy(c_buf.at[i], cache[i][1], c_sems.at[1, i]).wait()


def mlp_call(o, x, w_out, gain, wg, wu, wd, k_all, v_all, fb=1280, rt=512):
    vm = pl.BlockSpec(memory_space=pltpu.VMEM)
    hbm = pl.BlockSpec(memory_space=pl.ANY)
    flops = 2 * ROWS * DIM * (DIM + 3 * FFN)
    return pl.pallas_call(
        functools.partial(mlp_kernel, fb, rt),
        out_shape=(jax.ShapeDtypeStruct((ROWS, DIM), jnp.bfloat16),) + (jax.ShapeDtypeStruct(k_all.shape, jnp.bfloat16),) * 2,
        in_specs=[vm] * 4 + [hbm] * 5,
        out_specs=(vm, hbm, hbm),
        scratch_shapes=[
            pltpu.VMEM((ROWS, DIM), jnp.float32),
            pltpu.VMEM((ROWS, DIM), jnp.bfloat16),
            pltpu.VMEM((rt, fb), jnp.bfloat16),
            pltpu.VMEM((2, DIM, fb), jnp.bfloat16),
            pltpu.VMEM((2, DIM, fb), jnp.bfloat16),
            pltpu.VMEM((2, fb, DIM), jnp.bfloat16),
            pltpu.VMEM((2, 4 * ROWS, 128), jnp.bfloat16),
            pltpu.SemaphoreType.DMA((2, 3)),
            pltpu.SemaphoreType.DMA((2, 2)),
        ],
        compiler_params=pltpu.CompilerParams(vmem_limit_bytes=60 << 20),
        cost_estimate=pl.CostEstimate(flops=flops, bytes_accessed=3 * DIM * FFN * 2, transcendentals=ROWS * FFN),
        name="mlp_block",
    )(o, x, w_out, gain, wg, wu, wd, k_all, v_all)


HEAD_DIM = 128
ROPE_THETA = 500000
SCALE_LOG2E = 1.4426950408889634 * HEAD_DIM ** -0.5
NEG = -2.0e38
QB = 512
KC = 256
PC = 64
FOREIGN = 3
TRI, REAL, BOTH, NONE, FREE = range(5)
MESH = pl.DeviceIdType.MESH


def schedules():
    def code(st, kb, b):
        return (st * 8 + kb) * 8 + b

    a_masked = [code(3 * tb + p, tb, BOTH if tb == 0 else TRI) for tb in range(4) for p in range(3)]
    a_masked += [code(3 * tb + p, 0, REAL) for tb in range(1, 4) for p in range(3)]
    a_plain = [code(3 * tb + p, kb, FREE) for tb in range(2, 4) for kb in range(1, tb) for p in range(3)]
    a_masked.append(a_plain.pop(0))
    a_masked += [a_plain[-1] - FREE + NONE] * 2
    pairs = {tb: 2 if tb < FOREIGN else 3 for tb in range(4)}
    b_masked = [code(3 * tb + p, 4 + tb, TRI) for tb in range(4) for p in range(pairs[tb])]
    b_plain = [code(3 * tb + p, 4 + kb, FREE) for tb in range(1, 4) for kb in range(tb) for p in range(pairs[tb])]
    while len(b_masked) % 4:
        b_masked.append(b_plain.pop(0))
    b_real = [code(3 * tb + p, 0, REAL) for tb in range(4) for p in range(pairs[tb])]
    b_far = [code(3 * tb + p, kb, FREE) for tb in range(4) for kb in range(1, 4) for p in range(pairs[tb])]
    while len(b_real) % 4:
        b_real.append(b_far.pop(0))
    foreign = []
    for tb in (2, 0, 1):
        run = [code(12 + tb, 0, REAL)] + [code(12 + tb, kb, FREE) for kb in range(1, 4 + tb)] + [code(12 + tb, 4 + tb, TRI)]
        foreign.append(run + [code(12 + tb, 4 + tb, NONE)] * (len(run) % 2))
    return a_masked, a_plain, b_masked, b_plain, b_real, b_far, foreign


def lookup(i, values):
    if len(values) == 1:
        return values[0]
    if all(v == values[0] for v in values):
        return values[0]
    half = len(values) // 2
    return jnp.where(i < half, lookup(i, values[:half]), lookup(i - half, values[half:]))


def flash_run(n, unroll, code_fn, biased, me_c, q_buf, kv, vt, acc, m_s, l_s, s_buf, p_buf, top_s, decay_s, bias):
    def fields(i):
        code = code_fn(i)
        return code // 64, lax.rem(code // 8, 8), lax.rem(code, 8)

    def scores(i, slot):
        st, kb, b = fields(i)
        tb = st // 3
        own = st < 12
        place = jnp.where(own, jnp.where(tb // 2 == me_c, me_c, 2), 3)
        entry = jnp.where(own, lax.rem(tb, 2) * 3 + lax.rem(st, 3), st - 12)
        k_off = pl.multiple_of(lax.rem(kb, 2) * QB, QB)
        for u in range(2):
            q_blk = q_buf[place, entry, u]
            top = jnp.full((8, QB), NEG, jnp.float32)
            for k0 in range(0, QB, KC):
                k_blk = kv[kb // 2, me_c, 0, pl.ds(k_off + k0, KC), :]
                s = lax.dot_general(k_blk, q_blk, (((1,), (1,)), ((), ())), preferred_element_type=jnp.float32)
                if biased:
                    s = s + bias[b, k0:k0 + KC, :]
                s_buf[slot, u, k0:k0 + KC, :] = s
                top = jnp.maximum(top, jnp.max(s.reshape(KC // 8, 8, QB), axis=0))
                yield
            top_s[slot, u] = top

    def weights(i, slot):
        st = fields(i)[0]
        for u in range(2):
            m_prev = m_s[st, u]
            m_new = jnp.maximum(m_prev, jnp.max(top_s[slot, u], axis=0, keepdims=True))
            m8 = jnp.broadcast_to(m_new, (8, QB))
            total = jnp.zeros((8, QB), jnp.float32)
            for k0 in range(0, QB, PC):
                s = s_buf[slot, u, k0:k0 + PC, :].reshape(PC // 8, 8, QB)
                p = jnp.exp2((s - m8[None]) * SCALE_LOG2E)
                total = total + jnp.sum(p, axis=0)
                p_buf[slot, u, k0:k0 + PC, :] = p.reshape(PC, QB).astype(jnp.bfloat16)
                if (k0 + PC) % KC == 0:
                    yield
            decay = jnp.exp2((m_prev - m_new) * SCALE_LOG2E)
            decay_s[slot, u] = decay
            l_s[st, u] = l_s[st, u] * decay + jnp.sum(total, axis=0, keepdims=True)
            m_s[st, u] = m_new

    def values(i, slot):
        st, kb, _ = fields(i)
        k_off = pl.multiple_of(lax.rem(kb, 2) * QB, QB)
        for u in range(2):
            pv = jnp.dot(vt[kb // 2, :, pl.ds(k_off, QB)], p_buf[slot, u], preferred_element_type=jnp.float32)
            acc[st, u] = acc[st, u] * decay_s[slot, u] + pv
            for _ in range(QB // KC):
                yield

    def together(*parts):
        for _ in itertools.zip_longest(*parts):
            pass

    @pl.when(n > 0)
    def _():
        p_buf[1] = jnp.zeros_like(p_buf[1])
        decay_s[1] = jnp.ones_like(decay_s[1])
        together(scores(0, 0))

        def step(j, _):
            i = j * unroll
            for k in range(unroll):
                slot = k % 2
                prev = jnp.maximum(i - 1, 0) if k == 0 else i + k - 1
                nxt = jnp.minimum(i + k + 1, n - 1) if k == unroll - 1 else i + k + 1
                together(weights(i + k, slot), scores(nxt, 1 - slot), values(prev, 1 - slot))
            return 0

        lax.fori_loop(0, n // unroll, step, 0)
        together(values(n - 1, 1))


def attn_kernel(pos_ref, freq_ref, x_ref, gain_ref, wq_ref, wk_ref, wv_ref, out_ref, kc_ref, vc_ref,
                cos_s, sin_s, h_buf, q_buf, kv, vt, acc, m_s, l_s, s_buf, p_buf, top_s, decay_s, bias, o_buf,
                send_sem, recv_sem, qsend_sem, qrecv_sem, osend_sem, orecv_sem, cache_sem, ocopy_sem):
    me = lax.axis_index("sp")
    x = me // 2
    c = lax.rem(me, 2)
    partner = 2 * x + (1 - c)
    cross = 2 * (1 - x) + c
    diag = 2 * (1 - x) + (1 - c)
    pad = me * ROWS + (ROWS - 1) - pos_ref[ROWS - 1]
    a_masked, a_plain, b_masked, b_plain, b_real, b_far, foreign = schedules()

    barrier = pltpu.get_barrier_semaphore()
    for peer in (partner, cross, diag):
        pl.semaphore_signal(barrier, inc=1, device_id={"sp": peer}, device_id_type=MESH)

    gain = gain_ref[...].reshape(1, DIM).astype(jnp.float32)
    lane = lax.broadcasted_iota(jnp.int32, (256, 128), 1)

    def angle_rows(r):
        rows = pl.ds(r * 256, 256)
        row = lax.broadcasted_iota(jnp.int32, (256, 128), 0) + (me * ROWS + r * 256 - pad)
        ang = jnp.maximum(row, -1).astype(jnp.float32) * freq_ref[...]
        turns = jnp.floor(ang * 0.6366197723675814 + 0.5)
        red = ((ang - turns * 1.5703125) - turns * 4.837512969970703125e-4) - turns * 7.54978995489188216e-8
        sq = red * red
        sin_p = ((-1.9515295891e-4 * sq + 8.3321608736e-3) * sq - 1.6666654611e-1) * sq * red + red
        cos_p = ((2.443315711809948e-5 * sq - 1.388731625493765e-3) * sq + 4.166664568298827e-2) * sq * sq - 0.5 * sq + 1.0
        quad = (turns.astype(jnp.int32) + jnp.where(lane < 64, 0, 3)) & 3
        val = jnp.where((quad & 1) == 0, cos_p, sin_p)
        val = jnp.where((quad == 1) | (quad == 2), -val, val)
        swapped = pltpu.roll(val, 64, 1)
        cos_s[rows, :] = jnp.where(lane < 64, val, swapped)
        sin_s[rows, :] = jnp.where(lane < 64, -swapped, val)

    def rope(t, rows):
        return (t * cos_s[rows, :] + pltpu.roll(t, 64, 1) * sin_s[rows, :]).astype(jnp.bfloat16)

    for r in range(ROWS // 256):
        rows = pl.ds(r * 256, 256)
        angle_rows(r)
        xf = x_ref[rows, :].astype(jnp.float32)
        ms = jnp.mean(xf * xf, axis=-1, keepdims=True)
        h = (xf * lax.rsqrt(ms + NORM_EPS) * gain).astype(jnp.bfloat16)
        h_buf[rows, :] = h
        k = jnp.dot(h, wk_ref[...], preferred_element_type=jnp.float32)
        v = jnp.dot(h, wv_ref[...], preferred_element_type=jnp.float32).astype(jnp.bfloat16)
        for g in range(2):
            kv[me, g, 0, rows, :] = rope(k[:, g * 128:(g + 1) * 128], rows)
            kv[me, g, 1, rows, :] = v[:, g * 128:(g + 1) * 128]

    pl.semaphore_wait(barrier, 3)

    def kv_copy(src, i, peer):
        return pltpu.make_async_remote_copy(src_ref=kv.at[src], dst_ref=kv.at[src], send_sem=send_sem.at[i], recv_sem=recv_sem.at[i],
                                            device_id={"sp": peer}, device_id_type=MESH)

    to_cross = kv_copy(me, 0, cross)
    to_cross.start()
    to_partner = kv_copy(me, 1, partner)
    to_partner.start()

    def q_rows(t):
        def body(r, _):
            rows = pl.ds(pl.multiple_of(t * QB + r * 256, 256), 256)
            inner = pl.ds(pl.multiple_of(r * 256, 256), 256)
            q = jnp.dot(h_buf[rows, :], wq_ref[...], preferred_element_type=jnp.float32)
            for h in range(12):
                q_buf[h // 6, t * 3 + (h % 6) // 2, h % 2, inner, :] = rope(q[:, h * 128:(h + 1) * 128], rows)
            return 0

        lax.fori_loop(0, 2, body, 0)

    def foreign_q(t, g, peer):
        ft = 2 * c + t
        return pltpu.make_async_remote_copy(src_ref=q_buf.at[g, t * 3 + 2], dst_ref=q_buf.at[3, ft], send_sem=qsend_sem.at[t, g],
                                            recv_sem=qrecv_sem.at[ft], device_id={"sp": peer}, device_id_type=MESH)

    def send_foreign(t):
        @pl.when((x == 1) & (2 * c + t < FOREIGN))
        def _():
            foreign_q(t, c, cross).start()
            foreign_q(t, 1 - c, diag).start()

    q_rows(0)
    send_foreign(0)
    q_rows(1)
    send_foreign(1)
    q_copy = pltpu.make_async_remote_copy(src_ref=q_buf.at[1 - c], dst_ref=q_buf.at[2], send_sem=send_sem.at[3], recv_sem=recv_sem.at[3],
                                          device_id={"sp": partner}, device_id_type=MESH)
    q_copy.start()

    def flip(src):
        vt[src] = kv[src, c, 1].T

    def cache_copy(src, i):
        rows = pl.ds(pl.multiple_of(src * ROWS, ROWS), ROWS)
        return (pltpu.make_async_copy(kv.at[src, x, 0], kc_ref.at[rows, :], cache_sem.at[i, 0]),
                pltpu.make_async_copy(kv.at[src, x, 1], vc_ref.at[rows, :], cache_sem.at[i, 1]))

    for cp in cache_copy(me, 0):
        cp.start()
    flip(me)
    tri = lax.broadcasted_iota(jnp.int32, (QB, QB), 0) <= lax.broadcasted_iota(jnp.int32, (QB, QB), 1)
    real = lax.broadcasted_iota(jnp.int32, (QB, QB), 0) >= pad
    bias[TRI] = jnp.where(tri, 0.0, NEG)
    bias[REAL] = jnp.where(real, 0.0, NEG)
    bias[BOTH] = jnp.where(tri & real, 0.0, NEG)
    bias[NONE] = jnp.full((QB, QB), NEG, jnp.float32)
    bias[FREE] = jnp.zeros((QB, QB), jnp.float32)
    m_s[...] = jnp.full_like(m_s, NEG)
    l_s[...] = jnp.zeros_like(l_s)
    acc[...] = jnp.zeros_like(acc)
    to_partner.wait_recv()
    for cp in cache_copy(partner, 1):
        cp.start()
    flip(partner)
    q_copy.wait_recv()

    def flash(n, unroll, code_fn, biased):
        flash_run(n, unroll, code_fn, biased, c, q_buf, kv, vt, acc, m_s, l_s, s_buf, p_buf, top_s, decay_s, bias)

    def by_chip(a, b):
        return jnp.where(x == 0, a, b)

    flash(by_chip(len(a_masked), len(b_masked)), 4, lambda i: by_chip(lookup(i, a_masked), lookup(i, b_masked)), True)
    flash(by_chip(len(a_plain), len(b_plain)), 4, lambda i: by_chip(lookup(i, a_plain), lookup(i, b_plain)), False)

    def o_place(t, col):
        return out_ref.at[pl.ds(pl.multiple_of(t * QB, QB), QB), pl.ds(pl.multiple_of(col * 256, 256), 256)]

    def o_send(st, t, col, peer):
        return pltpu.make_async_remote_copy(src_ref=o_buf.at[st], dst_ref=o_place(t, col), send_sem=osend_sem.at[st], recv_sem=orecv_sem.at[t, col],
                                            device_id={"sp": peer}, device_id_type=MESH)

    def o_keep(st, t, col):
        return pltpu.make_async_copy(o_buf.at[st], o_place(t, col), ocopy_sem.at[t, lax.rem(col, 3)])

    def finish(st):
        q_idx = lax.broadcasted_iota(jnp.int32, (1, QB), 1) + (x * 2 * ROWS + (st // 3) * QB)
        for u in range(2):
            inv = jnp.where(q_idx >= pad, 1.0 / l_s[st, u], 0.0)
            o_buf[st, :, u * 128:(u + 1) * 128] = (acc[st, u] * inv).T.astype(jnp.bfloat16)

    def here(tb, pair):
        return (x == 0) | (pair < 2) | (tb >= FOREIGN)

    def finish_own(j, _):
        half = jnp.where(j < 6, 1 - c, c)
        t = lax.rem(j, 6) // 3
        pair = lax.rem(j, 3)
        tb = 2 * half + t
        st = 3 * tb + pair

        @pl.when(here(tb, pair))
        def _():
            finish(st)

            @pl.when(j < 6)
            def _():
                o_send(st, t, 3 * c + pair, partner).start()

            @pl.when(j >= 6)
            def _():
                o_keep(st, t, 3 * c + pair).start()

        return 0

    @pl.when(x == 0)
    def _():
        lax.fori_loop(0, 12, finish_own, 0)

    to_cross.wait_recv()
    forward = kv_copy(cross, 2, partner)
    forward.start()
    for cp in cache_copy(cross, 2):
        cp.start()
    flip(cross)
    kv_copy(diag, 2, partner).wait_recv()
    for cp in cache_copy(diag, 3):
        cp.start()
    flip(diag)

    f_len = [len(run) for run in foreign]
    f_all = sum(foreign, [])
    f_tb = [2, 0, 1]

    def far_round(j, _):
        ft = lookup(j, f_tb)

        @pl.when(x == 0)
        def _():
            pltpu.make_async_remote_copy(src_ref=q_buf.at[0, 2], dst_ref=q_buf.at[3, ft], send_sem=qsend_sem.at[0, 0],
                                         recv_sem=qrecv_sem.at[ft], device_id={"sp": cross}, device_id_type=MESH).wait_recv()

        start = lookup(j, [sum(f_len[:k]) for k in range(FOREIGN)])
        flash(by_chip(lookup(j, f_len), len(b_real)), 2, lambda i: by_chip(lookup(i + start, f_all), lookup(i, b_real)), True)

        @pl.when(x == 0)
        def _():
            finish(12 + ft)
            o_send(12 + ft, lax.rem(ft, 2), 3 * c + 2, 2 + ft // 2).start()

        return 0

    lax.fori_loop(0, by_chip(FOREIGN, 1), far_round, 0)
    flash(by_chip(0, len(b_far)), 4, lambda i: lookup(i, b_far), False)

    @pl.when(x == 1)
    def _():
        lax.fori_loop(0, 12, finish_own, 0)

    to_cross.wait_send()
    to_partner.wait_send()
    forward.wait_send()
    q_copy.wait_send()
    for i, src in enumerate((me, partner, cross, diag)):
        for cp in cache_copy(src, i):
            cp.wait()
    for t in range(2):
        @pl.when((x == 1) & (2 * c + t < FOREIGN))
        def _():
            foreign_q(t, c, cross).wait_send()
            foreign_q(t, 1 - c, diag).wait_send()

        for pair in range(3):
            mine = here(2 * c + t, pair)
            theirs = here(2 * (1 - c) + t, pair)

            @pl.when(mine)
            def _():
                o_keep(0, t, 3 * c + pair).wait()

            @pl.when(jnp.logical_not(mine))
            def _():
                o_send(0, t, 3 * c + pair, cross).wait_recv()

            o_send(0, t, 3 * (1 - c) + pair, partner).wait_recv()

            @pl.when(theirs)
            def _():
                o_send(3 * (2 * (1 - c) + t) + pair, t, 3 * c + pair, partner).wait_send()

    @pl.when(x == 0)
    def _():
        for ft in range(FOREIGN):
            o_send(12 + ft, ft % 2, 3 * c + 2, 2 + ft // 2).wait_send()


def attn_call(positions, freq, x, gain, w_query, w_key, w_value):
    vm = pl.BlockSpec(memory_space=pltpu.VMEM)
    hbm = pl.BlockSpec(memory_space=pl.ANY)
    flops = 2 * ROWS * DIM * 2048 + 4 * 128 * 3 * 4096 * 2048
    bf, f32 = jnp.bfloat16, jnp.float32
    dma = pltpu.SemaphoreType.DMA
    return pl.pallas_call(
        attn_kernel,
        out_shape=(jax.ShapeDtypeStruct((ROWS, DIM), bf), jax.ShapeDtypeStruct((4 * ROWS, 128), bf), jax.ShapeDtypeStruct((4 * ROWS, 128), bf)),
        in_specs=[pl.BlockSpec(memory_space=pltpu.SMEM)] + [vm] * 6,
        out_specs=(hbm, hbm, hbm),
        scratch_shapes=[
            pltpu.VMEM((ROWS, 128), f32),
            pltpu.VMEM((ROWS, 128), f32),
            pltpu.VMEM((ROWS, DIM), bf),
            pltpu.VMEM((4, 6, 2, QB, 128), bf),
            pltpu.VMEM((4, 2, 2, ROWS, 128), bf),
            pltpu.VMEM((4, 128, ROWS), bf),
            pltpu.VMEM((12 + FOREIGN, 2, 128, QB), f32),
            pltpu.VMEM((12 + FOREIGN, 2, 1, QB), f32),
            pltpu.VMEM((12 + FOREIGN, 2, 1, QB), f32),
            pltpu.VMEM((2, 2, QB, QB), f32),
            pltpu.VMEM((2, 2, QB, QB), bf),
            pltpu.VMEM((2, 2, 8, QB), f32),
            pltpu.VMEM((2, 2, 1, QB), f32),
            pltpu.VMEM((5, QB, QB), f32),
            pltpu.VMEM((12 + FOREIGN, QB, 256), bf),
            dma((4,)), dma((4,)), dma((2, 2)), dma((FOREIGN,)), dma((12 + FOREIGN,)), dma((2, 6)), dma((4, 2)), dma((2, 3)),
        ],
        compiler_params=pltpu.CompilerParams(vmem_limit_bytes=62 << 20, collective_id=0, has_side_effects=True),
        cost_estimate=pl.CostEstimate(flops=flops, bytes_accessed=20 << 20, transcendentals=3 * 4096 * 2048),
        name="attn_block",
    )(positions, freq, x, gain, w_query, w_key, w_value)


def solution(mesh):
    freq = 1.0 / (ROPE_THETA ** (np.arange(0, HEAD_DIM, 2, dtype=np.float64) / HEAD_DIM))
    freq = np.concatenate([freq, freq]).astype(np.float32).reshape(1, HEAD_DIM)

    def layer_shard(hidden, positions, attn_gain, w_query, w_key, w_value, w_out, mlp_gain, w_gate, w_up, w_down):
        attn, k_all, v_all = attn_call(positions, jnp.asarray(freq), hidden, attn_gain, w_query, w_key, w_value)
        hidden_out, k_cache, v_cache = mlp_call(attn, hidden, w_out, mlp_gain, w_gate, w_up, w_down, k_all, v_all)
        return hidden_out, k_cache.reshape(4 * ROWS, 1, HEAD_DIM), v_cache.reshape(4 * ROWS, 1, HEAD_DIM)

    row_spec = P(("dp", "sp"), None)
    cache_spec = P("dp", "sp", None)
    return jax.shard_map(layer_shard, mesh=mesh, in_specs=(row_spec, P(("dp", "sp")), P(), P(), P(), P(), P(), P(), P(), P(), P()), out_specs=(row_spec, cache_spec, cache_spec), check_vma=False)
```

```python
import functools
import itertools
import jax
import jax.numpy as jnp
import numpy as np
from jax import lax
from jax.experimental import pallas as pl
from jax.experimental.pallas import tpu as pltpu
from jax.sharding import PartitionSpec as P

ROWS = 1024
DIM = 1536
FFN = 8960
NORM_EPS = 1e-5


def mlp_kernel(fb, rt, o_ref, x_ref, wout_ref, gain_ref, wg_hbm, wu_hbm, wd_hbm, k_in, v_in, out_ref, k_out, v_out, acc, g_buf, m_buf, wg, wu, wd, c_buf, sems, c_sems):
    steps = FFN // fb

    def copies(j, slot):
        off = pl.multiple_of(j * fb, 128)
        return (
            pltpu.make_async_copy(wg_hbm.at[:, pl.ds(off, fb)], wg.at[slot], sems.at[slot, 0]),
            pltpu.make_async_copy(wu_hbm.at[:, pl.ds(off, fb)], wu.at[slot], sems.at[slot, 1]),
            pltpu.make_async_copy(wd_hbm.at[pl.ds(off, fb), :], wd.at[slot], sems.at[slot, 2]),
        )

    for c in copies(0, 0):
        c.start()

    cache = ((k_in, k_out), (v_in, v_out))
    for i in range(2):
        pltpu.make_async_copy(cache[i][0], c_buf.at[i], c_sems.at[0, i]).start()
    gain = gain_ref[...].reshape(1, DIM).astype(jnp.float32)

    def proj(r, _):
        rows = pl.ds(pl.multiple_of(r * 256, 256), 256)
        y = x_ref[rows, :].astype(jnp.float32) + jnp.dot(o_ref[rows, :], wout_ref[...], preferred_element_type=jnp.float32)
        y = y.astype(jnp.bfloat16).astype(jnp.float32)
        acc[rows, :] = y
        ms = jnp.mean(y * y, axis=-1, keepdims=True)
        g_buf[rows, :] = (y * lax.rsqrt(ms + NORM_EPS) * gain).astype(jnp.bfloat16)
        return 0

    lax.fori_loop(0, ROWS // 256, proj, 0)
    for i in range(2):
        pltpu.make_async_copy(cache[i][0], c_buf.at[i], c_sems.at[0, i]).wait()
        pltpu.make_async_copy(c_buf.at[i], cache[i][1], c_sems.at[1, i]).start()

    def step(j, _):
        slot = lax.rem(j, 2)
        for c in copies(j, slot):
            c.wait()

        @pl.when(j + 1 < steps)
        def _():
            for c in copies(j + 1, 1 - slot):
                c.start()

        def tile(r, _):
            rows = pl.ds(pl.multiple_of(r * rt, rt), rt)
            for c0 in range(0, fb, 256):
                cols = pl.ds(c0, 256)
                gate = jnp.dot(g_buf[rows, :], wg[slot, :, cols], preferred_element_type=jnp.float32)
                up = jnp.dot(g_buf[rows, :], wu[slot, :, cols], preferred_element_type=jnp.float32)
                m_buf[:, cols] = (gate / (1.0 + jnp.exp(-gate)) * up).astype(jnp.bfloat16)
            acc[rows, :] += jnp.dot(m_buf[...], wd[slot], preferred_element_type=jnp.float32)
            return 0

        lax.fori_loop(0, ROWS // rt, tile, 0)
        return 0

    lax.fori_loop(0, steps, step, 0)

    def fin(r, _):
        rows = pl.ds(pl.multiple_of(r * 128, 128), 128)
        out_ref[rows, :] = acc[rows, :].astype(jnp.bfloat16)
        return 0

    lax.fori_loop(0, ROWS // 128, fin, 0)
    for i in range(2):
        pltpu.make_async_copy(c_buf.at[i], cache[i][1], c_sems.at[1, i]).wait()


def mlp_call(o, x, w_out, gain, wg, wu, wd, k_all, v_all, fb=1280, rt=512):
    vm = pl.BlockSpec(memory_space=pltpu.VMEM)
    hbm = pl.BlockSpec(memory_space=pl.ANY)
    flops = 2 * ROWS * DIM * (DIM + 3 * FFN)
    return pl.pallas_call(
        functools.partial(mlp_kernel, fb, rt),
        out_shape=(jax.ShapeDtypeStruct((ROWS, DIM), jnp.bfloat16),) + (jax.ShapeDtypeStruct(k_all.shape, jnp.bfloat16),) * 2,
        in_specs=[vm] * 4 + [hbm] * 5,
        out_specs=(vm, hbm, hbm),
        scratch_shapes=[
            pltpu.VMEM((ROWS, DIM), jnp.float32),
            pltpu.VMEM((ROWS, DIM), jnp.bfloat16),
            pltpu.VMEM((rt, fb), jnp.bfloat16),
            pltpu.VMEM((2, DIM, fb), jnp.bfloat16),
            pltpu.VMEM((2, DIM, fb), jnp.bfloat16),
            pltpu.VMEM((2, fb, DIM), jnp.bfloat16),
            pltpu.VMEM((2, 4 * ROWS, 128), jnp.bfloat16),
            pltpu.SemaphoreType.DMA((2, 3)),
            pltpu.SemaphoreType.DMA((2, 2)),
        ],
        compiler_params=pltpu.CompilerParams(vmem_limit_bytes=60 << 20),
        cost_estimate=pl.CostEstimate(flops=flops, bytes_accessed=3 * DIM * FFN * 2, transcendentals=ROWS * FFN),
        name="mlp_block",
    )(o, x, w_out, gain, wg, wu, wd, k_all, v_all)


HEAD_DIM = 128
ROPE_THETA = 500000
SCALE_LOG2E = 1.4426950408889634 * HEAD_DIM ** -0.5
NEG = -2.0e38
QB = 512
KC = 512
PC = 64
FOREIGN = 3
TRI, REAL, BOTH, NONE, FREE = range(5)
MESH = pl.DeviceIdType.MESH


def schedules():
    def code(st, kb, b):
        return (st * 8 + kb) * 8 + b

    a_masked = [code(3 * tb + p, tb, BOTH if tb == 0 else TRI) for tb in range(4) for p in range(3)]
    a_masked += [code(3 * tb + p, 0, REAL) for tb in range(1, 4) for p in range(3)]
    a_plain = [code(3 * tb + p, kb, FREE) for tb in range(2, 4) for kb in range(1, tb) for p in range(3)]
    a_masked.append(a_plain.pop(0))
    a_masked += [a_plain[-1] - FREE + NONE] * 2
    pairs = {tb: 2 if tb < FOREIGN else 3 for tb in range(4)}
    b_masked = [code(3 * tb + p, 4 + tb, TRI) for tb in range(4) for p in range(pairs[tb])]
    b_plain = [code(3 * tb + p, 4 + kb, FREE) for tb in range(1, 4) for kb in range(tb) for p in range(pairs[tb])]
    while len(b_masked) % 4:
        b_masked.append(b_plain.pop(0))
    b_real = [code(3 * tb + p, 0, REAL) for tb in range(4) for p in range(pairs[tb])]
    b_far = [code(3 * tb + p, kb, FREE) for tb in range(4) for kb in range(1, 4) for p in range(pairs[tb])]
    while len(b_real) % 4:
        b_real.append(b_far.pop(0))
    runs = {}
    for tb in range(FOREIGN):
        runs[tb] = [code(12 + tb, 0, REAL)] + [code(12 + tb, kb, FREE) for kb in range(1, 4 + tb)] + [code(12 + tb, 4 + tb, TRI)]
    foreign = [runs[2] + runs[0][:1], runs[0][1:], runs[1] + [code(13, 5, NONE)] * 2]
    return a_masked, a_plain, b_masked, b_plain, b_real, b_far, foreign


def packed(runs):
    words = ([], [], [], [])
    for run in runs:
        for j in range(0, len(run), 4):
            ahead = [run[min(j + k, len(run) - 1)] for k in range(6)]
            for w in range(3):
                words[w].append(ahead[2 * w] + 1024 * ahead[2 * w + 1])
            words[3].append(run[max(j - 1, 0)])
    return words


def lookup(i, values):
    if len(values) == 1:
        return values[0]
    if all(v == values[0] for v in values):
        return values[0]
    half = len(values) // 2
    return jnp.where(i < half, lookup(i, values[:half]), lookup(i - half, values[half:]))


def flash_run(groups, words_fn, biased, me_c, q_buf, kv, vt, acc, m_s, l_s, s_buf, p_buf, top_s, decay_s, bias):
    def fields(code):
        return lax.div(code, 64), lax.rem(lax.div(code, 8), 8), lax.rem(code, 8)

    def split(word):
        return [lax.rem(word, 1024), lax.div(word, 1024)]

    def scores(code, slot):
        st, kb, b = fields(code)
        tb = lax.div(st, 3)
        own = st < 12
        place = jnp.where(own, jnp.where(lax.div(tb, 2) == me_c, me_c, 2), 3)
        entry = jnp.where(own, lax.rem(tb, 2) * 3 + lax.rem(st, 3), st - 12)
        k_off = pl.multiple_of(lax.rem(kb, 2) * QB, QB)
        for u in range(2):
            q_blk = q_buf[place, entry, u]
            top = jnp.full((8, QB), NEG, jnp.float32)
            for k0 in range(0, QB, KC):
                k_blk = kv[lax.div(kb, 2), me_c, 0, pl.ds(k_off + k0, KC), :]
                s = lax.dot_general(k_blk, q_blk, (((1,), (1,)), ((), ())), preferred_element_type=jnp.float32)
                if biased:
                    s = s + bias[b, k0:k0 + KC, :]
                s_buf[slot % 4, u, k0:k0 + KC, :] = s
                top = jnp.maximum(top, jnp.max(s.reshape(KC // 8, 8, QB), axis=0))
                yield
            top_s[slot % 4, u] = top

    def weights(code, slot):
        st = fields(code)[0]
        for u in range(2):
            m_prev = m_s[st, u]
            m_new = jnp.maximum(m_prev, jnp.max(top_s[slot % 4, u], axis=0, keepdims=True))
            m8 = jnp.broadcast_to(m_new, (8, QB))
            total = jnp.zeros((8, QB), jnp.float32)
            for k0 in range(0, QB, PC):
                s = s_buf[slot % 4, u, k0:k0 + PC, :].reshape(PC // 8, 8, QB)
                p = jnp.exp2((s - m8[None]) * SCALE_LOG2E)
                total = total + jnp.sum(p, axis=0)
                p_buf[slot % 2, u, k0:k0 + PC, :] = p.reshape(PC, QB).astype(jnp.bfloat16)
                if (k0 + PC) % KC == 0:
                    yield
            decay = jnp.exp2((m_prev - m_new) * SCALE_LOG2E)
            decay_s[slot % 2, u] = decay
            l_s[st, u] = l_s[st, u] * decay + jnp.sum(total, axis=0, keepdims=True)
            m_s[st, u] = m_new

    def values(code, slot):
        st, kb, _ = fields(code)
        k_off = pl.multiple_of(lax.rem(kb, 2) * QB, QB)
        for u in range(2):
            pv = jnp.dot(vt[lax.div(kb, 2), :, pl.ds(k_off, QB)], p_buf[slot % 2, u], preferred_element_type=jnp.float32)
            acc[st, u] = acc[st, u] * decay_s[slot % 2, u] + pv
            for _ in range(QB // KC):
                yield

    def together(*parts):
        for _ in itertools.zip_longest(*parts):
            pass

    @pl.when(groups > 0)
    def _():
        p_buf[1] = jnp.zeros_like(p_buf[1])
        decay_s[1] = jnp.ones_like(decay_s[1])
        first = split(words_fn(0)[0])
        together(scores(first[0], 0))
        together(scores(first[1], 1))

        def step(j, _):
            words = words_fn(j)
            codes = [words[3]] + split(words[0]) + split(words[1]) + split(words[2])
            for k in range(4):
                together(weights(codes[k + 1], k), scores(codes[k + 3], k + 2), values(codes[k], k + 1))
            return 0

        lax.fori_loop(0, groups, step, 0)
        together(values(split(words_fn(groups - 1)[1])[1], 1))


def attn_kernel(pos_ref, freq_ref, x_ref, gain_ref, wq_ref, wk_ref, wv_ref, out_ref, kc_ref, vc_ref,
                cos_s, sin_s, h_buf, q_buf, kv, vt, acc, m_s, l_s, s_buf, p_buf, top_s, decay_s, bias, o_buf,
                send_sem, recv_sem, qsend_sem, qrecv_sem, osend_sem, orecv_sem, cache_sem, ocopy_sem):
    me = lax.axis_index("sp")
    x = me // 2
    c = lax.rem(me, 2)
    partner = 2 * x + (1 - c)
    cross = 2 * (1 - x) + c
    diag = 2 * (1 - x) + (1 - c)
    pad = me * ROWS + (ROWS - 1) - pos_ref[ROWS - 1]
    a_masked, a_plain, b_masked, b_plain, b_real, b_far, foreign = schedules()

    barrier = pltpu.get_barrier_semaphore()
    for peer in (partner, cross, diag):
        pl.semaphore_signal(barrier, inc=1, device_id={"sp": peer}, device_id_type=MESH)

    gain = gain_ref[...].reshape(1, DIM).astype(jnp.float32)
    lane = lax.broadcasted_iota(jnp.int32, (256, 128), 1)

    def angle_rows(r):
        rows = pl.ds(r * 256, 256)
        row = lax.broadcasted_iota(jnp.int32, (256, 128), 0) + (me * ROWS + r * 256 - pad)
        ang = jnp.maximum(row, -1).astype(jnp.float32) * freq_ref[...]
        turns = jnp.floor(ang * 0.6366197723675814 + 0.5)
        red = ((ang - turns * 1.5703125) - turns * 4.837512969970703125e-4) - turns * 7.54978995489188216e-8
        sq = red * red
        sin_p = ((-1.9515295891e-4 * sq + 8.3321608736e-3) * sq - 1.6666654611e-1) * sq * red + red
        cos_p = ((2.443315711809948e-5 * sq - 1.388731625493765e-3) * sq + 4.166664568298827e-2) * sq * sq - 0.5 * sq + 1.0
        quad = (turns.astype(jnp.int32) + jnp.where(lane < 64, 0, 3)) & 3
        val = jnp.where((quad & 1) == 0, cos_p, sin_p)
        val = jnp.where((quad == 1) | (quad == 2), -val, val)
        swapped = pltpu.roll(val, 64, 1)
        cos_s[rows, :] = jnp.where(lane < 64, val, swapped)
        sin_s[rows, :] = jnp.where(lane < 64, -swapped, val)

    def rope(t, rows):
        return (t * cos_s[rows, :] + pltpu.roll(t, 64, 1) * sin_s[rows, :]).astype(jnp.bfloat16)

    for r in range(ROWS // 256):
        rows = pl.ds(r * 256, 256)
        angle_rows(r)
        xf = x_ref[rows, :].astype(jnp.float32)
        ms = jnp.mean(xf * xf, axis=-1, keepdims=True)
        h = (xf * lax.rsqrt(ms + NORM_EPS) * gain).astype(jnp.bfloat16)
        h_buf[rows, :] = h
        k = jnp.dot(h, wk_ref[...], preferred_element_type=jnp.float32)
        v = jnp.dot(h, wv_ref[...], preferred_element_type=jnp.float32).astype(jnp.bfloat16)
        for g in range(2):
            kv[me, g, 0, rows, :] = rope(k[:, g * 128:(g + 1) * 128], rows)
            kv[me, g, 1, rows, :] = v[:, g * 128:(g + 1) * 128]

    pl.semaphore_wait(barrier, 3)

    def kv_copy(src, i, peer):
        return pltpu.make_async_remote_copy(src_ref=kv.at[src], dst_ref=kv.at[src], send_sem=send_sem.at[i], recv_sem=recv_sem.at[i],
                                            device_id={"sp": peer}, device_id_type=MESH)

    to_cross = kv_copy(me, 0, cross)
    to_cross.start()
    to_partner = kv_copy(me, 1, partner)
    to_partner.start()

    def q_rows(t):
        def body(r, _):
            rows = pl.ds(pl.multiple_of(t * QB + r * 256, 256), 256)
            inner = pl.ds(pl.multiple_of(r * 256, 256), 256)
            q = jnp.dot(h_buf[rows, :], wq_ref[...], preferred_element_type=jnp.float32)
            for h in range(12):
                q_buf[h // 6, t * 3 + (h % 6) // 2, h % 2, inner, :] = rope(q[:, h * 128:(h + 1) * 128], rows)
            return 0

        lax.fori_loop(0, 2, body, 0)

    def foreign_q(t, g, peer):
        ft = 2 * c + t
        return pltpu.make_async_remote_copy(src_ref=q_buf.at[g, t * 3 + 2], dst_ref=q_buf.at[3, ft], send_sem=qsend_sem.at[t, g],
                                            recv_sem=qrecv_sem.at[ft], device_id={"sp": peer}, device_id_type=MESH)

    def send_foreign(t):
        @pl.when((x == 1) & (2 * c + t < FOREIGN))
        def _():
            foreign_q(t, c, cross).start()
            foreign_q(t, 1 - c, diag).start()

    q_rows(0)
    send_foreign(0)
    q_rows(1)
    send_foreign(1)
    q_copy = pltpu.make_async_remote_copy(src_ref=q_buf.at[1 - c], dst_ref=q_buf.at[2], send_sem=send_sem.at[3], recv_sem=recv_sem.at[3],
                                          device_id={"sp": partner}, device_id_type=MESH)
    q_copy.start()

    def flip(src):
        vt[src] = kv[src, c, 1].T

    def cache_copy(src, i):
        rows = pl.ds(pl.multiple_of(src * ROWS, ROWS), ROWS)
        return (pltpu.make_async_copy(kv.at[src, x, 0], kc_ref.at[rows, :], cache_sem.at[i, 0]),
                pltpu.make_async_copy(kv.at[src, x, 1], vc_ref.at[rows, :], cache_sem.at[i, 1]))

    for cp in cache_copy(me, 0):
        cp.start()
    flip(me)
    tri = lax.broadcasted_iota(jnp.int32, (QB, QB), 0) <= lax.broadcasted_iota(jnp.int32, (QB, QB), 1)
    real = lax.broadcasted_iota(jnp.int32, (QB, QB), 0) >= pad
    bias[TRI] = jnp.where(tri, 0.0, NEG)
    bias[REAL] = jnp.where(real, 0.0, NEG)
    bias[BOTH] = jnp.where(tri & real, 0.0, NEG)
    bias[NONE] = jnp.full((QB, QB), NEG, jnp.float32)
    bias[FREE] = jnp.zeros((QB, QB), jnp.float32)
    m_s[...] = jnp.full_like(m_s, NEG)
    l_s[...] = jnp.zeros_like(l_s)
    acc[...] = jnp.zeros_like(acc)
    to_partner.wait_recv()
    for cp in cache_copy(partner, 1):
        cp.start()
    flip(partner)
    q_copy.wait_recv()

    def by_chip(a, b):
        return jnp.where(x == 0, a, b)

    def flash(a_groups, a_words, a_start, b_run, biased):
        b_words = packed([b_run])

        def words_fn(j):
            return [by_chip(lookup(j + a_start, a), lookup(j, b)) for a, b in zip(a_words, b_words)]

        flash_run(by_chip(a_groups, len(b_run) // 4), words_fn, biased, c, q_buf, kv, vt, acc, m_s, l_s, s_buf, p_buf, top_s, decay_s, bias)

    flash(len(a_masked) // 4, packed([a_masked]), 0, b_masked, True)
    flash(len(a_plain) // 4, packed([a_plain]), 0, b_plain, False)

    def o_place(t, col):
        return out_ref.at[pl.ds(pl.multiple_of(t * QB, QB), QB), pl.ds(pl.multiple_of(col * 256, 256), 256)]

    def o_send(st, t, col, peer):
        return pltpu.make_async_remote_copy(src_ref=o_buf.at[st], dst_ref=o_place(t, col), send_sem=osend_sem.at[st], recv_sem=orecv_sem.at[t, col],
                                            device_id={"sp": peer}, device_id_type=MESH)

    def o_keep(st, t, col):
        return pltpu.make_async_copy(o_buf.at[st], o_place(t, col), ocopy_sem.at[t, lax.rem(col, 3)])

    def finish(st):
        q_idx = lax.broadcasted_iota(jnp.int32, (1, QB), 1) + (x * 2 * ROWS + (st // 3) * QB)
        for u in range(2):
            inv = jnp.where(q_idx >= pad, 1.0 / l_s[st, u], 0.0)
            o_buf[st, :, u * 128:(u + 1) * 128] = (acc[st, u] * inv).T.astype(jnp.bfloat16)

    def here(tb, pair):
        return (x == 0) | (pair < 2) | (tb >= FOREIGN)

    def finish_own(j, _):
        half = jnp.where(j < 6, 1 - c, c)
        t = lax.rem(j, 6) // 3
        pair = lax.rem(j, 3)
        tb = 2 * half + t
        st = 3 * tb + pair

        @pl.when(here(tb, pair))
        def _():
            finish(st)

            @pl.when(j < 6)
            def _():
                o_send(st, t, 3 * c + pair, partner).start()

            @pl.when(j >= 6)
            def _():
                o_keep(st, t, 3 * c + pair).start()

        return 0

    @pl.when(x == 0)
    def _():
        lax.fori_loop(0, 12, finish_own, 0)

    to_cross.wait_recv()
    forward = kv_copy(cross, 2, partner)
    forward.start()
    for cp in cache_copy(cross, 2):
        cp.start()
    flip(cross)
    kv_copy(diag, 2, partner).wait_recv()
    for cp in cache_copy(diag, 3):
        cp.start()
    flip(diag)

    f_len = [len(run) // 4 for run in foreign]
    f_start = [sum(f_len[:k]) for k in range(FOREIGN)]
    f_tb = [2, 0, 1]

    def far_round(j, _):
        ft = lookup(j, f_tb)

        def q_arrived(i):
            pltpu.make_async_remote_copy(src_ref=q_buf.at[0, 2], dst_ref=q_buf.at[3, i], send_sem=qsend_sem.at[0, 0],
                                         recv_sem=qrecv_sem.at[i], device_id={"sp": cross}, device_id_type=MESH).wait_recv()

        @pl.when((x == 0) & (j == 0))
        def _():
            q_arrived(2)
            q_arrived(0)

        @pl.when((x == 0) & (j == 2))
        def _():
            q_arrived(1)

        flash(lookup(j, f_len), packed(foreign), lookup(j, f_start), b_real, True)

        @pl.when(x == 0)
        def _():
            finish(12 + ft)
            o_send(12 + ft, lax.rem(ft, 2), 3 * c + 2, 2 + ft // 2).start()

        return 0

    lax.fori_loop(0, by_chip(FOREIGN, 1), far_round, 0)
    flash(0, packed([b_far]), 0, b_far, False)

    @pl.when(x == 1)
    def _():
        lax.fori_loop(0, 12, finish_own, 0)

    to_cross.wait_send()
    to_partner.wait_send()
    forward.wait_send()
    q_copy.wait_send()
    for i, src in enumerate((me, partner, cross, diag)):
        for cp in cache_copy(src, i):
            cp.wait()
    for t in range(2):
        @pl.when((x == 1) & (2 * c + t < FOREIGN))
        def _():
            foreign_q(t, c, cross).wait_send()
            foreign_q(t, 1 - c, diag).wait_send()

        for pair in range(3):
            mine = here(2 * c + t, pair)
            theirs = here(2 * (1 - c) + t, pair)

            @pl.when(mine)
            def _():
                o_keep(0, t, 3 * c + pair).wait()

            @pl.when(jnp.logical_not(mine))
            def _():
                o_send(0, t, 3 * c + pair, cross).wait_recv()

            o_send(0, t, 3 * (1 - c) + pair, partner).wait_recv()

            @pl.when(theirs)
            def _():
                o_send(3 * (2 * (1 - c) + t) + pair, t, 3 * c + pair, partner).wait_send()

    @pl.when(x == 0)
    def _():
        for ft in range(FOREIGN):
            o_send(12 + ft, ft % 2, 3 * c + 2, 2 + ft // 2).wait_send()


def attn_call(positions, freq, x, gain, w_query, w_key, w_value):
    vm = pl.BlockSpec(memory_space=pltpu.VMEM)
    hbm = pl.BlockSpec(memory_space=pl.ANY)
    flops = 2 * ROWS * DIM * 2048 + 4 * 128 * 3 * 4096 * 2048
    bf, f32 = jnp.bfloat16, jnp.float32
    dma = pltpu.SemaphoreType.DMA
    return pl.pallas_call(
        attn_kernel,
        out_shape=(jax.ShapeDtypeStruct((ROWS, DIM), bf), jax.ShapeDtypeStruct((4 * ROWS, 128), bf), jax.ShapeDtypeStruct((4 * ROWS, 128), bf)),
        in_specs=[pl.BlockSpec(memory_space=pltpu.SMEM)] + [vm] * 6,
        out_specs=(hbm, hbm, hbm),
        scratch_shapes=[
            pltpu.VMEM((ROWS, 128), f32),
            pltpu.VMEM((ROWS, 128), f32),
            pltpu.VMEM((ROWS, DIM), bf),
            pltpu.VMEM((4, 6, 2, QB, 128), bf),
            pltpu.VMEM((4, 2, 2, ROWS, 128), bf),
            pltpu.VMEM((4, 128, ROWS), bf),
            pltpu.VMEM((12 + FOREIGN, 2, 128, QB), f32),
            pltpu.VMEM((12 + FOREIGN, 2, 1, QB), f32),
            pltpu.VMEM((12 + FOREIGN, 2, 1, QB), f32),
            pltpu.VMEM((4, 2, QB, QB), f32),
            pltpu.VMEM((2, 2, QB, QB), bf),
            pltpu.VMEM((4, 2, 8, QB), f32),
            pltpu.VMEM((2, 2, 1, QB), f32),
            pltpu.VMEM((5, QB, QB), f32),
            pltpu.VMEM((12 + FOREIGN, QB, 256), bf),
            dma((4,)), dma((4,)), dma((2, 2)), dma((FOREIGN,)), dma((12 + FOREIGN,)), dma((2, 6)), dma((4, 2)), dma((2, 3)),
        ],
        compiler_params=pltpu.CompilerParams(vmem_limit_bytes=62 << 20, collective_id=0, has_side_effects=True),
        cost_estimate=pl.CostEstimate(flops=flops, bytes_accessed=20 << 20, transcendentals=3 * 4096 * 2048),
        name="attn_block",
    )(positions, freq, x, gain, w_query, w_key, w_value)


def solution(mesh):
    freq = 1.0 / (ROPE_THETA ** (np.arange(0, HEAD_DIM, 2, dtype=np.float64) / HEAD_DIM))
    freq = np.concatenate([freq, freq]).astype(np.float32).reshape(1, HEAD_DIM)

    def layer_shard(hidden, positions, attn_gain, w_query, w_key, w_value, w_out, mlp_gain, w_gate, w_up, w_down):
        attn, k_all, v_all = attn_call(positions, jnp.asarray(freq), hidden, attn_gain, w_query, w_key, w_value)
        hidden_out, k_cache, v_cache = mlp_call(attn, hidden, w_out, mlp_gain, w_gate, w_up, w_down, k_all, v_all)
        return hidden_out, k_cache.reshape(4 * ROWS, 1, HEAD_DIM), v_cache.reshape(4 * ROWS, 1, HEAD_DIM)

    row_spec = P(("dp", "sp"), None)
    cache_spec = P("dp", "sp", None)
    return jax.shard_map(layer_shard, mesh=mesh, in_specs=(row_spec, P(("dp", "sp")), P(), P(), P(), P(), P(), P(), P(), P(), P()), out_specs=(row_spec, cache_spec, cache_spec), check_vma=False)
```

```python
import functools
import itertools
import jax
import jax.numpy as jnp
import numpy as np
from jax import lax
from jax.experimental import pallas as pl
from jax.experimental.pallas import tpu as pltpu
from jax.sharding import PartitionSpec as P

ROWS = 1024
DIM = 1536
FFN = 8960
NORM_EPS = 1e-5


def mlp_kernel(fb, rt, o_hbm, x_hbm, wout_hbm, gain_ref, wg_hbm, wu_hbm, wd_hbm, k_in, v_in, out_hbm, k_out, v_out, o_ref, x_ref, wout_ref, acc, g_buf, m_buf, wg, wu, wd, c_buf, sems, c_sems, in_sems, out_sems):
    steps = FFN // fb

    def copies(j, slot):
        off = pl.multiple_of(j * fb, 128)
        return (
            pltpu.make_async_copy(wg_hbm.at[:, pl.ds(off, fb)], wg.at[slot], sems.at[slot, 0]),
            pltpu.make_async_copy(wu_hbm.at[:, pl.ds(off, fb)], wu.at[slot], sems.at[slot, 1]),
            pltpu.make_async_copy(wd_hbm.at[pl.ds(off, fb), :], wd.at[slot], sems.at[slot, 2]),
        )

    wout_copy = pltpu.make_async_copy(wout_hbm, wout_ref, in_sems.at[2, 0])
    wout_copy.start()

    def row_copies(r):
        rows = pl.ds(r * 256, 256)
        return (pltpu.make_async_copy(o_hbm.at[rows, :], o_ref.at[rows, :], in_sems.at[0, r]),
                pltpu.make_async_copy(x_hbm.at[rows, :], x_ref.at[rows, :], in_sems.at[1, r]))

    for r in range(ROWS // 256):
        for c in row_copies(r):
            c.start()
    for c in copies(0, 0):
        c.start()

    cache = ((k_in, k_out), (v_in, v_out))
    for i in range(2):
        pltpu.make_async_copy(cache[i][0], c_buf.at[i], c_sems.at[0, i]).start()
    gain = gain_ref[...].reshape(1, DIM).astype(jnp.float32)

    wout_copy.wait()

    def proj(half):
        for r in (2 * half, 2 * half + 1):
            for c in row_copies(r):
                c.wait()
        for r in range(2 * half, 2 * half + 2):
            rows = pl.ds(r * 256, 256)
            y = x_ref[rows, :].astype(jnp.float32) + jnp.dot(o_ref[rows, :], wout_ref[...], preferred_element_type=jnp.float32)
            y = y.astype(jnp.bfloat16).astype(jnp.float32)
            acc[rows, :] = y
            ms = jnp.mean(y * y, axis=-1, keepdims=True)
            g_buf[rows, :] = (y * lax.rsqrt(ms + NORM_EPS) * gain).astype(jnp.bfloat16)

    proj(0)
    proj(1)
    for i in range(2):
        pltpu.make_async_copy(cache[i][0], c_buf.at[i], c_sems.at[0, i]).wait()
        pltpu.make_async_copy(c_buf.at[i], cache[i][1], c_sems.at[1, i]).start()

    def step(j, _):
        slot = lax.rem(j, 2)
        for c in copies(j, slot):
            c.wait()

        @pl.when(j + 1 < steps)
        def _():
            for c in copies(j + 1, 1 - slot):
                c.start()

        def tile(r, _):
            rows = pl.ds(pl.multiple_of(r * rt, rt), rt)
            for c0 in range(0, fb, 256):
                cols = pl.ds(c0, 256)
                gate = jnp.dot(g_buf[rows, :], wg[slot, :, cols], preferred_element_type=jnp.float32)
                up = jnp.dot(g_buf[rows, :], wu[slot, :, cols], preferred_element_type=jnp.float32)
                m_buf[:, cols] = (gate / (1.0 + jnp.exp(-gate)) * up).astype(jnp.bfloat16)
            acc[rows, :] += jnp.dot(m_buf[...], wd[slot], preferred_element_type=jnp.float32)

            @pl.when(j == steps - 1)
            def _():
                def fin(q, _):
                    part = pl.ds(pl.multiple_of(r * rt + q * 128, 128), 128)
                    o_ref[part, :] = acc[part, :].astype(jnp.bfloat16)
                    return 0

                lax.fori_loop(0, rt // 128, fin, 0)
                pltpu.make_async_copy(o_ref.at[rows, :], out_hbm.at[rows, :], out_sems.at[r]).start()

            return 0

        lax.fori_loop(0, ROWS // rt, tile, 0)
        return 0

    lax.fori_loop(0, steps, step, 0)

    for r in range(ROWS // rt):
        rows = pl.ds(r * rt, rt)
        pltpu.make_async_copy(o_ref.at[rows, :], out_hbm.at[rows, :], out_sems.at[r]).wait()
    for i in range(2):
        pltpu.make_async_copy(c_buf.at[i], cache[i][1], c_sems.at[1, i]).wait()


def mlp_call(o, x, w_out, gain, wg, wu, wd, k_all, v_all, fb=1280, rt=512):
    vm = pl.BlockSpec(memory_space=pltpu.VMEM)
    hbm = pl.BlockSpec(memory_space=pl.ANY)
    flops = 2 * ROWS * DIM * (DIM + 3 * FFN)
    return pl.pallas_call(
        functools.partial(mlp_kernel, fb, rt),
        out_shape=(jax.ShapeDtypeStruct((ROWS, DIM), jnp.bfloat16),) + (jax.ShapeDtypeStruct(k_all.shape, jnp.bfloat16),) * 2,
        in_specs=[hbm] * 3 + [vm] + [hbm] * 5,
        out_specs=(hbm, hbm, hbm),
        scratch_shapes=[
            pltpu.VMEM((ROWS, DIM), jnp.bfloat16),
            pltpu.VMEM((ROWS, DIM), jnp.bfloat16),
            pltpu.VMEM((DIM, DIM), jnp.bfloat16),
            pltpu.VMEM((ROWS, DIM), jnp.float32),
            pltpu.VMEM((ROWS, DIM), jnp.bfloat16),
            pltpu.VMEM((rt, fb), jnp.bfloat16),
            pltpu.VMEM((2, DIM, fb), jnp.bfloat16),
            pltpu.VMEM((2, DIM, fb), jnp.bfloat16),
            pltpu.VMEM((2, fb, DIM), jnp.bfloat16),
            pltpu.VMEM((2, 4 * ROWS, 128), jnp.bfloat16),
            pltpu.SemaphoreType.DMA((2, 3)),
            pltpu.SemaphoreType.DMA((2, 2)),
            pltpu.SemaphoreType.DMA((3, 4)),
            pltpu.SemaphoreType.DMA((ROWS // rt,)),
        ],
        compiler_params=pltpu.CompilerParams(vmem_limit_bytes=60 << 20),
        cost_estimate=pl.CostEstimate(flops=flops, bytes_accessed=3 * DIM * FFN * 2, transcendentals=ROWS * FFN),
        name="mlp_block",
    )(o, x, w_out, gain, wg, wu, wd, k_all, v_all)


HEAD_DIM = 128
ROPE_THETA = 500000
SCALE_LOG2E = 1.4426950408889634 * HEAD_DIM ** -0.5
NEG = -2.0e38
QB = 512
KC = 512
PC = 64
FOREIGN = 2
TRI, REAL, BOTH, NONE, FREE = range(5)
MESH = pl.DeviceIdType.MESH


def schedules():
    def code(st, kb, b):
        return (st * 8 + kb) * 8 + b

    a_masked = [code(3 * tb + p, tb, BOTH if tb == 0 else TRI) for tb in range(4) for p in range(3)]
    a_masked += [code(3 * tb + p, 0, REAL) for tb in range(1, 4) for p in range(3)]
    a_plain = [code(3 * tb + p, kb, FREE) for tb in range(2, 4) for kb in range(1, tb) for p in range(3)]
    a_masked += [a_plain.pop(0), *[a_plain[-1] - FREE + NONE] * 2]
    pairs = {tb: 2 if tb < FOREIGN else 3 for tb in range(4)}
    b_masked = [code(3 * tb + p, 4 + tb, TRI) for tb in range(4) for p in range(pairs[tb])]
    b_plain = [code(3 * tb + p, 4 + kb, FREE) for tb in range(1, 4) for kb in range(tb) for p in range(pairs[tb])]
    b_masked += [b_plain.pop(0), b_plain[-1] - FREE + NONE]
    b_real = [code(3 * tb + p, 0, REAL) for tb in range(4) for p in range(pairs[tb])]
    b_far = [code(3 * tb + p, kb, FREE) for tb in range(4) for kb in range(1, 4) for p in range(pairs[tb])]
    b_real += [b_far.pop(0), b_far.pop(0)]
    foreign = []
    for tb in range(FOREIGN):
        run = [code(12 + tb, 0, REAL)] + [code(12 + tb, kb, FREE) for kb in range(1, 4 + tb)] + [code(12 + tb, 4 + tb, TRI)]
        foreign.append(run + [code(12 + tb, 4 + tb, NONE)] * (-len(run) % 4))
    for run in (a_masked, a_plain, b_masked, b_plain, b_real, b_far, *foreign):
        assert len(run) % 4 == 0
    return a_masked, a_plain, b_masked, b_plain, b_real, b_far, foreign


def packed(runs):
    words = ([], [], [], [])
    for run in runs:
        for j in range(0, len(run), 4):
            ahead = [run[min(j + k, len(run) - 1)] for k in range(6)]
            for w in range(3):
                words[w].append(ahead[2 * w] + 1024 * ahead[2 * w + 1])
            words[3].append(run[max(j - 1, 0)])
    return words


def lookup(i, values):
    if len(values) == 1:
        return values[0]
    if all(v == values[0] for v in values):
        return values[0]
    half = len(values) // 2
    return jnp.where(i < half, lookup(i, values[:half]), lookup(i - half, values[half:]))


def flash_run(groups, words_fn, biased, me_c, q_buf, kv, vt, acc, m_s, l_s, s_buf, p_buf, top_s, decay_s, bias):
    def fields(code):
        return lax.div(code, 64), lax.rem(lax.div(code, 8), 8), lax.rem(code, 8)

    def split(word):
        return [lax.rem(word, 1024), lax.div(word, 1024)]

    def scores(code, slot):
        st, kb, b = fields(code)
        tb = lax.div(st, 3)
        own = st < 12
        place = jnp.where(own, jnp.where(lax.div(tb, 2) == me_c, me_c, 2), 3)
        entry = jnp.where(own, lax.rem(tb, 2) * 3 + lax.rem(st, 3), st - 12)
        k_off = pl.multiple_of(lax.rem(kb, 2) * QB, QB)
        for u in range(2):
            q_blk = q_buf[place, entry, u]
            top = jnp.full((8, QB), NEG, jnp.float32)
            for k0 in range(0, QB, KC):
                k_blk = kv[lax.div(kb, 2), me_c, 0, pl.ds(k_off + k0, KC), :]
                s = lax.dot_general(k_blk, q_blk, (((1,), (1,)), ((), ())), preferred_element_type=jnp.float32)
                if biased:
                    s = s + bias[b, k0:k0 + KC, :]
                s_buf[slot % 4, u, k0:k0 + KC, :] = s
                top = jnp.maximum(top, jnp.max(s.reshape(KC // 8, 8, QB), axis=0))
                yield
            top_s[slot % 4, u] = top

    def weights(code, slot):
        st = fields(code)[0]
        for u in range(2):
            m_prev = m_s[st, u]
            m_new = jnp.maximum(m_prev, jnp.max(top_s[slot % 4, u], axis=0, keepdims=True))
            m8 = jnp.broadcast_to(m_new, (8, QB))
            total = jnp.zeros((8, QB), jnp.float32)
            for k0 in range(0, QB, PC):
                s = s_buf[slot % 4, u, k0:k0 + PC, :].reshape(PC // 8, 8, QB)
                p = jnp.exp2((s - m8[None]) * SCALE_LOG2E)
                total = total + jnp.sum(p, axis=0)
                p_buf[slot % 2, u, k0:k0 + PC, :] = p.reshape(PC, QB).astype(jnp.bfloat16)
                if (k0 + PC) % KC == 0:
                    yield
            decay = jnp.exp2((m_prev - m_new) * SCALE_LOG2E)
            decay_s[slot % 2, u] = decay
            l_s[st, u] = l_s[st, u] * decay + jnp.sum(total, axis=0, keepdims=True)
            m_s[st, u] = m_new

    def values(code, slot):
        st, kb, _ = fields(code)
        k_off = pl.multiple_of(lax.rem(kb, 2) * QB, QB)
        for u in range(2):
            pv = jnp.dot(vt[lax.div(kb, 2), :, pl.ds(k_off, QB)], p_buf[slot % 2, u], preferred_element_type=jnp.float32)
            acc[st, u] = acc[st, u] * decay_s[slot % 2, u] + pv
            for _ in range(QB // KC):
                yield

    def together(*parts):
        for _ in itertools.zip_longest(*parts):
            pass

    @pl.when(groups > 0)
    def _():
        p_buf[1] = jnp.zeros_like(p_buf[1])
        decay_s[1] = jnp.ones_like(decay_s[1])
        first = split(words_fn(0)[0])
        together(scores(first[0], 0))
        together(scores(first[1], 1))

        def step(j, _):
            words = words_fn(j)
            codes = [words[3]] + split(words[0]) + split(words[1]) + split(words[2])
            for k in range(4):
                together(weights(codes[k + 1], k), scores(codes[k + 3], k + 2), values(codes[k], k + 1))
            return 0

        lax.fori_loop(0, groups, step, 0)
        together(values(split(words_fn(groups - 1)[1])[1], 1))


def attn_kernel(pos_ref, freq_ref, x_ref, gain_ref, wk_ref, wv_ref, wq_hbm, out_ref, kc_ref, vc_ref,
                wq_ref, cos_s, sin_s, h_buf, q_buf, kv, vt, acc, m_s, l_s, s_buf, p_buf, top_s, decay_s, bias, o_buf,
                send_sem, recv_sem, qsend_sem, qrecv_sem, osend_sem, orecv_sem, cache_sem, ocopy_sem, wq_sem):
    me = lax.axis_index("sp")
    x = me // 2
    c = lax.rem(me, 2)
    partner = 2 * x + (1 - c)
    cross = 2 * (1 - x) + c
    diag = 2 * (1 - x) + (1 - c)
    pad = me * ROWS + (ROWS - 1) - pos_ref[ROWS - 1]
    a_masked, a_plain, b_masked, b_plain, b_real, b_far, foreign = schedules()

    wq_copy = pltpu.make_async_copy(wq_hbm, wq_ref, wq_sem.at[0])
    wq_copy.start()
    barrier = pltpu.get_barrier_semaphore()
    for peer in (partner, cross, diag):
        pl.semaphore_signal(barrier, inc=1, device_id={"sp": peer}, device_id_type=MESH)

    gain = gain_ref[...].reshape(1, DIM).astype(jnp.float32)
    lane = lax.broadcasted_iota(jnp.int32, (256, 128), 1)

    def angle_rows(r):
        rows = pl.ds(r * 256, 256)
        row = lax.broadcasted_iota(jnp.int32, (256, 128), 0) + (me * ROWS + r * 256 - pad)
        ang = jnp.maximum(row, -1).astype(jnp.float32) * freq_ref[...]
        turns = jnp.floor(ang * 0.6366197723675814 + 0.5)
        red = ((ang - turns * 1.5703125) - turns * 4.837512969970703125e-4) - turns * 7.54978995489188216e-8
        sq = red * red
        sin_p = ((-1.9515295891e-4 * sq + 8.3321608736e-3) * sq - 1.6666654611e-1) * sq * red + red
        cos_p = ((2.443315711809948e-5 * sq - 1.388731625493765e-3) * sq + 4.166664568298827e-2) * sq * sq - 0.5 * sq + 1.0
        quad = (turns.astype(jnp.int32) + jnp.where(lane < 64, 0, 3)) & 3
        val = jnp.where((quad & 1) == 0, cos_p, sin_p)
        val = jnp.where((quad == 1) | (quad == 2), -val, val)
        swapped = pltpu.roll(val, 64, 1)
        cos_s[rows, :] = jnp.where(lane < 64, val, swapped)
        sin_s[rows, :] = jnp.where(lane < 64, -swapped, val)

    def rope(t, rows):
        return (t * cos_s[rows, :] + pltpu.roll(t, 64, 1) * sin_s[rows, :]).astype(jnp.bfloat16)

    for r in range(ROWS // 256):
        rows = pl.ds(r * 256, 256)
        angle_rows(r)
        xf = x_ref[rows, :].astype(jnp.float32)
        ms = jnp.mean(xf * xf, axis=-1, keepdims=True)
        h = (xf * lax.rsqrt(ms + NORM_EPS) * gain).astype(jnp.bfloat16)
        h_buf[rows, :] = h
        k = jnp.dot(h, wk_ref[...], preferred_element_type=jnp.float32)
        v = jnp.dot(h, wv_ref[...], preferred_element_type=jnp.float32).astype(jnp.bfloat16)
        for g in range(2):
            kv[me, g, 0, rows, :] = rope(k[:, g * 128:(g + 1) * 128], rows)
            kv[me, g, 1, rows, :] = v[:, g * 128:(g + 1) * 128]

    pl.semaphore_wait(barrier, 3)

    def kv_copy(src, i, peer):
        return pltpu.make_async_remote_copy(src_ref=kv.at[src], dst_ref=kv.at[src], send_sem=send_sem.at[i], recv_sem=recv_sem.at[i],
                                            device_id={"sp": peer}, device_id_type=MESH)

    to_cross = kv_copy(me, 0, cross)
    to_cross.start()
    to_partner = kv_copy(me, 1, partner)
    to_partner.start()

    def q_rows(t):
        def body(r, _):
            rows = pl.ds(pl.multiple_of(t * QB + r * 256, 256), 256)
            inner = pl.ds(pl.multiple_of(r * 256, 256), 256)
            part = t * 2 + r
            k_rows = pl.ds(pl.multiple_of(part * 128, 128), 128)
            k_idx = lax.broadcasted_iota(jnp.int32, (128, QB), 0) + part * 128
            tri = k_idx <= lax.broadcasted_iota(jnp.int32, (128, QB), 1)
            real = k_idx >= pad
            bias[TRI, k_rows, :] = jnp.where(tri, 0.0, NEG)
            bias[REAL, k_rows, :] = jnp.where(real, 0.0, NEG)
            bias[BOTH, k_rows, :] = jnp.where(tri & real, 0.0, NEG)
            bias[NONE, k_rows, :] = jnp.full((128, QB), NEG, jnp.float32)
            bias[FREE, k_rows, :] = jnp.zeros((128, QB), jnp.float32)
            acc[:, :, pl.ds(pl.multiple_of(part * 32, 32), 32), :] = jnp.zeros((12 + FOREIGN, 2, 32, QB), jnp.float32)
            q = jnp.dot(h_buf[rows, :], wq_ref[...], preferred_element_type=jnp.float32)
            for h in range(12):
                q_buf[h // 6, t * 3 + (h % 6) // 2, h % 2, inner, :] = rope(q[:, h * 128:(h + 1) * 128], rows)
            return 0

        lax.fori_loop(0, 2, body, 0)

    def foreign_q(t, g, peer):
        ft = 2 * c + t
        return pltpu.make_async_remote_copy(src_ref=q_buf.at[g, t * 3 + 2], dst_ref=q_buf.at[3, ft], send_sem=qsend_sem.at[t, g],
                                            recv_sem=qrecv_sem.at[ft], device_id={"sp": peer}, device_id_type=MESH)

    def send_foreign(t):
        @pl.when((x == 1) & (2 * c + t < FOREIGN))
        def _():
            foreign_q(t, c, cross).start()
            foreign_q(t, 1 - c, diag).start()

    wq_copy.wait()
    q_rows(0)
    send_foreign(0)
    q_rows(1)
    send_foreign(1)
    q_copy = pltpu.make_async_remote_copy(src_ref=q_buf.at[1 - c], dst_ref=q_buf.at[2], send_sem=send_sem.at[3], recv_sem=recv_sem.at[3],
                                          device_id={"sp": partner}, device_id_type=MESH)
    q_copy.start()

    def flip(src):
        vt[src] = kv[src, c, 1].T

    def cache_copy(src, i):
        rows = pl.ds(pl.multiple_of(src * ROWS, ROWS), ROWS)
        return (pltpu.make_async_copy(kv.at[src, x, 0], kc_ref.at[rows, :], cache_sem.at[i, 0]),
                pltpu.make_async_copy(kv.at[src, x, 1], vc_ref.at[rows, :], cache_sem.at[i, 1]))

    for cp in cache_copy(me, 0):
        cp.start()
    flip(me)
    m_s[...] = jnp.full_like(m_s, NEG)
    l_s[...] = jnp.zeros_like(l_s)
    to_partner.wait_recv()
    for cp in cache_copy(partner, 1):
        cp.start()
    flip(partner)
    q_copy.wait_recv()

    def by_chip(a, b):
        return jnp.where(x == 0, a, b)

    def flash(a_groups, a_words, a_start, b_run, biased):
        b_words = packed([b_run])

        def words_fn(j):
            return [by_chip(lookup(j + a_start, a), lookup(j, b)) for a, b in zip(a_words, b_words)]

        flash_run(by_chip(a_groups, len(b_run) // 4), words_fn, biased, c, q_buf, kv, vt, acc, m_s, l_s, s_buf, p_buf, top_s, decay_s, bias)

    flash(len(a_masked) // 4, packed([a_masked]), 0, b_masked, True)
    flash(len(a_plain) // 4, packed([a_plain]), 0, b_plain, False)

    def o_place(t, col):
        return out_ref.at[pl.ds(pl.multiple_of(t * QB, QB), QB), pl.ds(pl.multiple_of(col * 256, 256), 256)]

    def o_send(st, t, col, peer):
        return pltpu.make_async_remote_copy(src_ref=o_buf.at[st], dst_ref=o_place(t, col), send_sem=osend_sem.at[st], recv_sem=orecv_sem.at[t, col],
                                            device_id={"sp": peer}, device_id_type=MESH)

    def o_keep(st, t, col):
        return pltpu.make_async_copy(o_buf.at[st], o_place(t, col), ocopy_sem.at[t, lax.rem(col, 3)])

    def finish(st):
        q_idx = lax.broadcasted_iota(jnp.int32, (1, QB), 1) + (x * 2 * ROWS + (st // 3) * QB)
        for u in range(2):
            inv = jnp.where(q_idx >= pad, 1.0 / l_s[st, u], 0.0)
            o_buf[st, :, u * 128:(u + 1) * 128] = (acc[st, u] * inv).T.astype(jnp.bfloat16)

    def here(tb, pair):
        return (x == 0) | (pair < 2) | (tb >= FOREIGN)

    def finish_own(j, _):
        half = jnp.where(j < 6, 1 - c, c)
        t = lax.rem(j, 6) // 3
        pair = lax.rem(j, 3)
        tb = 2 * half + t
        st = 3 * tb + pair

        @pl.when(here(tb, pair))
        def _():
            finish(st)

            @pl.when(j < 6)
            def _():
                o_send(st, t, 3 * c + pair, partner).start()

            @pl.when(j >= 6)
            def _():
                o_keep(st, t, 3 * c + pair).start()

        return 0

    @pl.when(x == 0)
    def _():
        lax.fori_loop(0, 12, finish_own, 0)

    to_cross.wait_recv()
    forward = kv_copy(cross, 2, partner)
    forward.start()
    for cp in cache_copy(cross, 2):
        cp.start()
    flip(cross)
    kv_copy(diag, 2, partner).wait_recv()
    for cp in cache_copy(diag, 3):
        cp.start()
    flip(diag)

    f_len = [len(run) // 4 for run in foreign]
    f_start = [sum(f_len[:k]) for k in range(FOREIGN)]

    def far_round(j, _):
        @pl.when(x == 0)
        def _():
            pltpu.make_async_remote_copy(src_ref=q_buf.at[0, 2], dst_ref=q_buf.at[3, j], send_sem=qsend_sem.at[0, 0],
                                         recv_sem=qrecv_sem.at[j], device_id={"sp": cross}, device_id_type=MESH).wait_recv()

        flash(lookup(j, f_len), packed(foreign), lookup(j, f_start), b_real, True)

        @pl.when(x == 0)
        def _():
            finish(12 + j)
            o_send(12 + j, lax.rem(j, 2), 3 * c + 2, 2 + j // 2).start()

        return 0

    lax.fori_loop(0, by_chip(FOREIGN, 1), far_round, 0)
    flash(0, packed([b_far]), 0, b_far, False)

    @pl.when(x == 1)
    def _():
        lax.fori_loop(0, 12, finish_own, 0)

    to_cross.wait_send()
    to_partner.wait_send()
    forward.wait_send()
    q_copy.wait_send()
    for i, src in enumerate((me, partner, cross, diag)):
        for cp in cache_copy(src, i):
            cp.wait()
    for t in range(2):
        @pl.when((x == 1) & (2 * c + t < FOREIGN))
        def _():
            foreign_q(t, c, cross).wait_send()
            foreign_q(t, 1 - c, diag).wait_send()

        for pair in range(3):
            mine = here(2 * c + t, pair)
            theirs = here(2 * (1 - c) + t, pair)

            @pl.when(mine)
            def _():
                o_keep(0, t, 3 * c + pair).wait()

            @pl.when(jnp.logical_not(mine))
            def _():
                o_send(0, t, 3 * c + pair, cross).wait_recv()

            o_send(0, t, 3 * (1 - c) + pair, partner).wait_recv()

            @pl.when(theirs)
            def _():
                o_send(3 * (2 * (1 - c) + t) + pair, t, 3 * c + pair, partner).wait_send()

    @pl.when(x == 0)
    def _():
        for ft in range(FOREIGN):
            o_send(12 + ft, ft % 2, 3 * c + 2, 2 + ft // 2).wait_send()


def attn_call(positions, freq, x, gain, w_query, w_key, w_value):
    vm = pl.BlockSpec(memory_space=pltpu.VMEM)
    hbm = pl.BlockSpec(memory_space=pl.ANY)
    flops = 2 * ROWS * DIM * 2048 + 4 * 128 * 3 * 4096 * 2048
    bf, f32 = jnp.bfloat16, jnp.float32
    dma = pltpu.SemaphoreType.DMA
    return pl.pallas_call(
        attn_kernel,
        out_shape=(jax.ShapeDtypeStruct((ROWS, DIM), bf), jax.ShapeDtypeStruct((4 * ROWS, 128), bf), jax.ShapeDtypeStruct((4 * ROWS, 128), bf)),
        in_specs=[pl.BlockSpec(memory_space=pltpu.SMEM)] + [vm] * 5 + [hbm],
        out_specs=(hbm, hbm, hbm),
        scratch_shapes=[
            pltpu.VMEM((DIM, DIM), bf),
            pltpu.VMEM((ROWS, 128), f32),
            pltpu.VMEM((ROWS, 128), f32),
            pltpu.VMEM((ROWS, DIM), bf),
            pltpu.VMEM((4, 6, 2, QB, 128), bf),
            pltpu.VMEM((4, 2, 2, ROWS, 128), bf),
            pltpu.VMEM((4, 128, ROWS), bf),
            pltpu.VMEM((12 + FOREIGN, 2, 128, QB), f32),
            pltpu.VMEM((12 + FOREIGN, 2, 1, QB), f32),
            pltpu.VMEM((12 + FOREIGN, 2, 1, QB), f32),
            pltpu.VMEM((4, 2, QB, QB), f32),
            pltpu.VMEM((2, 2, QB, QB), bf),
            pltpu.VMEM((4, 2, 8, QB), f32),
            pltpu.VMEM((2, 2, 1, QB), f32),
            pltpu.VMEM((5, QB, QB), f32),
            pltpu.VMEM((12 + FOREIGN, QB, 256), bf),
            dma((4,)), dma((4,)), dma((2, 2)), dma((FOREIGN,)), dma((12 + FOREIGN,)), dma((2, 6)), dma((4, 2)), dma((2, 3)), dma((1,)),
        ],
        compiler_params=pltpu.CompilerParams(vmem_limit_bytes=62 << 20, collective_id=0, has_side_effects=True),
        cost_estimate=pl.CostEstimate(flops=flops, bytes_accessed=20 << 20, transcendentals=3 * 4096 * 2048),
        name="attn_block",
    )(positions, freq, x, gain, w_key, w_value, w_query)


def solution(mesh):
    freq = 1.0 / (ROPE_THETA ** (np.arange(0, HEAD_DIM, 2, dtype=np.float64) / HEAD_DIM))
    freq = np.concatenate([freq, freq]).astype(np.float32).reshape(1, HEAD_DIM)

    def layer_shard(hidden, positions, attn_gain, w_query, w_key, w_value, w_out, mlp_gain, w_gate, w_up, w_down):
        attn, k_all, v_all = attn_call(positions, jnp.asarray(freq), hidden, attn_gain, w_query, w_key, w_value)
        hidden_out, k_cache, v_cache = mlp_call(attn, hidden, w_out, mlp_gain, w_gate, w_up, w_down, k_all, v_all)
        return hidden_out, k_cache.reshape(4 * ROWS, 1, HEAD_DIM), v_cache.reshape(4 * ROWS, 1, HEAD_DIM)

    row_spec = P(("dp", "sp"), None)
    cache_spec = P("dp", "sp", None)
    return jax.shard_map(layer_shard, mesh=mesh, in_specs=(row_spec, P(("dp", "sp")), P(), P(), P(), P(), P(), P(), P(), P(), P()), out_specs=(row_spec, cache_spec, cache_spec), check_vma=False)
```

```python
import functools
import itertools
import jax
import jax.numpy as jnp
import numpy as np
from jax import lax
from jax.experimental import pallas as pl
from jax.experimental.pallas import tpu as pltpu
from jax.sharding import PartitionSpec as P

ROWS = 1024
DIM = 1536
FFN = 8960
NORM_EPS = 1e-5


def mlp_kernel(fb, rt, o_hbm, x_hbm, wout_hbm, gain_ref, wg_hbm, wu_hbm, wd_hbm, k_in, v_in, out_hbm, k_out, v_out, o_ref, x_ref, wout_ref, acc, g_buf, m_buf, wg, wu, wd, c_buf, sems, c_sems, in_sems, out_sems):
    steps = FFN // fb

    def copies(j, slot):
        off = pl.multiple_of(j * fb, 128)
        return (
            pltpu.make_async_copy(wg_hbm.at[:, pl.ds(off, fb)], wg.at[slot], sems.at[slot, 0]),
            pltpu.make_async_copy(wu_hbm.at[:, pl.ds(off, fb)], wu.at[slot], sems.at[slot, 1]),
            pltpu.make_async_copy(wd_hbm.at[pl.ds(off, fb), :], wd.at[slot], sems.at[slot, 2]),
        )

    wout_copy = pltpu.make_async_copy(wout_hbm, wout_ref, in_sems.at[2, 0])
    wout_copy.start()

    def row_copies(r):
        rows = pl.ds(r * 256, 256)
        return (pltpu.make_async_copy(o_hbm.at[rows, :], o_ref.at[rows, :], in_sems.at[0, r]),
                pltpu.make_async_copy(x_hbm.at[rows, :], x_ref.at[rows, :], in_sems.at[1, r]))

    for r in range(ROWS // 256):
        for c in row_copies(r):
            c.start()
    for c in copies(0, 0):
        c.start()

    cache = ((k_in, k_out), (v_in, v_out))
    for i in range(2):
        pltpu.make_async_copy(cache[i][0], c_buf.at[i], c_sems.at[0, i]).start()
    gain = gain_ref[...].reshape(1, DIM).astype(jnp.float32)

    wout_copy.wait()

    def proj(half):
        for r in (2 * half, 2 * half + 1):
            for c in row_copies(r):
                c.wait()
        for r in range(2 * half, 2 * half + 2):
            rows = pl.ds(r * 256, 256)
            y = x_ref[rows, :].astype(jnp.float32) + jnp.dot(o_ref[rows, :], wout_ref[...], preferred_element_type=jnp.float32)
            y = y.astype(jnp.bfloat16).astype(jnp.float32)
            acc[rows, :] = y
            ms = jnp.mean(y * y, axis=-1, keepdims=True)
            g_buf[rows, :] = (y * lax.rsqrt(ms + NORM_EPS) * gain).astype(jnp.bfloat16)

    proj(0)
    proj(1)
    for i in range(2):
        pltpu.make_async_copy(cache[i][0], c_buf.at[i], c_sems.at[0, i]).wait()
        pltpu.make_async_copy(c_buf.at[i], cache[i][1], c_sems.at[1, i]).start()

    def step(j, _):
        slot = lax.rem(j, 2)
        for c in copies(j, slot):
            c.wait()

        @pl.when(j + 1 < steps)
        def _():
            for c in copies(j + 1, 1 - slot):
                c.start()

        def tile(r, _):
            rows = pl.ds(pl.multiple_of(r * rt, rt), rt)
            for c0 in range(0, fb, 256):
                cols = pl.ds(c0, 256)
                gate = jnp.dot(g_buf[rows, :], wg[slot, :, cols], preferred_element_type=jnp.float32)
                up = jnp.dot(g_buf[rows, :], wu[slot, :, cols], preferred_element_type=jnp.float32)
                m_buf[:, cols] = (gate / (1.0 + jnp.exp(-gate)) * up).astype(jnp.bfloat16)
            acc[rows, :] += jnp.dot(m_buf[...], wd[slot], preferred_element_type=jnp.float32)

            @pl.when(j == steps - 1)
            def _():
                def fin(q, _):
                    part = pl.ds(pl.multiple_of(r * rt + q * 128, 128), 128)
                    o_ref[part, :] = acc[part, :].astype(jnp.bfloat16)
                    return 0

                lax.fori_loop(0, rt // 128, fin, 0)
                pltpu.make_async_copy(o_ref.at[rows, :], out_hbm.at[rows, :], out_sems.at[r]).start()

            return 0

        lax.fori_loop(0, ROWS // rt, tile, 0)
        return 0

    lax.fori_loop(0, steps, step, 0)

    for r in range(ROWS // rt):
        rows = pl.ds(r * rt, rt)
        pltpu.make_async_copy(o_ref.at[rows, :], out_hbm.at[rows, :], out_sems.at[r]).wait()
    for i in range(2):
        pltpu.make_async_copy(c_buf.at[i], cache[i][1], c_sems.at[1, i]).wait()


def mlp_call(o, x, w_out, gain, wg, wu, wd, k_all, v_all, fb=1792, rt=512):
    vm = pl.BlockSpec(memory_space=pltpu.VMEM)
    hbm = pl.BlockSpec(memory_space=pl.ANY)
    flops = 2 * ROWS * DIM * (DIM + 3 * FFN)
    return pl.pallas_call(
        functools.partial(mlp_kernel, fb, rt),
        out_shape=(jax.ShapeDtypeStruct((ROWS, DIM), jnp.bfloat16),) + (jax.ShapeDtypeStruct(k_all.shape, jnp.bfloat16),) * 2,
        in_specs=[hbm] * 3 + [vm] + [hbm] * 5,
        out_specs=(hbm, hbm, hbm),
        scratch_shapes=[
            pltpu.VMEM((ROWS, DIM), jnp.bfloat16),
            pltpu.VMEM((ROWS, DIM), jnp.bfloat16),
            pltpu.VMEM((DIM, DIM), jnp.bfloat16),
            pltpu.VMEM((ROWS, DIM), jnp.float32),
            pltpu.VMEM((ROWS, DIM), jnp.bfloat16),
            pltpu.VMEM((rt, fb), jnp.bfloat16),
            pltpu.VMEM((2, DIM, fb), jnp.bfloat16),
            pltpu.VMEM((2, DIM, fb), jnp.bfloat16),
            pltpu.VMEM((2, fb, DIM), jnp.bfloat16),
            pltpu.VMEM((2, 4 * ROWS, 128), jnp.bfloat16),
            pltpu.SemaphoreType.DMA((2, 3)),
            pltpu.SemaphoreType.DMA((2, 2)),
            pltpu.SemaphoreType.DMA((3, 4)),
            pltpu.SemaphoreType.DMA((ROWS // rt,)),
        ],
        compiler_params=pltpu.CompilerParams(vmem_limit_bytes=60 << 20),
        cost_estimate=pl.CostEstimate(flops=flops, bytes_accessed=3 * DIM * FFN * 2, transcendentals=ROWS * FFN),
        name="mlp_block",
    )(o, x, w_out, gain, wg, wu, wd, k_all, v_all)


HEAD_DIM = 128
ROPE_THETA = 500000
SCALE_LOG2E = 1.4426950408889634 * HEAD_DIM ** -0.5
NEG = -2.0e38
QB = 512
KC = 512
PC = 64
FOREIGN = 2
TRI, REAL, BOTH, NONE, FREE = range(5)
MESH = pl.DeviceIdType.MESH


def schedules():
    def code(st, kb, b):
        return (st * 8 + kb) * 8 + b

    a_masked = [code(3 * tb + p, tb, BOTH if tb == 0 else TRI) for tb in range(4) for p in range(3)]
    a_masked += [code(3 * tb + p, 0, REAL) for tb in range(1, 4) for p in range(3)]
    a_plain = [code(3 * tb + p, kb, FREE) for tb in range(2, 4) for kb in range(1, tb) for p in range(3)]
    a_masked += [a_plain.pop(0), *[a_plain[-1] - FREE + NONE] * 2]
    pairs = {tb: 2 if tb < FOREIGN else 3 for tb in range(4)}
    b_masked = [code(3 * tb + p, 4 + tb, TRI) for tb in range(4) for p in range(pairs[tb])]
    b_plain = [code(3 * tb + p, 4 + kb, FREE) for tb in range(1, 4) for kb in range(tb) for p in range(pairs[tb])]
    b_masked += [b_plain.pop(0), b_plain[-1] - FREE + NONE]
    b_real = [code(3 * tb + p, 0, REAL) for tb in range(4) for p in range(pairs[tb])]
    b_far = [code(3 * tb + p, kb, FREE) for tb in range(4) for kb in range(1, 4) for p in range(pairs[tb])]
    b_real += [b_far.pop(0), b_far.pop(0)]
    foreign = []
    for tb in range(FOREIGN):
        run = [code(12 + tb, 0, REAL)] + [code(12 + tb, kb, FREE) for kb in range(1, 4 + tb)] + [code(12 + tb, 4 + tb, TRI)]
        foreign.append(run + [code(12 + tb, 4 + tb, NONE)] * (-len(run) % 4))
    for run in (a_masked, a_plain, b_masked, b_plain, b_real, b_far, *foreign):
        assert len(run) % 4 == 0
    return a_masked, a_plain, b_masked, b_plain, b_real, b_far, foreign


def packed(runs):
    words = ([], [], [], [])
    for run in runs:
        for j in range(0, len(run), 4):
            ahead = [run[min(j + k, len(run) - 1)] for k in range(6)]
            for w in range(3):
                words[w].append(ahead[2 * w] + 1024 * ahead[2 * w + 1])
            words[3].append(run[max(j - 1, 0)])
    return words


def lookup(i, values):
    if len(values) == 1:
        return values[0]
    if all(v == values[0] for v in values):
        return values[0]
    half = len(values) // 2
    return jnp.where(i < half, lookup(i, values[:half]), lookup(i - half, values[half:]))


def flash_run(groups, words_fn, biased, me_c, q_buf, kv, vt, acc, m_s, l_s, s_buf, p_buf, top_s, decay_s, bias):
    def fields(code):
        return lax.div(code, 64), lax.rem(lax.div(code, 8), 8), lax.rem(code, 8)

    def split(word):
        return [lax.rem(word, 1024), lax.div(word, 1024)]

    def scores(code, slot):
        st, kb, b = fields(code)
        tb = lax.div(st, 3)
        own = st < 12
        place = jnp.where(own, jnp.where(lax.div(tb, 2) == me_c, me_c, 2), 3)
        entry = jnp.where(own, lax.rem(tb, 2) * 3 + lax.rem(st, 3), st - 12)
        k_off = pl.multiple_of(lax.rem(kb, 2) * QB, QB)
        for u in range(2):
            q_blk = q_buf[place, entry, u]
            top = jnp.full((8, QB), NEG, jnp.float32)
            for k0 in range(0, QB, KC):
                k_blk = kv[lax.div(kb, 2), me_c, 0, pl.ds(k_off + k0, KC), :]
                s = lax.dot_general(k_blk, q_blk, (((1,), (1,)), ((), ())), preferred_element_type=jnp.float32)
                if biased:
                    s = s + bias[b, k0:k0 + KC, :]
                s_buf[slot % 4, u, k0:k0 + KC, :] = s
                top = jnp.maximum(top, jnp.max(s.reshape(KC // 8, 8, QB), axis=0))
                yield
            top_s[slot % 4, u] = top

    def weights(code, slot):
        st = fields(code)[0]
        for u in range(2):
            m_prev = m_s[st, u]
            m_new = jnp.maximum(m_prev, jnp.max(top_s[slot % 4, u], axis=0, keepdims=True))
            m8 = jnp.broadcast_to(m_new, (8, QB))
            total = jnp.zeros((8, QB), jnp.float32)
            for k0 in range(0, QB, PC):
                s = s_buf[slot % 4, u, k0:k0 + PC, :].reshape(PC // 8, 8, QB)
                p = jnp.exp2((s - m8[None]) * SCALE_LOG2E)
                total = total + jnp.sum(p, axis=0)
                p_buf[slot % 2, u, k0:k0 + PC, :] = p.reshape(PC, QB).astype(jnp.bfloat16)
                if (k0 + PC) % KC == 0:
                    yield
            decay = jnp.exp2((m_prev - m_new) * SCALE_LOG2E)
            decay_s[slot % 2, u] = decay
            l_s[st, u] = l_s[st, u] * decay + jnp.sum(total, axis=0, keepdims=True)
            m_s[st, u] = m_new

    def values(code, slot):
        st, kb, _ = fields(code)
        k_off = pl.multiple_of(lax.rem(kb, 2) * QB, QB)
        for u in range(2):
            pv = jnp.dot(vt[lax.div(kb, 2), :, pl.ds(k_off, QB)], p_buf[slot % 2, u], preferred_element_type=jnp.float32)
            acc[st, u] = acc[st, u] * decay_s[slot % 2, u] + pv
            for _ in range(QB // KC):
                yield

    def together(*parts):
        for _ in itertools.zip_longest(*parts):
            pass

    @pl.when(groups > 0)
    def _():
        p_buf[1] = jnp.zeros_like(p_buf[1])
        decay_s[1] = jnp.ones_like(decay_s[1])
        first = split(words_fn(0)[0])
        together(scores(first[0], 0))
        together(scores(first[1], 1))

        def step(j, _):
            words = words_fn(j)
            codes = [words[3]] + split(words[0]) + split(words[1]) + split(words[2])
            for k in range(4):
                together(weights(codes[k + 1], k), scores(codes[k + 3], k + 2), values(codes[k], k + 1))
            return 0

        lax.fori_loop(0, groups, step, 0)
        together(values(split(words_fn(groups - 1)[1])[1], 1))


def attn_kernel(pos_ref, freq_ref, x_ref, gain_ref, wk_ref, wv_ref, wq_hbm, out_ref, kc_ref, vc_ref,
                wq_ref, cos_s, sin_s, h_buf, q_buf, kv, vt, acc, m_s, l_s, s_buf, p_buf, top_s, decay_s, bias, o_buf,
                send_sem, recv_sem, qsend_sem, qrecv_sem, osend_sem, orecv_sem, cache_sem, ocopy_sem, wq_sem):
    me = lax.axis_index("sp")
    x = me // 2
    c = lax.rem(me, 2)
    partner = 2 * x + (1 - c)
    cross = 2 * (1 - x) + c
    diag = 2 * (1 - x) + (1 - c)
    pad = me * ROWS + (ROWS - 1) - pos_ref[ROWS - 1]
    a_masked, a_plain, b_masked, b_plain, b_real, b_far, foreign = schedules()

    wq_copy = pltpu.make_async_copy(wq_hbm, wq_ref, wq_sem.at[0])
    wq_copy.start()
    barrier = pltpu.get_barrier_semaphore()
    for peer in (partner, cross, diag):
        pl.semaphore_signal(barrier, inc=1, device_id={"sp": peer}, device_id_type=MESH)

    gain = gain_ref[...].reshape(1, DIM).astype(jnp.float32)
    lane = lax.broadcasted_iota(jnp.int32, (256, 128), 1)

    def angle_rows(r):
        rows = pl.ds(r * 256, 256)
        row = lax.broadcasted_iota(jnp.int32, (256, 128), 0) + (me * ROWS + r * 256 - pad)
        ang = jnp.maximum(row, -1).astype(jnp.float32) * freq_ref[...]
        turns = jnp.floor(ang * 0.6366197723675814 + 0.5)
        red = ((ang - turns * 1.5703125) - turns * 4.837512969970703125e-4) - turns * 7.54978995489188216e-8
        sq = red * red
        sin_p = ((-1.9515295891e-4 * sq + 8.3321608736e-3) * sq - 1.6666654611e-1) * sq * red + red
        cos_p = ((2.443315711809948e-5 * sq - 1.388731625493765e-3) * sq + 4.166664568298827e-2) * sq * sq - 0.5 * sq + 1.0
        quad = (turns.astype(jnp.int32) + jnp.where(lane < 64, 0, 3)) & 3
        val = jnp.where((quad & 1) == 0, cos_p, sin_p)
        val = jnp.where((quad == 1) | (quad == 2), -val, val)
        swapped = pltpu.roll(val, 64, 1)
        cos_s[rows, :] = jnp.where(lane < 64, val, swapped)
        sin_s[rows, :] = jnp.where(lane < 64, -swapped, val)

    def rope(t, rows):
        return (t * cos_s[rows, :] + pltpu.roll(t, 64, 1) * sin_s[rows, :]).astype(jnp.bfloat16)

    for r in range(ROWS // 256):
        rows = pl.ds(r * 256, 256)
        angle_rows(r)
        xf = x_ref[rows, :].astype(jnp.float32)
        ms = jnp.mean(xf * xf, axis=-1, keepdims=True)
        h = (xf * lax.rsqrt(ms + NORM_EPS) * gain).astype(jnp.bfloat16)
        h_buf[rows, :] = h
        k = jnp.dot(h, wk_ref[...], preferred_element_type=jnp.float32)
        v = jnp.dot(h, wv_ref[...], preferred_element_type=jnp.float32).astype(jnp.bfloat16)
        for g in range(2):
            kv[me, g, 0, rows, :] = rope(k[:, g * 128:(g + 1) * 128], rows)
            kv[me, g, 1, rows, :] = v[:, g * 128:(g + 1) * 128]

    pl.semaphore_wait(barrier, 3)

    def kv_copy(src, g, i, peer):
        return pltpu.make_async_remote_copy(src_ref=kv.at[src, g], dst_ref=kv.at[src, g], send_sem=send_sem.at[i], recv_sem=recv_sem.at[i],
                                            device_id={"sp": peer}, device_id_type=MESH)

    to_cross = kv_copy(me, c, 0, cross)
    to_cross.start()
    to_diag = kv_copy(me, 1 - c, 1, diag)
    to_diag.start()
    to_partner = [kv_copy(me, g, 2 + g, partner) for g in range(2)]
    for cp in to_partner:
        cp.start()

    def q_rows(t):
        def body(r, _):
            rows = pl.ds(pl.multiple_of(t * QB + r * 256, 256), 256)
            inner = pl.ds(pl.multiple_of(r * 256, 256), 256)
            part = t * 2 + r
            k_rows = pl.ds(pl.multiple_of(part * 128, 128), 128)
            k_idx = lax.broadcasted_iota(jnp.int32, (128, QB), 0) + part * 128
            tri = k_idx <= lax.broadcasted_iota(jnp.int32, (128, QB), 1)
            real = k_idx >= pad
            bias[TRI, k_rows, :] = jnp.where(tri, 0.0, NEG)
            bias[REAL, k_rows, :] = jnp.where(real, 0.0, NEG)
            bias[BOTH, k_rows, :] = jnp.where(tri & real, 0.0, NEG)
            bias[NONE, k_rows, :] = jnp.full((128, QB), NEG, jnp.float32)
            bias[FREE, k_rows, :] = jnp.zeros((128, QB), jnp.float32)
            acc[:, :, pl.ds(pl.multiple_of(part * 32, 32), 32), :] = jnp.zeros((12 + FOREIGN, 2, 32, QB), jnp.float32)
            q = jnp.dot(h_buf[rows, :], wq_ref[...], preferred_element_type=jnp.float32)
            for h in range(12):
                q_buf[h // 6, t * 3 + (h % 6) // 2, h % 2, inner, :] = rope(q[:, h * 128:(h + 1) * 128], rows)
            return 0

        lax.fori_loop(0, 2, body, 0)

    def foreign_q(t, g, peer):
        ft = 2 * c + t
        return pltpu.make_async_remote_copy(src_ref=q_buf.at[g, t * 3 + 2], dst_ref=q_buf.at[3, ft], send_sem=qsend_sem.at[t, g],
                                            recv_sem=qrecv_sem.at[ft], device_id={"sp": peer}, device_id_type=MESH)

    def send_foreign(t):
        @pl.when((x == 1) & (2 * c + t < FOREIGN))
        def _():
            foreign_q(t, c, cross).start()
            foreign_q(t, 1 - c, diag).start()

    wq_copy.wait()
    def q_copy(t):
        half = pl.ds(t * 3, 3)
        return pltpu.make_async_remote_copy(src_ref=q_buf.at[1 - c, half], dst_ref=q_buf.at[2, half], send_sem=send_sem.at[6 + t], recv_sem=recv_sem.at[6 + t],
                                            device_id={"sp": partner}, device_id_type=MESH)

    for t in range(2):
        q_rows(t)
        send_foreign(t)
        q_copy(t).start()

    def flip(src):
        vt[src] = kv[src, c, 1].T

    def cache_copy(src, i):
        rows = pl.ds(pl.multiple_of(src * ROWS, ROWS), ROWS)
        return (pltpu.make_async_copy(kv.at[src, x, 0], kc_ref.at[rows, :], cache_sem.at[i, 0]),
                pltpu.make_async_copy(kv.at[src, x, 1], vc_ref.at[rows, :], cache_sem.at[i, 1]))

    for cp in cache_copy(me, 0):
        cp.start()
    flip(me)
    m_s[...] = jnp.full_like(m_s, NEG)
    l_s[...] = jnp.zeros_like(l_s)
    for cp in to_partner:
        cp.wait_recv()
    for cp in cache_copy(partner, 1):
        cp.start()
    flip(partner)
    for t in range(2):
        q_copy(t).wait_recv()

    def by_chip(a, b):
        return jnp.where(x == 0, a, b)

    def flash(a_groups, a_words, a_start, b_run, biased):
        b_words = packed([b_run])

        def words_fn(j):
            return [by_chip(lookup(j + a_start, a), lookup(j, b)) for a, b in zip(a_words, b_words)]

        flash_run(by_chip(a_groups, len(b_run) // 4), words_fn, biased, c, q_buf, kv, vt, acc, m_s, l_s, s_buf, p_buf, top_s, decay_s, bias)

    flash(len(a_masked) // 4, packed([a_masked]), 0, b_masked, True)
    flash(len(a_plain) // 4, packed([a_plain]), 0, b_plain, False)

    def o_place(t, col):
        return out_ref.at[pl.ds(pl.multiple_of(t * QB, QB), QB), pl.ds(pl.multiple_of(col * 256, 256), 256)]

    def o_send(st, t, col, peer):
        return pltpu.make_async_remote_copy(src_ref=o_buf.at[st], dst_ref=o_place(t, col), send_sem=osend_sem.at[st], recv_sem=orecv_sem.at[t, col],
                                            device_id={"sp": peer}, device_id_type=MESH)

    def o_keep(st, t, col):
        return pltpu.make_async_copy(o_buf.at[st], o_place(t, col), ocopy_sem.at[t, lax.rem(col, 3)])

    def finish(st):
        q_idx = lax.broadcasted_iota(jnp.int32, (1, QB), 1) + (x * 2 * ROWS + (st // 3) * QB)
        for u in range(2):
            inv = jnp.where(q_idx >= pad, 1.0 / l_s[st, u], 0.0)
            o_buf[st, :, u * 128:(u + 1) * 128] = (acc[st, u] * inv).T.astype(jnp.bfloat16)

    def here(tb, pair):
        return (x == 0) | (pair < 2) | (tb >= FOREIGN)

    def finish_own(j, _):
        half = jnp.where(j < 6, 1 - c, c)
        t = lax.rem(j, 6) // 3
        pair = lax.rem(j, 3)
        tb = 2 * half + t
        st = 3 * tb + pair

        @pl.when(here(tb, pair))
        def _():
            finish(st)

            @pl.when(j < 6)
            def _():
                o_send(st, t, 3 * c + pair, partner).start()

            @pl.when(j >= 6)
            def _():
                o_keep(st, t, 3 * c + pair).start()

        return 0

    @pl.when(x == 0)
    def _():
        lax.fori_loop(0, 12, finish_own, 0)

    def arrived(src, i):
        kv_copy(src, c, i, cross).wait_recv()
        kv_copy(src, c, 4 + i, partner).start()
        flip(src)

    arrived(cross, 0)
    arrived(diag, 1)

    f_len = [len(run) // 4 for run in foreign]
    f_start = [sum(f_len[:k]) for k in range(FOREIGN)]

    def far_round(j, _):
        @pl.when(x == 0)
        def _():
            pltpu.make_async_remote_copy(src_ref=q_buf.at[0, 2], dst_ref=q_buf.at[3, j], send_sem=qsend_sem.at[0, 0],
                                         recv_sem=qrecv_sem.at[j], device_id={"sp": cross}, device_id_type=MESH).wait_recv()

        flash(lookup(j, f_len), packed(foreign), lookup(j, f_start), b_real, True)

        @pl.when(x == 0)
        def _():
            finish(12 + j)
            o_send(12 + j, lax.rem(j, 2), 3 * c + 2, 2 + j // 2).start()

        return 0

    lax.fori_loop(0, by_chip(FOREIGN, 1), far_round, 0)
    for sem, src, i in ((4, diag, 3), (5, cross, 2)):
        kv_copy(src, 1 - c, sem, partner).wait_recv()
        for cp in cache_copy(src, i):
            cp.start()
    flash(0, packed([b_far]), 0, b_far, False)

    @pl.when(x == 1)
    def _():
        lax.fori_loop(0, 12, finish_own, 0)

    to_cross.wait_send()
    to_diag.wait_send()
    for cp in to_partner:
        cp.wait_send()
    for i, src in enumerate((cross, diag)):
        kv_copy(src, c, 4 + i, partner).wait_send()
    for t in range(2):
        q_copy(t).wait_send()
    for i, src in enumerate((me, partner, cross, diag)):
        for cp in cache_copy(src, i):
            cp.wait()
    for t in range(2):
        @pl.when((x == 1) & (2 * c + t < FOREIGN))
        def _():
            foreign_q(t, c, cross).wait_send()
            foreign_q(t, 1 - c, diag).wait_send()

        for pair in range(3):
            mine = here(2 * c + t, pair)
            theirs = here(2 * (1 - c) + t, pair)

            @pl.when(mine)
            def _():
                o_keep(0, t, 3 * c + pair).wait()

            @pl.when(jnp.logical_not(mine))
            def _():
                o_send(0, t, 3 * c + pair, cross).wait_recv()

            o_send(0, t, 3 * (1 - c) + pair, partner).wait_recv()

            @pl.when(theirs)
            def _():
                o_send(3 * (2 * (1 - c) + t) + pair, t, 3 * c + pair, partner).wait_send()

    @pl.when(x == 0)
    def _():
        for ft in range(FOREIGN):
            o_send(12 + ft, ft % 2, 3 * c + 2, 2 + ft // 2).wait_send()


def attn_call(positions, freq, x, gain, w_query, w_key, w_value):
    vm = pl.BlockSpec(memory_space=pltpu.VMEM)
    hbm = pl.BlockSpec(memory_space=pl.ANY)
    flops = 2 * ROWS * DIM * 2048 + 4 * 128 * 3 * 4096 * 2048
    bf, f32 = jnp.bfloat16, jnp.float32
    dma = pltpu.SemaphoreType.DMA
    return pl.pallas_call(
        attn_kernel,
        out_shape=(jax.ShapeDtypeStruct((ROWS, DIM), bf), jax.ShapeDtypeStruct((4 * ROWS, 128), bf), jax.ShapeDtypeStruct((4 * ROWS, 128), bf)),
        in_specs=[pl.BlockSpec(memory_space=pltpu.SMEM)] + [vm] * 5 + [hbm],
        out_specs=(hbm, hbm, hbm),
        scratch_shapes=[
            pltpu.VMEM((DIM, DIM), bf),
            pltpu.VMEM((ROWS, 128), f32),
            pltpu.VMEM((ROWS, 128), f32),
            pltpu.VMEM((ROWS, DIM), bf),
            pltpu.VMEM((4, 6, 2, QB, 128), bf),
            pltpu.VMEM((4, 2, 2, ROWS, 128), bf),
            pltpu.VMEM((4, 128, ROWS), bf),
            pltpu.VMEM((12 + FOREIGN, 2, 128, QB), f32),
            pltpu.VMEM((12 + FOREIGN, 2, 1, QB), f32),
            pltpu.VMEM((12 + FOREIGN, 2, 1, QB), f32),
            pltpu.VMEM((4, 2, QB, QB), f32),
            pltpu.VMEM((2, 2, QB, QB), bf),
            pltpu.VMEM((4, 2, 8, QB), f32),
            pltpu.VMEM((2, 2, 1, QB), f32),
            pltpu.VMEM((5, QB, QB), f32),
            pltpu.VMEM((12 + FOREIGN, QB, 256), bf),
            dma((8,)), dma((8,)), dma((2, 2)), dma((FOREIGN,)), dma((12 + FOREIGN,)), dma((2, 6)), dma((4, 2)), dma((2, 3)), dma((1,)),
        ],
        compiler_params=pltpu.CompilerParams(vmem_limit_bytes=62 << 20, collective_id=0, has_side_effects=True),
        cost_estimate=pl.CostEstimate(flops=flops, bytes_accessed=20 << 20, transcendentals=3 * 4096 * 2048),
        name="attn_block",
    )(positions, freq, x, gain, w_key, w_value, w_query)


def solution(mesh):
    freq = 1.0 / (ROPE_THETA ** (np.arange(0, HEAD_DIM, 2, dtype=np.float64) / HEAD_DIM))
    freq = np.concatenate([freq, freq]).astype(np.float32).reshape(1, HEAD_DIM)

    def layer_shard(hidden, positions, attn_gain, w_query, w_key, w_value, w_out, mlp_gain, w_gate, w_up, w_down):
        attn, k_all, v_all = attn_call(positions, jnp.asarray(freq), hidden, attn_gain, w_query, w_key, w_value)
        hidden_out, k_cache, v_cache = mlp_call(attn, hidden, w_out, mlp_gain, w_gate, w_up, w_down, k_all, v_all)
        return hidden_out, k_cache.reshape(4 * ROWS, 1, HEAD_DIM), v_cache.reshape(4 * ROWS, 1, HEAD_DIM)

    row_spec = P(("dp", "sp"), None)
    cache_spec = P("dp", "sp", None)
    return jax.shard_map(layer_shard, mesh=mesh, in_specs=(row_spec, P(("dp", "sp")), P(), P(), P(), P(), P(), P(), P(), P(), P()), out_specs=(row_spec, cache_spec, cache_spec), check_vma=False)
```

```python
import functools
import itertools
import jax
import jax.numpy as jnp
import numpy as np
from jax import lax
from jax.experimental import pallas as pl
from jax.experimental.pallas import tpu as pltpu
from jax.sharding import PartitionSpec as P

ROWS = 1024
DIM = 1536
FFN = 8960
NORM_EPS = 1e-5


def mlp_kernel(fb, rt, o_hbm, x_hbm, wout_hbm, gain_ref, wg_hbm, wu_hbm, wd_hbm, k_in, v_in, out_hbm, k_out, v_out, o_ref, x_ref, wout_ref, acc, g_buf, m_buf, wg, wu, wd, c_buf, sems, c_sems, in_sems, out_sems):
    steps = FFN // fb

    def copies(j, slot):
        off = pl.multiple_of(j * fb, 128)
        return (
            pltpu.make_async_copy(wg_hbm.at[:, pl.ds(off, fb)], wg.at[slot], sems.at[slot, 0]),
            pltpu.make_async_copy(wu_hbm.at[:, pl.ds(off, fb)], wu.at[slot], sems.at[slot, 1]),
            pltpu.make_async_copy(wd_hbm.at[pl.ds(off, fb), :], wd.at[slot], sems.at[slot, 2]),
        )

    wout_copy = pltpu.make_async_copy(wout_hbm, wout_ref, in_sems.at[2, 0])
    wout_copy.start()

    def row_copies(r):
        rows = pl.ds(r * 256, 256)
        return (pltpu.make_async_copy(o_hbm.at[rows, :], o_ref.at[rows, :], in_sems.at[0, r]),
                pltpu.make_async_copy(x_hbm.at[rows, :], x_ref.at[rows, :], in_sems.at[1, r]))

    for r in range(ROWS // 256):
        for c in row_copies(r):
            c.start()
    for c in copies(0, 0):
        c.start()

    cache = ((k_in, k_out), (v_in, v_out))
    for i in range(2):
        pltpu.make_async_copy(cache[i][0], c_buf.at[i], c_sems.at[0, i]).start()
    gain = gain_ref[...].reshape(1, DIM).astype(jnp.float32)

    wout_copy.wait()

    def proj(half):
        for r in (2 * half, 2 * half + 1):
            for c in row_copies(r):
                c.wait()
        for r in range(2 * half, 2 * half + 2):
            rows = pl.ds(r * 256, 256)
            y = x_ref[rows, :].astype(jnp.float32) + jnp.dot(o_ref[rows, :], wout_ref[...], preferred_element_type=jnp.float32)
            y = y.astype(jnp.bfloat16).astype(jnp.float32)
            acc[rows, :] = y
            ms = jnp.mean(y * y, axis=-1, keepdims=True)
            g_buf[rows, :] = (y * lax.rsqrt(ms + NORM_EPS) * gain).astype(jnp.bfloat16)

    proj(0)
    proj(1)
    for i in range(2):
        pltpu.make_async_copy(cache[i][0], c_buf.at[i], c_sems.at[0, i]).wait()
        pltpu.make_async_copy(c_buf.at[i], cache[i][1], c_sems.at[1, i]).start()

    def step(j, _):
        slot = lax.rem(j, 2)
        for c in copies(j, slot):
            c.wait()

        @pl.when(j + 1 < steps)
        def _():
            for c in copies(j + 1, 1 - slot):
                c.start()

        def tile(r, _):
            rows = pl.ds(pl.multiple_of(r * rt, rt), rt)
            for c0 in range(0, fb, 256):
                cols = pl.ds(c0, 256)
                gate = jnp.dot(g_buf[rows, :], wg[slot, :, cols], preferred_element_type=jnp.float32)
                up = jnp.dot(g_buf[rows, :], wu[slot, :, cols], preferred_element_type=jnp.float32)
                m_buf[:, cols] = (gate / (1.0 + jnp.exp(-gate)) * up).astype(jnp.bfloat16)
            acc[rows, :] += jnp.dot(m_buf[...], wd[slot], preferred_element_type=jnp.float32)

            @pl.when(j == steps - 1)
            def _():
                def fin(q, _):
                    part = pl.ds(pl.multiple_of(r * rt + q * 128, 128), 128)
                    o_ref[part, :] = acc[part, :].astype(jnp.bfloat16)
                    return 0

                lax.fori_loop(0, rt // 128, fin, 0)
                pltpu.make_async_copy(o_ref.at[rows, :], out_hbm.at[rows, :], out_sems.at[r]).start()

            return 0

        lax.fori_loop(0, ROWS // rt, tile, 0)
        return 0

    lax.fori_loop(0, steps, step, 0)

    for r in range(ROWS // rt):
        rows = pl.ds(r * rt, rt)
        pltpu.make_async_copy(o_ref.at[rows, :], out_hbm.at[rows, :], out_sems.at[r]).wait()
    for i in range(2):
        pltpu.make_async_copy(c_buf.at[i], cache[i][1], c_sems.at[1, i]).wait()


def mlp_call(o, x, w_out, gain, wg, wu, wd, k_all, v_all, fb=1280, rt=512):
    vm = pl.BlockSpec(memory_space=pltpu.VMEM)
    hbm = pl.BlockSpec(memory_space=pl.ANY)
    flops = 2 * ROWS * DIM * (DIM + 3 * FFN)
    return pl.pallas_call(
        functools.partial(mlp_kernel, fb, rt),
        out_shape=(jax.ShapeDtypeStruct((ROWS, DIM), jnp.bfloat16),) + (jax.ShapeDtypeStruct(k_all.shape, jnp.bfloat16),) * 2,
        in_specs=[hbm] * 3 + [vm] + [hbm] * 5,
        out_specs=(hbm, hbm, hbm),
        scratch_shapes=[
            pltpu.VMEM((ROWS, DIM), jnp.bfloat16),
            pltpu.VMEM((ROWS, DIM), jnp.bfloat16),
            pltpu.VMEM((DIM, DIM), jnp.bfloat16),
            pltpu.VMEM((ROWS, DIM), jnp.float32),
            pltpu.VMEM((ROWS, DIM), jnp.bfloat16),
            pltpu.VMEM((rt, fb), jnp.bfloat16),
            pltpu.VMEM((2, DIM, fb), jnp.bfloat16),
            pltpu.VMEM((2, DIM, fb), jnp.bfloat16),
            pltpu.VMEM((2, fb, DIM), jnp.bfloat16),
            pltpu.VMEM((2, 4 * ROWS, 128), jnp.bfloat16),
            pltpu.SemaphoreType.DMA((2, 3)),
            pltpu.SemaphoreType.DMA((2, 2)),
            pltpu.SemaphoreType.DMA((3, 4)),
            pltpu.SemaphoreType.DMA((ROWS // rt,)),
        ],
        compiler_params=pltpu.CompilerParams(vmem_limit_bytes=60 << 20),
        cost_estimate=pl.CostEstimate(flops=flops, bytes_accessed=3 * DIM * FFN * 2, transcendentals=ROWS * FFN),
        name="mlp_block",
    )(o, x, w_out, gain, wg, wu, wd, k_all, v_all)


HEAD_DIM = 128
ROPE_THETA = 500000
SCALE_LOG2E = 1.4426950408889634 * HEAD_DIM ** -0.5
NEG = -2.0e38
QB = 512
KC = 512
PC = 64
MOVED = ((0, 2), (1, 2), (0, 1))
FOREIGN = len(MOVED)
TRI, REAL, BOTH, NONE, FREE = range(5)
MESH = pl.DeviceIdType.MESH


def schedules():
    def code(st, kb, b):
        return (st * 8 + kb) * 8 + b

    a_masked = [code(3 * tb + p, tb, BOTH if tb == 0 else TRI) for tb in range(4) for p in range(3)]
    a_masked += [code(3 * tb + p, 0, REAL) for tb in range(1, 4) for p in range(3)]
    a_plain = [code(3 * tb + p, kb, FREE) for tb in range(2, 4) for kb in range(1, tb) for p in range(3)]
    a_masked += [a_plain.pop(0), *[a_plain[-1] - FREE + NONE] * 2]
    pairs = {tb: [p for p in range(3) if (tb, p) not in MOVED] for tb in range(4)}
    b_masked = [code(3 * tb + p, 4 + tb, TRI) for tb in range(4) for p in pairs[tb]]
    b_plain = [code(3 * tb + p, 4 + kb, FREE) for tb in range(1, 4) for kb in range(tb) for p in pairs[tb]]
    b_masked += [b_plain.pop(0), *[b_plain[-1] - FREE + NONE] * 2]
    b_real = [code(3 * tb + p, 0, REAL) for tb in range(4) for p in pairs[tb]]
    b_far = [code(3 * tb + p, kb, FREE) for tb in range(4) for kb in range(1, 4) for p in pairs[tb]]
    b_real += [b_far.pop(0) for _ in range(3)]
    foreign = []
    for f, (tb, _) in enumerate(MOVED):
        run = [code(12 + f, 0, REAL)] + [code(12 + f, kb, FREE) for kb in range(1, 4 + tb)] + [code(12 + f, 4 + tb, TRI)]
        foreign.append(run + [code(12 + f, 4 + tb, NONE)] * (-len(run) % 4))
    for run in (a_masked, a_plain, b_masked, b_plain, b_real, b_far, *foreign):
        assert len(run) % 4 == 0
    return a_masked, a_plain, b_masked, b_plain, b_real, b_far, foreign


def packed(runs):
    words = ([], [], [], [])
    for run in runs:
        for j in range(0, len(run), 4):
            ahead = [run[min(j + k, len(run) - 1)] for k in range(6)]
            for w in range(3):
                words[w].append(ahead[2 * w] + 1024 * ahead[2 * w + 1])
            words[3].append(run[max(j - 1, 0)])
    return words


def lookup(i, values):
    if len(values) == 1:
        return values[0]
    if all(v == values[0] for v in values):
        return values[0]
    half = len(values) // 2
    return jnp.where(i < half, lookup(i, values[:half]), lookup(i - half, values[half:]))


def flash_run(groups, words_fn, biased, me_c, q_buf, kv, vt, acc, m_s, l_s, s_buf, p_buf, top_s, decay_s, bias):
    def fields(code):
        return lax.div(code, 64), lax.rem(lax.div(code, 8), 8), lax.rem(code, 8)

    def split(word):
        return [lax.rem(word, 1024), lax.div(word, 1024)]

    def scores(code, slot):
        st, kb, b = fields(code)
        tb = lax.div(st, 3)
        own = st < 12
        place = jnp.where(own, jnp.where(lax.div(tb, 2) == me_c, me_c, 2), 3)
        entry = jnp.where(own, lax.rem(tb, 2) * 3 + lax.rem(st, 3), st - 12)
        k_off = pl.multiple_of(lax.rem(kb, 2) * QB, QB)
        for u in range(2):
            q_blk = q_buf[place, entry, u]
            top = jnp.full((8, QB), NEG, jnp.float32)
            for k0 in range(0, QB, KC):
                k_blk = kv[lax.div(kb, 2), me_c, 0, pl.ds(k_off + k0, KC), :]
                s = lax.dot_general(k_blk, q_blk, (((1,), (1,)), ((), ())), preferred_element_type=jnp.float32)
                if biased:
                    s = s + bias[b, k0:k0 + KC, :]
                s_buf[slot % 4, u, k0:k0 + KC, :] = s
                top = jnp.maximum(top, jnp.max(s.reshape(KC // 8, 8, QB), axis=0))
                yield
            top_s[slot % 4, u] = top

    def weights(code, slot):
        st = fields(code)[0]
        for u in range(2):
            m_prev = m_s[st, u]
            m_new = jnp.maximum(m_prev, jnp.max(top_s[slot % 4, u], axis=0, keepdims=True))
            m8 = jnp.broadcast_to(m_new, (8, QB))
            total = jnp.zeros((8, QB), jnp.float32)
            for k0 in range(0, QB, PC):
                s = s_buf[slot % 4, u, k0:k0 + PC, :].reshape(PC // 8, 8, QB)
                p = jnp.exp2((s - m8[None]) * SCALE_LOG2E)
                total = total + jnp.sum(p, axis=0)
                p_buf[slot % 2, u, k0:k0 + PC, :] = p.reshape(PC, QB).astype(jnp.bfloat16)
                if (k0 + PC) % KC == 0:
                    yield
            decay = jnp.exp2((m_prev - m_new) * SCALE_LOG2E)
            decay_s[slot % 2, u] = decay
            l_s[st, u] = l_s[st, u] * decay + jnp.sum(total, axis=0, keepdims=True)
            m_s[st, u] = m_new

    def values(code, slot):
        st, kb, _ = fields(code)
        k_off = pl.multiple_of(lax.rem(kb, 2) * QB, QB)
        for u in range(2):
            pv = jnp.dot(vt[lax.div(kb, 2), :, pl.ds(k_off, QB)], p_buf[slot % 2, u], preferred_element_type=jnp.float32)
            acc[st, u] = acc[st, u] * decay_s[slot % 2, u] + pv
            for _ in range(QB // KC):
                yield

    def together(*parts):
        for _ in itertools.zip_longest(*parts):
            pass

    @pl.when(groups > 0)
    def _():
        p_buf[1] = jnp.zeros_like(p_buf[1])
        decay_s[1] = jnp.ones_like(decay_s[1])
        first = split(words_fn(0)[0])
        together(scores(first[0], 0))
        together(scores(first[1], 1))

        def step(j, _):
            words = words_fn(j)
            codes = [words[3]] + split(words[0]) + split(words[1]) + split(words[2])
            for k in range(4):
                together(weights(codes[k + 1], k), scores(codes[k + 3], k + 2), values(codes[k], k + 1))
            return 0

        lax.fori_loop(0, groups, step, 0)
        together(values(split(words_fn(groups - 1)[1])[1], 1))


def attn_kernel(pos_ref, freq_ref, gain_ref, x_hbm, wk_hbm, wv_hbm, wq_hbm, out_ref, kc_ref, vc_ref,
                x_ref, wk_ref, wv_ref, wq_ref, cos_s, sin_s, h_buf, q_buf, kv, vt, acc, m_s, l_s, s_buf, p_buf, top_s, decay_s, bias, o_buf,
                send_sem, recv_sem, qsend_sem, qrecv_sem, osend_sem, orecv_sem, cache_sem, ocopy_sem, wq_sem):
    me = lax.axis_index("sp")
    x = me // 2
    c = lax.rem(me, 2)
    partner = 2 * x + (1 - c)
    cross = 2 * (1 - x) + c
    diag = 2 * (1 - x) + (1 - c)
    pad = me * ROWS + (ROWS - 1) - pos_ref[ROWS - 1]
    a_masked, a_plain, b_masked, b_plain, b_real, b_far, foreign = schedules()

    def x_copy(r):
        rows = pl.ds(r * 256, 256)
        return pltpu.make_async_copy(x_hbm.at[rows, :], x_ref.at[rows, :], wq_sem.at[3 + r])

    wk_copy = pltpu.make_async_copy(wk_hbm, wk_ref, wq_sem.at[1])
    wv_copy = pltpu.make_async_copy(wv_hbm, wv_ref, wq_sem.at[2])
    wq_copy = pltpu.make_async_copy(wq_hbm, wq_ref, wq_sem.at[0])
    for cp in (wk_copy, wv_copy, *[x_copy(r) for r in range(4)], wq_copy):
        cp.start()
    barrier = pltpu.get_barrier_semaphore()
    for peer in (partner, cross, diag):
        pl.semaphore_signal(barrier, inc=1, device_id={"sp": peer}, device_id_type=MESH)

    gain = gain_ref[...].reshape(1, DIM).astype(jnp.float32)
    lane = lax.broadcasted_iota(jnp.int32, (256, 128), 1)

    def angle_rows(r):
        rows = pl.ds(r * 256, 256)
        row = lax.broadcasted_iota(jnp.int32, (256, 128), 0) + (me * ROWS + r * 256 - pad)
        ang = jnp.maximum(row, -1).astype(jnp.float32) * freq_ref[...]
        turns = jnp.floor(ang * 0.6366197723675814 + 0.5)
        red = ((ang - turns * 1.5703125) - turns * 4.837512969970703125e-4) - turns * 7.54978995489188216e-8
        sq = red * red
        sin_p = ((-1.9515295891e-4 * sq + 8.3321608736e-3) * sq - 1.6666654611e-1) * sq * red + red
        cos_p = ((2.443315711809948e-5 * sq - 1.388731625493765e-3) * sq + 4.166664568298827e-2) * sq * sq - 0.5 * sq + 1.0
        quad = (turns.astype(jnp.int32) + jnp.where(lane < 64, 0, 3)) & 3
        val = jnp.where((quad & 1) == 0, cos_p, sin_p)
        val = jnp.where((quad == 1) | (quad == 2), -val, val)
        swapped = pltpu.roll(val, 64, 1)
        cos_s[rows, :] = jnp.where(lane < 64, val, swapped)
        sin_s[rows, :] = jnp.where(lane < 64, -swapped, val)

    def rope(t, rows):
        return (t * cos_s[rows, :] + pltpu.roll(t, 64, 1) * sin_s[rows, :]).astype(jnp.bfloat16)

    for r in range(ROWS // 256):
        angle_rows(r)
    for cp in (wk_copy, wv_copy, *[x_copy(r) for r in range(4)]):
        cp.wait()
    for r in range(ROWS // 256):
        rows = pl.ds(r * 256, 256)
        xf = x_ref[rows, :].astype(jnp.float32)
        ms = jnp.mean(xf * xf, axis=-1, keepdims=True)
        h = (xf * lax.rsqrt(ms + NORM_EPS) * gain).astype(jnp.bfloat16)
        h_buf[rows, :] = h
        k = jnp.dot(h, wk_ref[...], preferred_element_type=jnp.float32)
        v = jnp.dot(h, wv_ref[...], preferred_element_type=jnp.float32).astype(jnp.bfloat16)
        for g in range(2):
            kv[me, g, 0, rows, :] = rope(k[:, g * 128:(g + 1) * 128], rows)
            kv[me, g, 1, rows, :] = v[:, g * 128:(g + 1) * 128]

    pl.semaphore_wait(barrier, 3)

    def kv_copy(src, g, i, peer):
        return pltpu.make_async_remote_copy(src_ref=kv.at[src, g], dst_ref=kv.at[src, g], send_sem=send_sem.at[i], recv_sem=recv_sem.at[i],
                                            device_id={"sp": peer}, device_id_type=MESH)

    to_cross = kv_copy(me, c, 0, cross)
    to_cross.start()
    to_diag = kv_copy(me, 1 - c, 1, diag)
    to_diag.start()
    to_partner = [kv_copy(me, g, 2 + g, partner) for g in range(2)]
    for cp in to_partner:
        cp.start()

    def q_rows(t):
        def body(r, _):
            rows = pl.ds(pl.multiple_of(t * QB + r * 256, 256), 256)
            inner = pl.ds(pl.multiple_of(r * 256, 256), 256)
            part = t * 2 + r
            k_rows = pl.ds(pl.multiple_of(part * 128, 128), 128)
            k_idx = lax.broadcasted_iota(jnp.int32, (128, QB), 0) + part * 128
            tri = k_idx <= lax.broadcasted_iota(jnp.int32, (128, QB), 1)
            real = k_idx >= pad
            bias[TRI, k_rows, :] = jnp.where(tri, 0.0, NEG)
            bias[REAL, k_rows, :] = jnp.where(real, 0.0, NEG)
            bias[BOTH, k_rows, :] = jnp.where(tri & real, 0.0, NEG)
            bias[NONE, k_rows, :] = jnp.full((128, QB), NEG, jnp.float32)
            bias[FREE, k_rows, :] = jnp.zeros((128, QB), jnp.float32)
            acc[:, :, pl.ds(pl.multiple_of(part * 32, 32), 32), :] = jnp.zeros((12 + FOREIGN, 2, 32, QB), jnp.float32)
            q = jnp.dot(h_buf[rows, :], wq_ref[...], preferred_element_type=jnp.float32)
            for h in range(12):
                q_buf[h // 6, t * 3 + (h % 6) // 2, h % 2, inner, :] = rope(q[:, h * 128:(h + 1) * 128], rows)
            return 0

        lax.fori_loop(0, 2, body, 0)

    def foreign_q(f, g, peer):
        tb, p = MOVED[f]
        return pltpu.make_async_remote_copy(src_ref=q_buf.at[g, tb % 2 * 3 + p], dst_ref=q_buf.at[3, f], send_sem=qsend_sem.at[f, g],
                                            recv_sem=qrecv_sem.at[f], device_id={"sp": peer}, device_id_type=MESH)

    def sends_q(f):
        return (x == 1) & (c == MOVED[f][0] // 2)

    wq_copy.wait()
    def q_copy(t):
        half = pl.ds(t * 3, 3)
        return pltpu.make_async_remote_copy(src_ref=q_buf.at[1 - c, half], dst_ref=q_buf.at[2, half], send_sem=send_sem.at[6 + t], recv_sem=recv_sem.at[6 + t],
                                            device_id={"sp": partner}, device_id_type=MESH)

    for t in range(2):
        q_rows(t)
        q_copy(t).start()
    for f in range(FOREIGN):
        @pl.when(sends_q(f))
        def _():
            foreign_q(f, c, cross).start()
            foreign_q(f, 1 - c, diag).start()

    def flip(src):
        vt[src] = kv[src, c, 1].T

    def cache_copy(src, i):
        rows = pl.ds(pl.multiple_of(src * ROWS, ROWS), ROWS)
        return (pltpu.make_async_copy(kv.at[src, x, 0], kc_ref.at[rows, :], cache_sem.at[i, 0]),
                pltpu.make_async_copy(kv.at[src, x, 1], vc_ref.at[rows, :], cache_sem.at[i, 1]))

    for cp in cache_copy(me, 0):
        cp.start()
    flip(me)
    m_s[...] = jnp.full_like(m_s, NEG)
    l_s[...] = jnp.zeros_like(l_s)
    for cp in to_partner:
        cp.wait_recv()
    for cp in cache_copy(partner, 1):
        cp.start()
    flip(partner)
    for t in range(2):
        q_copy(t).wait_recv()

    def by_chip(a, b):
        return jnp.where(x == 0, a, b)

    def flash(a_groups, a_words, a_start, b_run, biased):
        b_words = packed([b_run])

        def words_fn(j):
            return [by_chip(lookup(j + a_start, a), lookup(j, b)) for a, b in zip(a_words, b_words)]

        flash_run(by_chip(a_groups, len(b_run) // 4), words_fn, biased, c, q_buf, kv, vt, acc, m_s, l_s, s_buf, p_buf, top_s, decay_s, bias)

    flash(len(a_masked) // 4, packed([a_masked]), 0, b_masked, True)
    flash(len(a_plain) // 4, packed([a_plain]), 0, b_plain, False)

    def o_place(t, col):
        return out_ref.at[pl.ds(pl.multiple_of(t * QB, QB), QB), pl.ds(pl.multiple_of(col * 256, 256), 256)]

    def o_send(st, t, col, peer):
        return pltpu.make_async_remote_copy(src_ref=o_buf.at[st], dst_ref=o_place(t, col), send_sem=osend_sem.at[st], recv_sem=orecv_sem.at[t, col],
                                            device_id={"sp": peer}, device_id_type=MESH)

    def o_keep(st, t, col):
        return pltpu.make_async_copy(o_buf.at[st], o_place(t, col), ocopy_sem.at[t, lax.rem(col, 3)])

    def finish(st):
        q_idx = lax.broadcasted_iota(jnp.int32, (1, QB), 1) + (x * 2 * ROWS + (st // 3) * QB)
        for u in range(2):
            inv = jnp.where(q_idx >= pad, 1.0 / l_s[st, u], 0.0)
            o_buf[st, :, u * 128:(u + 1) * 128] = (acc[st, u] * inv).T.astype(jnp.bfloat16)

    def here(tb, pair):
        moved = [(tb == m_tb) & (pair == m_pair) for m_tb, m_pair in MOVED]
        return (x == 0) | jnp.logical_not(functools.reduce(jnp.logical_or, moved))

    def finish_own(j, _):
        half = jnp.where(j < 6, 1 - c, c)
        t = lax.rem(j, 6) // 3
        pair = lax.rem(j, 3)
        tb = 2 * half + t
        st = 3 * tb + pair

        @pl.when(here(tb, pair))
        def _():
            finish(st)

            @pl.when(j < 6)
            def _():
                o_send(st, t, 3 * c + pair, partner).start()

            @pl.when(j >= 6)
            def _():
                o_keep(st, t, 3 * c + pair).start()

        return 0

    @pl.when(x == 0)
    def _():
        lax.fori_loop(0, 12, finish_own, 0)

    def arrived(src, i):
        kv_copy(src, c, i, cross).wait_recv()
        kv_copy(src, c, 4 + i, partner).start()
        flip(src)

    arrived(cross, 0)
    arrived(diag, 1)

    f_len = [len(run) // 4 for run in foreign]
    f_start = [sum(f_len[:k]) for k in range(FOREIGN)]

    def far_round(j, _):
        @pl.when(x == 0)
        def _():
            pltpu.make_async_remote_copy(src_ref=q_buf.at[0, 2], dst_ref=q_buf.at[3, j], send_sem=qsend_sem.at[0, 0],
                                         recv_sem=qrecv_sem.at[j], device_id={"sp": cross}, device_id_type=MESH).wait_recv()

        flash(lookup(j, f_len), packed(foreign), lookup(j, f_start), b_real, True)

        @pl.when(x == 0)
        def _():
            finish(12 + j)
            tb = lookup(j, [m[0] for m in MOVED])
            o_send(12 + j, lax.rem(tb, 2), 3 * c + lookup(j, [m[1] for m in MOVED]), 2 + lax.div(tb, 2)).start()

        return 0

    lax.fori_loop(0, by_chip(FOREIGN, 1), far_round, 0)
    for sem, src, i in ((4, diag, 3), (5, cross, 2)):
        kv_copy(src, 1 - c, sem, partner).wait_recv()
        for cp in cache_copy(src, i):
            cp.start()
    flash(0, packed([b_far]), 0, b_far, False)

    @pl.when(x == 1)
    def _():
        lax.fori_loop(0, 12, finish_own, 0)

    to_cross.wait_send()
    to_diag.wait_send()
    for cp in to_partner:
        cp.wait_send()
    for i, src in enumerate((cross, diag)):
        kv_copy(src, c, 4 + i, partner).wait_send()
    for t in range(2):
        q_copy(t).wait_send()
    for i, src in enumerate((me, partner, cross, diag)):
        for cp in cache_copy(src, i):
            cp.wait()
    for f in range(FOREIGN):
        @pl.when(sends_q(f))
        def _():
            foreign_q(f, c, cross).wait_send()
            foreign_q(f, 1 - c, diag).wait_send()

    for t in range(2):
        for pair in range(3):
            mine = here(2 * c + t, pair)
            theirs = here(2 * (1 - c) + t, pair)

            @pl.when(mine)
            def _():
                o_keep(0, t, 3 * c + pair).wait()

            @pl.when(jnp.logical_not(mine))
            def _():
                o_send(0, t, 3 * c + pair, cross).wait_recv()

            o_send(0, t, 3 * (1 - c) + pair, partner).wait_recv()

            @pl.when(theirs)
            def _():
                o_send(3 * (2 * (1 - c) + t) + pair, t, 3 * c + pair, partner).wait_send()

    @pl.when(x == 0)
    def _():
        for f, (tb, p) in enumerate(MOVED):
            o_send(12 + f, tb % 2, 3 * c + p, 2 + tb // 2).wait_send()


def attn_call(positions, freq, x, gain, w_query, w_key, w_value):
    vm = pl.BlockSpec(memory_space=pltpu.VMEM)
    hbm = pl.BlockSpec(memory_space=pl.ANY)
    flops = 2 * ROWS * DIM * 2048 + 4 * 128 * 3 * 4096 * 2048
    bf, f32 = jnp.bfloat16, jnp.float32
    dma = pltpu.SemaphoreType.DMA
    return pl.pallas_call(
        attn_kernel,
        out_shape=(jax.ShapeDtypeStruct((ROWS, DIM), bf), jax.ShapeDtypeStruct((4 * ROWS, 128), bf), jax.ShapeDtypeStruct((4 * ROWS, 128), bf)),
        in_specs=[pl.BlockSpec(memory_space=pltpu.SMEM)] + [vm] * 2 + [hbm] * 4,
        out_specs=(hbm, hbm, hbm),
        scratch_shapes=[
            pltpu.VMEM((ROWS, DIM), bf),
            pltpu.VMEM((DIM, 256), bf),
            pltpu.VMEM((DIM, 256), bf),
            pltpu.VMEM((DIM, DIM), bf),
            pltpu.VMEM((ROWS, 128), f32),
            pltpu.VMEM((ROWS, 128), f32),
            pltpu.VMEM((ROWS, DIM), bf),
            pltpu.VMEM((4, 6, 2, QB, 128), bf),
            pltpu.VMEM((4, 2, 2, ROWS, 128), bf),
            pltpu.VMEM((4, 128, ROWS), bf),
            pltpu.VMEM((12 + FOREIGN, 2, 128, QB), f32),
            pltpu.VMEM((12 + FOREIGN, 2, 1, QB), f32),
            pltpu.VMEM((12 + FOREIGN, 2, 1, QB), f32),
            pltpu.VMEM((4, 2, QB, QB), f32),
            pltpu.VMEM((2, 2, QB, QB), bf),
            pltpu.VMEM((4, 2, 8, QB), f32),
            pltpu.VMEM((2, 2, 1, QB), f32),
            pltpu.VMEM((5, QB, QB), f32),
            pltpu.VMEM((12 + FOREIGN, QB, 256), bf),
            dma((8,)), dma((8,)), dma((FOREIGN, 2)), dma((FOREIGN,)), dma((12 + FOREIGN,)), dma((2, 6)), dma((4, 2)), dma((2, 3)), dma((7,)),
        ],
        compiler_params=pltpu.CompilerParams(vmem_limit_bytes=62 << 20, collective_id=0, has_side_effects=True),
        cost_estimate=pl.CostEstimate(flops=flops, bytes_accessed=20 << 20, transcendentals=3 * 4096 * 2048),
        name="attn_block",
    )(positions, freq, gain, x, w_key, w_value, w_query)


def solution(mesh):
    freq = 1.0 / (ROPE_THETA ** (np.arange(0, HEAD_DIM, 2, dtype=np.float64) / HEAD_DIM))
    freq = np.concatenate([freq, freq]).astype(np.float32).reshape(1, HEAD_DIM)

    def layer_shard(hidden, positions, attn_gain, w_query, w_key, w_value, w_out, mlp_gain, w_gate, w_up, w_down):
        attn, k_all, v_all = attn_call(positions, jnp.asarray(freq), hidden, attn_gain, w_query, w_key, w_value)
        hidden_out, k_cache, v_cache = mlp_call(attn, hidden, w_out, mlp_gain, w_gate, w_up, w_down, k_all, v_all)
        return hidden_out, k_cache.reshape(4 * ROWS, 1, HEAD_DIM), v_cache.reshape(4 * ROWS, 1, HEAD_DIM)

    row_spec = P(("dp", "sp"), None)
    cache_spec = P("dp", "sp", None)
    return jax.shard_map(layer_shard, mesh=mesh, in_specs=(row_spec, P(("dp", "sp")), P(), P(), P(), P(), P(), P(), P(), P(), P()), out_specs=(row_spec, cache_spec, cache_spec), check_vma=False)
```

```python
import functools
import itertools
import jax
import jax.numpy as jnp
import numpy as np
from jax import lax
from jax.experimental import pallas as pl
from jax.experimental.pallas import tpu as pltpu
from jax.sharding import PartitionSpec as P

ROWS = 1024
DIM = 1536
FFN = 8960
NORM_EPS = 1e-5


def mlp_kernel(fb, rt, o_hbm, x_hbm, wout_hbm, gain_ref, wg_hbm, wu_hbm, wd_hbm, k_in, v_in, out_hbm, k_out, v_out, o_ref, x_ref, wout_ref, acc, g_buf, m_buf, wg, wu, wd, c_buf, sems, c_sems, in_sems, out_sems):
    steps = FFN // fb

    def copies(j, slot):
        off = pl.multiple_of(j * fb, 128)
        return (
            pltpu.make_async_copy(wg_hbm.at[:, pl.ds(off, fb)], wg.at[slot], sems.at[slot, 0]),
            pltpu.make_async_copy(wu_hbm.at[:, pl.ds(off, fb)], wu.at[slot], sems.at[slot, 1]),
            pltpu.make_async_copy(wd_hbm.at[pl.ds(off, fb), :], wd.at[slot], sems.at[slot, 2]),
        )

    wout_copy = pltpu.make_async_copy(wout_hbm, wout_ref, in_sems.at[2, 0])
    wout_copy.start()

    def row_copies(r):
        rows = pl.ds(r * 256, 256)
        return (pltpu.make_async_copy(o_hbm.at[rows, :], o_ref.at[rows, :], in_sems.at[0, r]),
                pltpu.make_async_copy(x_hbm.at[rows, :], x_ref.at[rows, :], in_sems.at[1, r]))

    for r in range(ROWS // 256):
        for c in row_copies(r):
            c.start()
    for c in copies(0, 0):
        c.start()

    cache = ((k_in, k_out), (v_in, v_out))
    for i in range(2):
        pltpu.make_async_copy(cache[i][0], c_buf.at[i], c_sems.at[0, i]).start()
    gain = gain_ref[...].reshape(1, DIM).astype(jnp.float32)

    wout_copy.wait()

    def proj(half):
        for r in (2 * half, 2 * half + 1):
            for c in row_copies(r):
                c.wait()
        for r in range(2 * half, 2 * half + 2):
            rows = pl.ds(r * 256, 256)
            y = x_ref[rows, :].astype(jnp.float32) + jnp.dot(o_ref[rows, :], wout_ref[...], preferred_element_type=jnp.float32)
            y = y.astype(jnp.bfloat16).astype(jnp.float32)
            acc[rows, :] = y
            ms = jnp.mean(y * y, axis=-1, keepdims=True)
            g_buf[rows, :] = (y * lax.rsqrt(ms + NORM_EPS) * gain).astype(jnp.bfloat16)

    proj(0)
    proj(1)
    for i in range(2):
        pltpu.make_async_copy(cache[i][0], c_buf.at[i], c_sems.at[0, i]).wait()
        pltpu.make_async_copy(c_buf.at[i], cache[i][1], c_sems.at[1, i]).start()

    def step(j, _):
        slot = lax.rem(j, 2)
        for c in copies(j, slot):
            c.wait()

        @pl.when(j + 1 < steps)
        def _():
            for c in copies(j + 1, 1 - slot):
                c.start()

        def tile(r, _):
            rows = pl.ds(pl.multiple_of(r * rt, rt), rt)
            for c0 in range(0, fb, 256):
                cols = pl.ds(c0, 256)
                gate = jnp.dot(g_buf[rows, :], wg[slot, :, cols], preferred_element_type=jnp.float32)
                up = jnp.dot(g_buf[rows, :], wu[slot, :, cols], preferred_element_type=jnp.float32)
                m_buf[:, cols] = (gate / (1.0 + jnp.exp(-gate)) * up).astype(jnp.bfloat16)
            acc[rows, :] += jnp.dot(m_buf[...], wd[slot], preferred_element_type=jnp.float32)

            @pl.when(j == steps - 1)
            def _():
                def fin(q, _):
                    part = pl.ds(pl.multiple_of(r * rt + q * 128, 128), 128)
                    o_ref[part, :] = acc[part, :].astype(jnp.bfloat16)
                    return 0

                lax.fori_loop(0, rt // 128, fin, 0)
                pltpu.make_async_copy(o_ref.at[rows, :], out_hbm.at[rows, :], out_sems.at[r]).start()

            return 0

        lax.fori_loop(0, ROWS // rt, tile, 0)
        return 0

    lax.fori_loop(0, steps, step, 0)

    for r in range(ROWS // rt):
        rows = pl.ds(r * rt, rt)
        pltpu.make_async_copy(o_ref.at[rows, :], out_hbm.at[rows, :], out_sems.at[r]).wait()
    for i in range(2):
        pltpu.make_async_copy(c_buf.at[i], cache[i][1], c_sems.at[1, i]).wait()


def mlp_call(o, x, w_out, gain, wg, wu, wd, k_all, v_all, fb=1280, rt=512):
    vm = pl.BlockSpec(memory_space=pltpu.VMEM)
    hbm = pl.BlockSpec(memory_space=pl.ANY)
    flops = 2 * ROWS * DIM * (DIM + 3 * FFN)
    return pl.pallas_call(
        functools.partial(mlp_kernel, fb, rt),
        out_shape=(jax.ShapeDtypeStruct((ROWS, DIM), jnp.bfloat16),) + (jax.ShapeDtypeStruct(k_all.shape, jnp.bfloat16),) * 2,
        in_specs=[hbm] * 3 + [vm] + [hbm] * 5,
        out_specs=(hbm, hbm, hbm),
        scratch_shapes=[
            pltpu.VMEM((ROWS, DIM), jnp.bfloat16),
            pltpu.VMEM((ROWS, DIM), jnp.bfloat16),
            pltpu.VMEM((DIM, DIM), jnp.bfloat16),
            pltpu.VMEM((ROWS, DIM), jnp.float32),
            pltpu.VMEM((ROWS, DIM), jnp.bfloat16),
            pltpu.VMEM((rt, fb), jnp.bfloat16),
            pltpu.VMEM((2, DIM, fb), jnp.bfloat16),
            pltpu.VMEM((2, DIM, fb), jnp.bfloat16),
            pltpu.VMEM((2, fb, DIM), jnp.bfloat16),
            pltpu.VMEM((2, 4 * ROWS, 128), jnp.bfloat16),
            pltpu.SemaphoreType.DMA((2, 3)),
            pltpu.SemaphoreType.DMA((2, 2)),
            pltpu.SemaphoreType.DMA((3, 4)),
            pltpu.SemaphoreType.DMA((ROWS // rt,)),
        ],
        compiler_params=pltpu.CompilerParams(vmem_limit_bytes=60 << 20),
        cost_estimate=pl.CostEstimate(flops=flops, bytes_accessed=3 * DIM * FFN * 2, transcendentals=ROWS * FFN),
        name="mlp_block",
    )(o, x, w_out, gain, wg, wu, wd, k_all, v_all)


HEAD_DIM = 128
ROPE_THETA = 500000
SCALE_LOG2E = 1.4426950408889634 * HEAD_DIM ** -0.5
NEG = -2.0e38
QB = 512
KC = 512
PC = 64
MOVED = ((0, 2), (0, 1), (1, 2))
FOREIGN = len(MOVED)
TRI, REAL, BOTH, NONE, FREE = range(5)
MESH = pl.DeviceIdType.MESH


def schedules():
    def code(st, kb, b):
        return (st * 8 + kb) * 8 + b

    a_masked = [code(3 * tb + p, tb, BOTH if tb == 0 else TRI) for tb in range(4) for p in range(3)]
    a_masked += [code(3 * tb + p, 0, REAL) for tb in range(1, 4) for p in range(3)]
    a_plain = [code(3 * tb + p, kb, FREE) for tb in range(2, 4) for kb in range(1, tb) for p in range(3)]
    a_masked += [a_plain.pop(0), *[a_plain[-1] - FREE + NONE] * 2]
    pairs = {tb: [p for p in range(3) if (tb, p) not in MOVED] for tb in range(4)}
    b_masked = [code(3 * tb + p, 4 + tb, TRI) for tb in range(4) for p in pairs[tb]]
    b_plain = [code(3 * tb + p, 4 + kb, FREE) for tb in range(1, 4) for kb in range(tb) for p in pairs[tb]]
    b_masked += [b_plain.pop(0), *[b_plain[-1] - FREE + NONE] * 2]
    b_real = [code(3 * tb + p, 0, REAL) for tb in range(4) for p in pairs[tb]]
    b_far = [code(3 * tb + p, kb, FREE) for tb in range(4) for kb in range(1, 4) for p in pairs[tb]]
    b_real += [b_far.pop(0) for _ in range(3)]
    runs = []
    for f, (tb, _) in enumerate(MOVED):
        runs += [code(12 + f, 0, REAL)] + [code(12 + f, kb, FREE) for kb in range(1, 4 + tb)] + [code(12 + f, 4 + tb, TRI)]
    foreign = [runs[:8], runs[8:12], runs[12:]]
    for run in (a_masked, a_plain, b_masked, b_plain, b_real, b_far, *foreign):
        assert len(run) % 4 == 0
    return a_masked, a_plain, b_masked, b_plain, b_real, b_far, foreign


def packed(runs):
    words = ([], [], [], [])
    for run in runs:
        for j in range(0, len(run), 4):
            ahead = [run[min(j + k, len(run) - 1)] for k in range(6)]
            for w in range(3):
                words[w].append(ahead[2 * w] + 1024 * ahead[2 * w + 1])
            words[3].append(run[max(j - 1, 0)])
    return words


def lookup(i, values):
    if len(values) == 1:
        return values[0]
    if all(v == values[0] for v in values):
        return values[0]
    half = len(values) // 2
    return jnp.where(i < half, lookup(i, values[:half]), lookup(i - half, values[half:]))


def flash_run(groups, words_fn, biased, me_c, q_buf, kv, vt, acc, m_s, l_s, s_buf, p_buf, top_s, decay_s, bias):
    def fields(code):
        return lax.div(code, 64), lax.rem(lax.div(code, 8), 8), lax.rem(code, 8)

    def split(word):
        return [lax.rem(word, 1024), lax.div(word, 1024)]

    def scores(code, slot):
        st, kb, b = fields(code)
        tb = lax.div(st, 3)
        own = st < 12
        place = jnp.where(own, jnp.where(lax.div(tb, 2) == me_c, me_c, 2), 3)
        entry = jnp.where(own, lax.rem(tb, 2) * 3 + lax.rem(st, 3), st - 12)
        k_off = pl.multiple_of(lax.rem(kb, 2) * QB, QB)
        for u in range(2):
            q_blk = q_buf[place, entry, u]
            top = jnp.full((8, QB), NEG, jnp.float32)
            for k0 in range(0, QB, KC):
                k_blk = kv[lax.div(kb, 2), me_c, 0, pl.ds(k_off + k0, KC), :]
                s = lax.dot_general(k_blk, q_blk, (((1,), (1,)), ((), ())), preferred_element_type=jnp.float32)
                if biased:
                    s = s + bias[b, k0:k0 + KC, :]
                s_buf[slot % 4, u, k0:k0 + KC, :] = s
                top = jnp.maximum(top, jnp.max(s.reshape(KC // 8, 8, QB), axis=0))
                yield
            top_s[slot % 4, u] = top

    def weights(code, slot):
        st = fields(code)[0]
        for u in range(2):
            m_prev = m_s[st, u]
            m_new = jnp.maximum(m_prev, jnp.max(top_s[slot % 4, u], axis=0, keepdims=True))
            m8 = jnp.broadcast_to(m_new, (8, QB))
            total = jnp.zeros((8, QB), jnp.float32)
            for k0 in range(0, QB, PC):
                s = s_buf[slot % 4, u, k0:k0 + PC, :].reshape(PC // 8, 8, QB)
                p = jnp.exp2((s - m8[None]) * SCALE_LOG2E)
                total = total + jnp.sum(p, axis=0)
                p_buf[slot % 2, u, k0:k0 + PC, :] = p.reshape(PC, QB).astype(jnp.bfloat16)
                if (k0 + PC) % KC == 0:
                    yield
            decay = jnp.exp2((m_prev - m_new) * SCALE_LOG2E)
            decay_s[slot % 2, u] = decay
            l_s[st, u] = l_s[st, u] * decay + jnp.sum(total, axis=0, keepdims=True)
            m_s[st, u] = m_new

    def values(code, slot):
        st, kb, _ = fields(code)
        k_off = pl.multiple_of(lax.rem(kb, 2) * QB, QB)
        for u in range(2):
            pv = jnp.dot(vt[lax.div(kb, 2), :, pl.ds(k_off, QB)], p_buf[slot % 2, u], preferred_element_type=jnp.float32)
            acc[st, u] = acc[st, u] * decay_s[slot % 2, u] + pv
            for _ in range(QB // KC):
                yield

    def together(*parts):
        for _ in itertools.zip_longest(*parts):
            pass

    @pl.when(groups > 0)
    def _():
        p_buf[1] = jnp.zeros_like(p_buf[1])
        decay_s[1] = jnp.ones_like(decay_s[1])
        first = split(words_fn(0)[0])
        together(scores(first[0], 0))
        together(scores(first[1], 1))

        def step(j, _):
            words = words_fn(j)
            codes = [words[3]] + split(words[0]) + split(words[1]) + split(words[2])
            for k in range(4):
                together(weights(codes[k + 1], k), scores(codes[k + 3], k + 2), values(codes[k], k + 1))
            return 0

        lax.fori_loop(0, groups, step, 0)
        together(values(split(words_fn(groups - 1)[1])[1], 1))


def attn_kernel(pos_ref, freq_ref, gain_ref, x_hbm, wk_hbm, wv_hbm, wq_hbm, out_ref, kc_ref, vc_ref,
                x_ref, wk_ref, wv_ref, wq_ref, cos_s, sin_s, h_buf, q_buf, kv, vt, acc, m_s, l_s, s_buf, p_buf, top_s, decay_s, bias, o_buf,
                send_sem, recv_sem, qsend_sem, qrecv_sem, osend_sem, orecv_sem, cache_sem, ocopy_sem, wq_sem):
    me = lax.axis_index("sp")
    x = me // 2
    c = lax.rem(me, 2)
    partner = 2 * x + (1 - c)
    cross = 2 * (1 - x) + c
    diag = 2 * (1 - x) + (1 - c)
    pad = me * ROWS + (ROWS - 1) - pos_ref[ROWS - 1]
    a_masked, a_plain, b_masked, b_plain, b_real, b_far, foreign = schedules()

    def x_copy(r):
        rows = pl.ds(r * 256, 256)
        return pltpu.make_async_copy(x_hbm.at[rows, :], x_ref.at[rows, :], wq_sem.at[3 + r])

    wk_copy = pltpu.make_async_copy(wk_hbm, wk_ref, wq_sem.at[1])
    wv_copy = pltpu.make_async_copy(wv_hbm, wv_ref, wq_sem.at[2])
    wq_copy = pltpu.make_async_copy(wq_hbm, wq_ref, wq_sem.at[0])
    for cp in (wk_copy, wv_copy, *[x_copy(r) for r in range(4)], wq_copy):
        cp.start()
    barrier = pltpu.get_barrier_semaphore()
    for peer in (partner, cross, diag):
        pl.semaphore_signal(barrier, inc=1, device_id={"sp": peer}, device_id_type=MESH)

    gain = gain_ref[...].reshape(1, DIM).astype(jnp.float32)
    lane = lax.broadcasted_iota(jnp.int32, (256, 128), 1)

    def angle_rows(r):
        rows = pl.ds(r * 256, 256)
        row = lax.broadcasted_iota(jnp.int32, (256, 128), 0) + (me * ROWS + r * 256 - pad)
        ang = jnp.maximum(row, -1).astype(jnp.float32) * freq_ref[...]
        turns = jnp.floor(ang * 0.6366197723675814 + 0.5)
        red = ((ang - turns * 1.5703125) - turns * 4.837512969970703125e-4) - turns * 7.54978995489188216e-8
        sq = red * red
        sin_p = ((-1.9515295891e-4 * sq + 8.3321608736e-3) * sq - 1.6666654611e-1) * sq * red + red
        cos_p = ((2.443315711809948e-5 * sq - 1.388731625493765e-3) * sq + 4.166664568298827e-2) * sq * sq - 0.5 * sq + 1.0
        quad = (turns.astype(jnp.int32) + jnp.where(lane < 64, 0, 3)) & 3
        val = jnp.where((quad & 1) == 0, cos_p, sin_p)
        val = jnp.where((quad == 1) | (quad == 2), -val, val)
        swapped = pltpu.roll(val, 64, 1)
        cos_s[rows, :] = jnp.where(lane < 64, val, swapped)
        sin_s[rows, :] = jnp.where(lane < 64, -swapped, val)

    def rope(t, rows):
        return (t * cos_s[rows, :] + pltpu.roll(t, 64, 1) * sin_s[rows, :]).astype(jnp.bfloat16)

    for r in range(ROWS // 256):
        angle_rows(r)
    for cp in (wk_copy, wv_copy, *[x_copy(r) for r in range(4)]):
        cp.wait()
    for r in range(ROWS // 256):
        rows = pl.ds(r * 256, 256)
        xf = x_ref[rows, :].astype(jnp.float32)
        ms = jnp.mean(xf * xf, axis=-1, keepdims=True)
        h = (xf * lax.rsqrt(ms + NORM_EPS) * gain).astype(jnp.bfloat16)
        h_buf[rows, :] = h
        k = jnp.dot(h, wk_ref[...], preferred_element_type=jnp.float32)
        v = jnp.dot(h, wv_ref[...], preferred_element_type=jnp.float32).astype(jnp.bfloat16)
        for g in range(2):
            kv[me, g, 0, rows, :] = rope(k[:, g * 128:(g + 1) * 128], rows)
            kv[me, g, 1, rows, :] = v[:, g * 128:(g + 1) * 128]

    pl.semaphore_wait(barrier, 3)

    def kv_copy(src, g, i, peer):
        return pltpu.make_async_remote_copy(src_ref=kv.at[src, g], dst_ref=kv.at[src, g], send_sem=send_sem.at[i], recv_sem=recv_sem.at[i],
                                            device_id={"sp": peer}, device_id_type=MESH)

    to_cross = kv_copy(me, c, 0, cross)
    sends_cross = jnp.logical_not((x == 1) & (c == 1))
    gets_cross = jnp.logical_not((x == 0) & (c == 1))

    @pl.when(sends_cross)
    def _():
        to_cross.start()

    to_diag = kv_copy(me, 1 - c, 1, diag)
    to_diag.start()
    to_partner = [kv_copy(me, g, 2 + g, partner) for g in range(2)]
    for cp in to_partner:
        cp.start()

    def q_rows(t):
        def body(r, _):
            rows = pl.ds(pl.multiple_of(t * QB + r * 256, 256), 256)
            inner = pl.ds(pl.multiple_of(r * 256, 256), 256)
            part = t * 2 + r
            k_rows = pl.ds(pl.multiple_of(part * 128, 128), 128)
            k_idx = lax.broadcasted_iota(jnp.int32, (128, QB), 0) + part * 128
            tri = k_idx <= lax.broadcasted_iota(jnp.int32, (128, QB), 1)
            real = k_idx >= pad
            bias[TRI, k_rows, :] = jnp.where(tri, 0.0, NEG)
            bias[REAL, k_rows, :] = jnp.where(real, 0.0, NEG)
            bias[BOTH, k_rows, :] = jnp.where(tri & real, 0.0, NEG)
            bias[NONE, k_rows, :] = jnp.full((128, QB), NEG, jnp.float32)
            bias[FREE, k_rows, :] = jnp.zeros((128, QB), jnp.float32)
            acc[:, :, pl.ds(pl.multiple_of(part * 32, 32), 32), :] = jnp.zeros((12 + FOREIGN, 2, 32, QB), jnp.float32)
            q = jnp.dot(h_buf[rows, :], wq_ref[...], preferred_element_type=jnp.float32)
            for h in range(12):
                q_buf[h // 6, t * 3 + (h % 6) // 2, h % 2, inner, :] = rope(q[:, h * 128:(h + 1) * 128], rows)
            return 0

        lax.fori_loop(0, 2, body, 0)

    def foreign_q(f, g, peer):
        tb, p = MOVED[f]
        return pltpu.make_async_remote_copy(src_ref=q_buf.at[g, tb % 2 * 3 + p], dst_ref=q_buf.at[3, f], send_sem=qsend_sem.at[f, g],
                                            recv_sem=qrecv_sem.at[f], device_id={"sp": peer}, device_id_type=MESH)

    def sends_q(f):
        return (x == 1) & (c == MOVED[f][0] // 2)

    wq_copy.wait()
    def q_copy(t):
        half = pl.ds(t * 3, 3)
        return pltpu.make_async_remote_copy(src_ref=q_buf.at[1 - c, half], dst_ref=q_buf.at[2, half], send_sem=send_sem.at[6 + t], recv_sem=recv_sem.at[6 + t],
                                            device_id={"sp": partner}, device_id_type=MESH)

    for t in range(2):
        q_rows(t)
        q_copy(t).start()
    for f in range(FOREIGN):
        @pl.when(sends_q(f))
        def _():
            foreign_q(f, c, cross).start()
            foreign_q(f, 1 - c, diag).start()

    def flip(src):
        vt[src] = kv[src, c, 1].T

    def cache_copy(src, i):
        rows = pl.ds(pl.multiple_of(src * ROWS, ROWS), ROWS)
        return (pltpu.make_async_copy(kv.at[src, x, 0], kc_ref.at[rows, :], cache_sem.at[i, 0]),
                pltpu.make_async_copy(kv.at[src, x, 1], vc_ref.at[rows, :], cache_sem.at[i, 1]))

    for cp in cache_copy(me, 0):
        cp.start()
    flip(me)
    m_s[...] = jnp.full_like(m_s, NEG)
    l_s[...] = jnp.zeros_like(l_s)
    for cp in to_partner:
        cp.wait_recv()
    for cp in cache_copy(partner, 1):
        cp.start()
    flip(partner)
    for t in range(2):
        q_copy(t).wait_recv()

    def by_chip(a, b):
        return jnp.where(x == 0, a, b)

    def flash(a_groups, a_words, a_start, b_run, biased):
        b_words = packed([b_run])

        def words_fn(j):
            return [by_chip(lookup(j + a_start, a), lookup(j, b)) for a, b in zip(a_words, b_words)]

        flash_run(by_chip(a_groups, len(b_run) // 4), words_fn, biased, c, q_buf, kv, vt, acc, m_s, l_s, s_buf, p_buf, top_s, decay_s, bias)

    flash(len(a_masked) // 4, packed([a_masked]), 0, b_masked, True)
    flash(len(a_plain) // 4, packed([a_plain]), 0, b_plain, False)

    def o_place(t, col):
        return out_ref.at[pl.ds(pl.multiple_of(t * QB, QB), QB), pl.ds(pl.multiple_of(col * 256, 256), 256)]

    def o_send(st, t, col, peer):
        return pltpu.make_async_remote_copy(src_ref=o_buf.at[st], dst_ref=o_place(t, col), send_sem=osend_sem.at[st], recv_sem=orecv_sem.at[t, col],
                                            device_id={"sp": peer}, device_id_type=MESH)

    def o_keep(st, t, col):
        return pltpu.make_async_copy(o_buf.at[st], o_place(t, col), ocopy_sem.at[t, lax.rem(col, 3)])

    def finish(st):
        q_idx = lax.broadcasted_iota(jnp.int32, (1, QB), 1) + (x * 2 * ROWS + (st // 3) * QB)
        for u in range(2):
            inv = jnp.where(q_idx >= pad, 1.0 / l_s[st, u], 0.0)
            o_buf[st, :, u * 128:(u + 1) * 128] = (acc[st, u] * inv).T.astype(jnp.bfloat16)

    def here(tb, pair):
        moved = [(tb == m_tb) & (pair == m_pair) for m_tb, m_pair in MOVED]
        return (x == 0) | jnp.logical_not(functools.reduce(jnp.logical_or, moved))

    def finish_own(j, _):
        half = jnp.where(j < 6, 1 - c, c)
        t = lax.rem(j, 6) // 3
        pair = lax.rem(j, 3)
        tb = 2 * half + t
        st = 3 * tb + pair

        @pl.when(here(tb, pair))
        def _():
            finish(st)

            @pl.when(j < 6)
            def _():
                o_send(st, t, 3 * c + pair, partner).start()

            @pl.when(j >= 6)
            def _():
                o_keep(st, t, 3 * c + pair).start()

        return 0

    @pl.when(x == 0)
    def _():
        lax.fori_loop(0, 12, finish_own, 0)

    def arrived(src, i):
        kv_copy(src, c, i, cross).wait_recv()
        kv_copy(src, c, 4 + i, partner).start()
        flip(src)

    @pl.when(gets_cross)
    def _():
        arrived(cross, 0)

    arrived(diag, 1)

    f_len = [len(run) // 4 for run in foreign]
    f_start = [sum(f_len[:k]) for k in range(FOREIGN)]

    def far_round(j, _):
        for r, f in ((0, 0), (0, 1), (1, 2)):
            @pl.when((x == 0) & (j == r))
            def _():
                foreign_q(f, 0, cross).wait_recv()

        flash(lookup(j, f_len), packed(foreign), lookup(j, f_start), b_real, True)

        @pl.when(x == 0)
        def _():
            finish(12 + j)
            tb = lookup(j, [m[0] for m in MOVED])
            o_send(12 + j, lax.rem(tb, 2), 3 * c + lookup(j, [m[1] for m in MOVED]), 2 + lax.div(tb, 2)).start()

        return 0

    lax.fori_loop(0, by_chip(FOREIGN, 1), far_round, 0)
    for sem, src, i in ((4, diag, 3), (5, cross, 2)):
        def forwarded():
            kv_copy(src, 1 - c, sem, partner).wait_recv()

        if sem == 4:
            pl.when(me != 0)(forwarded)
        else:
            forwarded()
        for cp in cache_copy(src, i):
            cp.start()
    flash(0, packed([b_far]), 0, b_far, False)

    @pl.when(x == 1)
    def _():
        lax.fori_loop(0, 12, finish_own, 0)

    pl.when(sends_cross)(lambda: to_cross.wait_send())
    to_diag.wait_send()
    for cp in to_partner:
        cp.wait_send()
    pl.when(gets_cross)(lambda: kv_copy(cross, c, 4, partner).wait_send())
    kv_copy(diag, c, 5, partner).wait_send()
    for t in range(2):
        q_copy(t).wait_send()
    for i, src in enumerate((me, partner, cross, diag)):
        for cp in cache_copy(src, i):
            cp.wait()
    for f in range(FOREIGN):
        @pl.when(sends_q(f))
        def _():
            foreign_q(f, c, cross).wait_send()
            foreign_q(f, 1 - c, diag).wait_send()

    for t in range(2):
        for pair in range(3):
            mine = here(2 * c + t, pair)
            theirs = here(2 * (1 - c) + t, pair)

            @pl.when(mine)
            def _():
                o_keep(0, t, 3 * c + pair).wait()

            @pl.when(jnp.logical_not(mine))
            def _():
                o_send(0, t, 3 * c + pair, cross).wait_recv()

            o_send(0, t, 3 * (1 - c) + pair, partner).wait_recv()

            @pl.when(theirs)
            def _():
                o_send(3 * (2 * (1 - c) + t) + pair, t, 3 * c + pair, partner).wait_send()

    @pl.when(x == 0)
    def _():
        for f, (tb, p) in enumerate(MOVED):
            o_send(12 + f, tb % 2, 3 * c + p, 2 + tb // 2).wait_send()


def attn_call(positions, freq, x, gain, w_query, w_key, w_value):
    vm = pl.BlockSpec(memory_space=pltpu.VMEM)
    hbm = pl.BlockSpec(memory_space=pl.ANY)
    flops = 2 * ROWS * DIM * 2048 + 4 * 128 * 3 * 4096 * 2048
    bf, f32 = jnp.bfloat16, jnp.float32
    dma = pltpu.SemaphoreType.DMA
    return pl.pallas_call(
        attn_kernel,
        out_shape=(jax.ShapeDtypeStruct((ROWS, DIM), bf), jax.ShapeDtypeStruct((4 * ROWS, 128), bf), jax.ShapeDtypeStruct((4 * ROWS, 128), bf)),
        in_specs=[pl.BlockSpec(memory_space=pltpu.SMEM)] + [vm] * 2 + [hbm] * 4,
        out_specs=(hbm, hbm, hbm),
        scratch_shapes=[
            pltpu.VMEM((ROWS, DIM), bf),
            pltpu.VMEM((DIM, 256), bf),
            pltpu.VMEM((DIM, 256), bf),
            pltpu.VMEM((DIM, DIM), bf),
            pltpu.VMEM((ROWS, 128), f32),
            pltpu.VMEM((ROWS, 128), f32),
            pltpu.VMEM((ROWS, DIM), bf),
            pltpu.VMEM((4, 6, 2, QB, 128), bf),
            pltpu.VMEM((4, 2, 2, ROWS, 128), bf),
            pltpu.VMEM((4, 128, ROWS), bf),
            pltpu.VMEM((12 + FOREIGN, 2, 128, QB), f32),
            pltpu.VMEM((12 + FOREIGN, 2, 1, QB), f32),
            pltpu.VMEM((12 + FOREIGN, 2, 1, QB), f32),
            pltpu.VMEM((4, 2, QB, QB), f32),
            pltpu.VMEM((2, 2, QB, QB), bf),
            pltpu.VMEM((4, 2, 8, QB), f32),
            pltpu.VMEM((2, 2, 1, QB), f32),
            pltpu.VMEM((5, QB, QB), f32),
            pltpu.VMEM((12 + FOREIGN, QB, 256), bf),
            dma((8,)), dma((8,)), dma((FOREIGN, 2)), dma((FOREIGN,)), dma((12 + FOREIGN,)), dma((2, 6)), dma((4, 2)), dma((2, 3)), dma((7,)),
        ],
        compiler_params=pltpu.CompilerParams(vmem_limit_bytes=62 << 20, collective_id=0, has_side_effects=True),
        cost_estimate=pl.CostEstimate(flops=flops, bytes_accessed=20 << 20, transcendentals=3 * 4096 * 2048),
        name="attn_block",
    )(positions, freq, gain, x, w_key, w_value, w_query)


def solution(mesh):
    freq = 1.0 / (ROPE_THETA ** (np.arange(0, HEAD_DIM, 2, dtype=np.float64) / HEAD_DIM))
    freq = np.concatenate([freq, freq]).astype(np.float32).reshape(1, HEAD_DIM)

    def layer_shard(hidden, positions, attn_gain, w_query, w_key, w_value, w_out, mlp_gain, w_gate, w_up, w_down):
        attn, k_all, v_all = attn_call(positions, jnp.asarray(freq), hidden, attn_gain, w_query, w_key, w_value)
        hidden_out, k_cache, v_cache = mlp_call(attn, hidden, w_out, mlp_gain, w_gate, w_up, w_down, k_all, v_all)
        return hidden_out, k_cache.reshape(4 * ROWS, 1, HEAD_DIM), v_cache.reshape(4 * ROWS, 1, HEAD_DIM)

    row_spec = P(("dp", "sp"), None)
    cache_spec = P("dp", "sp", None)
    return jax.shard_map(layer_shard, mesh=mesh, in_specs=(row_spec, P(("dp", "sp")), P(), P(), P(), P(), P(), P(), P(), P(), P()), out_specs=(row_spec, cache_spec, cache_spec), check_vma=False)
```

```python
import functools
import itertools
import jax
import jax.numpy as jnp
import numpy as np
from jax import lax
from jax.experimental import pallas as pl
from jax.experimental.pallas import tpu as pltpu
from jax.sharding import PartitionSpec as P

ROWS = 1024
DIM = 1536
FFN = 8960
NORM_EPS = 1e-5


def mlp_kernel(fb, rt, o_hbm, x_hbm, wout_hbm, gain_ref, wg_hbm, wu_hbm, wd_hbm, k_in, v_in, out_hbm, k_out, v_out, o_ref, x_ref, wout_ref, acc, g_buf, m_buf, wg, wu, wd, c_buf, sems, c_sems, in_sems, out_sems):
    steps = FFN // fb

    def copies(j, slot):
        off = pl.multiple_of(j * fb, 128)
        return (
            pltpu.make_async_copy(wg_hbm.at[:, pl.ds(off, fb)], wg.at[slot], sems.at[slot, 0]),
            pltpu.make_async_copy(wu_hbm.at[:, pl.ds(off, fb)], wu.at[slot], sems.at[slot, 1]),
            pltpu.make_async_copy(wd_hbm.at[pl.ds(off, fb), :], wd.at[slot], sems.at[slot, 2]),
        )

    wout_copy = pltpu.make_async_copy(wout_hbm, wout_ref, in_sems.at[2, 0])
    wout_copy.start()

    def row_copies(r):
        rows = pl.ds(r * 256, 256)
        return (pltpu.make_async_copy(o_hbm.at[rows, :], o_ref.at[rows, :], in_sems.at[0, r]),
                pltpu.make_async_copy(x_hbm.at[rows, :], x_ref.at[rows, :], in_sems.at[1, r]))

    for r in range(ROWS // 256):
        for c in row_copies(r):
            c.start()
    for c in copies(0, 0):
        c.start()

    cache = ((k_in, k_out), (v_in, v_out))
    for i in range(2):
        pltpu.make_async_copy(cache[i][0], c_buf.at[i], c_sems.at[0, i]).start()
    gain = gain_ref[...].reshape(1, DIM).astype(jnp.float32)

    wout_copy.wait()

    def proj(half):
        for r in (2 * half, 2 * half + 1):
            for c in row_copies(r):
                c.wait()
        for r in range(2 * half, 2 * half + 2):
            rows = pl.ds(r * 256, 256)
            y = x_ref[rows, :].astype(jnp.float32) + jnp.dot(o_ref[rows, :], wout_ref[...], preferred_element_type=jnp.float32)
            y = y.astype(jnp.bfloat16).astype(jnp.float32)
            acc[rows, :] = y
            ms = jnp.mean(y * y, axis=-1, keepdims=True)
            g_buf[rows, :] = (y * lax.rsqrt(ms + NORM_EPS) * gain).astype(jnp.bfloat16)

    proj(0)
    proj(1)
    for i in range(2):
        pltpu.make_async_copy(cache[i][0], c_buf.at[i], c_sems.at[0, i]).wait()
        pltpu.make_async_copy(c_buf.at[i], cache[i][1], c_sems.at[1, i]).start()

    def step(j, _):
        slot = lax.rem(j, 2)
        for c in copies(j, slot):
            c.wait()

        @pl.when(j + 1 < steps)
        def _():
            for c in copies(j + 1, 1 - slot):
                c.start()

        def tile(r, _):
            rows = pl.ds(pl.multiple_of(r * rt, rt), rt)
            for c0 in range(0, fb, 256):
                cols = pl.ds(c0, 256)
                gate = jnp.dot(g_buf[rows, :], wg[slot, :, cols], preferred_element_type=jnp.float32)
                up = jnp.dot(g_buf[rows, :], wu[slot, :, cols], preferred_element_type=jnp.float32)
                m_buf[:, cols] = (gate / (1.0 + jnp.exp(-gate)) * up).astype(jnp.bfloat16)
            acc[rows, :] += jnp.dot(m_buf[...], wd[slot], preferred_element_type=jnp.float32)

            @pl.when(j == steps - 1)
            def _():
                def fin(q, _):
                    part = pl.ds(pl.multiple_of(r * rt + q * 128, 128), 128)
                    o_ref[part, :] = acc[part, :].astype(jnp.bfloat16)
                    return 0

                lax.fori_loop(0, rt // 128, fin, 0)
                pltpu.make_async_copy(o_ref.at[rows, :], out_hbm.at[rows, :], out_sems.at[r]).start()

            return 0

        lax.fori_loop(0, ROWS // rt, tile, 0)
        return 0

    lax.fori_loop(0, steps, step, 0)

    for r in range(ROWS // rt):
        rows = pl.ds(r * rt, rt)
        pltpu.make_async_copy(o_ref.at[rows, :], out_hbm.at[rows, :], out_sems.at[r]).wait()
    for i in range(2):
        pltpu.make_async_copy(c_buf.at[i], cache[i][1], c_sems.at[1, i]).wait()


def mlp_call(o, x, w_out, gain, wg, wu, wd, k_all, v_all, fb=1280, rt=512):
    vm = pl.BlockSpec(memory_space=pltpu.VMEM)
    hbm = pl.BlockSpec(memory_space=pl.ANY)
    flops = 2 * ROWS * DIM * (DIM + 3 * FFN)
    return pl.pallas_call(
        functools.partial(mlp_kernel, fb, rt),
        out_shape=(jax.ShapeDtypeStruct((ROWS, DIM), jnp.bfloat16),) + (jax.ShapeDtypeStruct(k_all.shape, jnp.bfloat16),) * 2,
        in_specs=[hbm] * 3 + [vm] + [hbm] * 5,
        out_specs=(hbm, hbm, hbm),
        scratch_shapes=[
            pltpu.VMEM((ROWS, DIM), jnp.bfloat16),
            pltpu.VMEM((ROWS, DIM), jnp.bfloat16),
            pltpu.VMEM((DIM, DIM), jnp.bfloat16),
            pltpu.VMEM((ROWS, DIM), jnp.float32),
            pltpu.VMEM((ROWS, DIM), jnp.bfloat16),
            pltpu.VMEM((rt, fb), jnp.bfloat16),
            pltpu.VMEM((2, DIM, fb), jnp.bfloat16),
            pltpu.VMEM((2, DIM, fb), jnp.bfloat16),
            pltpu.VMEM((2, fb, DIM), jnp.bfloat16),
            pltpu.VMEM((2, 4 * ROWS, 128), jnp.bfloat16),
            pltpu.SemaphoreType.DMA((2, 3)),
            pltpu.SemaphoreType.DMA((2, 2)),
            pltpu.SemaphoreType.DMA((3, 4)),
            pltpu.SemaphoreType.DMA((ROWS // rt,)),
        ],
        compiler_params=pltpu.CompilerParams(vmem_limit_bytes=60 << 20),
        cost_estimate=pl.CostEstimate(flops=flops, bytes_accessed=3 * DIM * FFN * 2, transcendentals=ROWS * FFN),
        name="mlp_block",
    )(o, x, w_out, gain, wg, wu, wd, k_all, v_all)


HEAD_DIM = 128
ROPE_THETA = 500000
SCALE_LOG2E = 1.4426950408889634 * HEAD_DIM ** -0.5
NEG = -2.0e38
QB = 512
KC = 512
PC = 64
MOVED = ((0, 2), (0, 1), (1, 2))
FOREIGN = len(MOVED)
TRI, REAL, BOTH, NONE, FREE = range(5)
MESH = pl.DeviceIdType.MESH


def schedules():
    def code(st, kb, b):
        return (st * 8 + kb) * 8 + b

    a_masked = [code(3 * tb + p, tb, BOTH if tb == 0 else TRI) for tb in range(4) for p in range(3)]
    a_masked += [code(3 * tb + p, 0, REAL) for tb in range(1, 4) for p in range(3)]
    a_plain = [code(3 * tb + p, kb, FREE) for tb in range(2, 4) for kb in range(1, tb) for p in range(3)]
    a_masked += [a_plain.pop(0), *[a_plain[-1] - FREE + NONE] * 2]
    pairs = {tb: [p for p in range(3) if (tb, p) not in MOVED] for tb in range(4)}
    b_masked = [code(3 * tb + p, 4 + tb, TRI) for tb in range(4) for p in pairs[tb]]
    b_plain = [code(3 * tb + p, 4 + kb, FREE) for tb in range(1, 4) for kb in range(tb) for p in pairs[tb]]
    b_masked += [b_plain.pop(0), *[b_plain[-1] - FREE + NONE] * 2]
    b_real = [code(3 * tb + p, 0, REAL) for tb in range(4) for p in pairs[tb]]
    b_far = [code(3 * tb + p, kb, FREE) for tb in range(4) for kb in range(1, 4) for p in pairs[tb]]
    b_real += [b_far.pop(0) for _ in range(3)]
    runs = []
    for f, (tb, _) in enumerate(MOVED):
        runs += [code(12 + f, 0, REAL)] + [code(12 + f, kb, FREE) for kb in range(1, 4 + tb)] + [code(12 + f, 4 + tb, TRI)]
    foreign = [runs[:8], runs[8:12], runs[12:]]
    for run in (a_masked, a_plain, b_masked, b_plain, b_real, b_far, *foreign):
        assert len(run) % 4 == 0
    return a_masked, a_plain, b_masked, b_plain, b_real, b_far, foreign


def packed(runs):
    words = ([], [], [], [])
    for run in runs:
        for j in range(0, len(run), 4):
            ahead = [run[min(j + k, len(run) - 1)] for k in range(6)]
            for w in range(3):
                words[w].append(ahead[2 * w] + 1024 * ahead[2 * w + 1])
            words[3].append(run[max(j - 1, 0)])
    return words


def lookup(i, values):
    if len(values) == 1:
        return values[0]
    if all(v == values[0] for v in values):
        return values[0]
    half = len(values) // 2
    return jnp.where(i < half, lookup(i, values[:half]), lookup(i - half, values[half:]))


def flash_run(groups, words_fn, biased, me_c, q_buf, kv, vt, acc, m_s, l_s, s_buf, p_buf, top_s, decay_s, bias):
    def fields(code):
        return lax.div(code, 64), lax.rem(lax.div(code, 8), 8), lax.rem(code, 8)

    def split(word):
        return [lax.rem(word, 1024), lax.div(word, 1024)]

    def scores(code, slot):
        st, kb, b = fields(code)
        tb = lax.div(st, 3)
        own = st < 12
        place = jnp.where(own, jnp.where(lax.div(tb, 2) == me_c, me_c, 2), 3)
        entry = jnp.where(own, lax.rem(tb, 2) * 3 + lax.rem(st, 3), st - 12)
        k_off = pl.multiple_of(lax.rem(kb, 2) * QB, QB)
        for u in range(2):
            q_blk = q_buf[place, entry, u]
            top = jnp.full((8, QB), NEG, jnp.float32)
            for k0 in range(0, QB, KC):
                k_blk = kv[lax.div(kb, 2), me_c, 0, pl.ds(k_off + k0, KC), :]
                s = lax.dot_general(k_blk, q_blk, (((1,), (1,)), ((), ())), preferred_element_type=jnp.float32)
                if biased:
                    s = s + bias[b, k0:k0 + KC, :]
                s_buf[slot % 4, u, k0:k0 + KC, :] = s
                top = jnp.maximum(top, jnp.max(s.reshape(KC // 8, 8, QB), axis=0))
                yield
            top_s[slot % 4, u] = top

    def weights(code, slot):
        st = fields(code)[0]
        for u in range(2):
            m_prev = m_s[st, u]
            m_new = jnp.maximum(m_prev, jnp.max(top_s[slot % 4, u], axis=0, keepdims=True))
            m8 = jnp.broadcast_to(m_new, (8, QB))
            total = jnp.zeros((8, QB), jnp.float32)
            for k0 in range(0, QB, PC):
                s = s_buf[slot % 4, u, k0:k0 + PC, :].reshape(PC // 8, 8, QB)
                p = jnp.exp2((s - m8[None]) * SCALE_LOG2E)
                total = total + jnp.sum(p, axis=0)
                p_buf[slot % 2, u, k0:k0 + PC, :] = p.reshape(PC, QB).astype(jnp.bfloat16)
                if (k0 + PC) % KC == 0:
                    yield
            decay = jnp.exp2((m_prev - m_new) * SCALE_LOG2E)
            decay_s[slot % 2, u] = decay
            l_s[st, u] = l_s[st, u] * decay + jnp.sum(total, axis=0, keepdims=True)
            m_s[st, u] = m_new

    def values(code, slot):
        st, kb, _ = fields(code)
        k_off = pl.multiple_of(lax.rem(kb, 2) * QB, QB)
        for u in range(2):
            pv = jnp.dot(vt[lax.div(kb, 2), :, pl.ds(k_off, QB)], p_buf[slot % 2, u], preferred_element_type=jnp.float32)
            acc[st, u] = acc[st, u] * decay_s[slot % 2, u] + pv
            for _ in range(QB // KC):
                yield

    def together(*parts):
        for _ in itertools.zip_longest(*parts):
            pass

    @pl.when(groups > 0)
    def _():
        p_buf[1] = jnp.zeros_like(p_buf[1])
        decay_s[1] = jnp.ones_like(decay_s[1])
        first = split(words_fn(0)[0])
        together(scores(first[0], 0))
        together(scores(first[1], 1))

        def step(j, _):
            words = words_fn(j)
            codes = [words[3]] + split(words[0]) + split(words[1]) + split(words[2])
            for k in range(4):
                together(weights(codes[k + 1], k), scores(codes[k + 3], k + 2), values(codes[k], k + 1))
            return 0

        lax.fori_loop(0, groups, step, 0)
        together(values(split(words_fn(groups - 1)[1])[1], 1))


def attn_kernel(pos_ref, freq_ref, gain_ref, x_hbm, wk_hbm, wv_hbm, wq_hbm, out_ref, kc_ref, vc_ref,
                x_ref, wk_ref, wv_ref, wq_ref, cos_s, sin_s, h_buf, q_buf, kv, vt, acc, m_s, l_s, s_buf, p_buf, top_s, decay_s, bias, o_buf,
                send_sem, recv_sem, qsend_sem, qrecv_sem, osend_sem, orecv_sem, cache_sem, ocopy_sem, wq_sem):
    me = lax.axis_index("sp")
    x = me // 2
    c = lax.rem(me, 2)
    partner = 2 * x + (1 - c)
    cross = 2 * (1 - x) + c
    diag = 2 * (1 - x) + (1 - c)
    pad = me * ROWS + (ROWS - 1) - pos_ref[ROWS - 1]
    a_masked, a_plain, b_masked, b_plain, b_real, b_far, foreign = schedules()

    def x_copy(r):
        rows = pl.ds(r * 256, 256)
        return pltpu.make_async_copy(x_hbm.at[rows, :], x_ref.at[rows, :], wq_sem.at[3 + r])

    wk_copy = pltpu.make_async_copy(wk_hbm, wk_ref, wq_sem.at[1])
    wv_copy = pltpu.make_async_copy(wv_hbm, wv_ref, wq_sem.at[2])
    wq_copy = pltpu.make_async_copy(wq_hbm, wq_ref, wq_sem.at[0])
    for cp in (wk_copy, wv_copy, *[x_copy(r) for r in range(4)], wq_copy):
        cp.start()
    barrier = pltpu.get_barrier_semaphore()
    for peer in (partner, cross, diag):
        pl.semaphore_signal(barrier, inc=1, device_id={"sp": peer}, device_id_type=MESH)

    gain = gain_ref[...].reshape(1, DIM).astype(jnp.float32)
    lane = lax.broadcasted_iota(jnp.int32, (256, 128), 1)

    def angle_rows(r):
        rows = pl.ds(r * 256, 256)
        row = lax.broadcasted_iota(jnp.int32, (256, 128), 0) + (me * ROWS + r * 256 - pad)
        ang = jnp.maximum(row, -1).astype(jnp.float32) * freq_ref[...]
        turns = jnp.floor(ang * 0.6366197723675814 + 0.5)
        red = ((ang - turns * 1.5703125) - turns * 4.837512969970703125e-4) - turns * 7.54978995489188216e-8
        sq = red * red
        sin_p = ((-1.9515295891e-4 * sq + 8.3321608736e-3) * sq - 1.6666654611e-1) * sq * red + red
        cos_p = ((2.443315711809948e-5 * sq - 1.388731625493765e-3) * sq + 4.166664568298827e-2) * sq * sq - 0.5 * sq + 1.0
        quad = (turns.astype(jnp.int32) + jnp.where(lane < 64, 0, 3)) & 3
        val = jnp.where((quad & 1) == 0, cos_p, sin_p)
        val = jnp.where((quad == 1) | (quad == 2), -val, val)
        swapped = pltpu.roll(val, 64, 1)
        cos_s[rows, :] = jnp.where(lane < 64, val, swapped)
        sin_s[rows, :] = jnp.where(lane < 64, -swapped, val)

    def rope(t, rows):
        return (t * cos_s[rows, :] + pltpu.roll(t, 64, 1) * sin_s[rows, :]).astype(jnp.bfloat16)

    for r in range(ROWS // 256):
        angle_rows(r)
    for cp in (wk_copy, wv_copy, *[x_copy(r) for r in range(4)]):
        cp.wait()
    for r in range(ROWS // 256):
        rows = pl.ds(r * 256, 256)
        xf = x_ref[rows, :].astype(jnp.float32)
        ms = jnp.mean(xf * xf, axis=-1, keepdims=True)
        h = (xf * lax.rsqrt(ms + NORM_EPS) * gain).astype(jnp.bfloat16)
        h_buf[rows, :] = h
        k = jnp.dot(h, wk_ref[...], preferred_element_type=jnp.float32)
        v = jnp.dot(h, wv_ref[...], preferred_element_type=jnp.float32).astype(jnp.bfloat16)
        for g in range(2):
            kv[me, g, 0, rows, :] = rope(k[:, g * 128:(g + 1) * 128], rows)
            kv[me, g, 1, rows, :] = v[:, g * 128:(g + 1) * 128]

    pl.semaphore_wait(barrier, 3)

    def kv_copy(src, g, i, peer):
        return pltpu.make_async_remote_copy(src_ref=kv.at[src, g], dst_ref=kv.at[src, g], send_sem=send_sem.at[i], recv_sem=recv_sem.at[i],
                                            device_id={"sp": peer}, device_id_type=MESH)

    to_cross = kv_copy(me, c, 0, cross)
    sends_cross = jnp.logical_not((x == 1) & (c == 1))
    gets_cross = jnp.logical_not((x == 0) & (c == 1))

    @pl.when(sends_cross)
    def _():
        to_cross.start()

    to_diag = kv_copy(me, 1 - c, 1, diag)
    to_diag.start()
    to_partner = [kv_copy(me, g, 2 + g, partner) for g in range(2)]
    for cp in to_partner:
        cp.start()

    def q_rows(t):
        def body(r, _):
            rows = pl.ds(pl.multiple_of(t * QB + r * 256, 256), 256)
            inner = pl.ds(pl.multiple_of(r * 256, 256), 256)
            part = t * 2 + r
            k_rows = pl.ds(pl.multiple_of(part * 128, 128), 128)
            k_idx = lax.broadcasted_iota(jnp.int32, (128, QB), 0) + part * 128
            tri = k_idx <= lax.broadcasted_iota(jnp.int32, (128, QB), 1)
            real = k_idx >= pad
            bias[TRI, k_rows, :] = jnp.where(tri, 0.0, NEG)
            bias[REAL, k_rows, :] = jnp.where(real, 0.0, NEG)
            bias[BOTH, k_rows, :] = jnp.where(tri & real, 0.0, NEG)
            bias[NONE, k_rows, :] = jnp.full((128, QB), NEG, jnp.float32)
            bias[FREE, k_rows, :] = jnp.zeros((128, QB), jnp.float32)
            acc[:, :, pl.ds(pl.multiple_of(part * 32, 32), 32), :] = jnp.zeros((12 + FOREIGN, 2, 32, QB), jnp.float32)
            q = jnp.dot(h_buf[rows, :], wq_ref[...], preferred_element_type=jnp.float32)
            for h in range(12):
                q_buf[h // 6, t * 3 + (h % 6) // 2, h % 2, inner, :] = rope(q[:, h * 128:(h + 1) * 128], rows)
            return 0

        for r in range(2):
            body(r, 0)

    def foreign_q(f, g, peer):
        tb, p = MOVED[f]
        return pltpu.make_async_remote_copy(src_ref=q_buf.at[g, tb % 2 * 3 + p], dst_ref=q_buf.at[3, f], send_sem=qsend_sem.at[f, g],
                                            recv_sem=qrecv_sem.at[f], device_id={"sp": peer}, device_id_type=MESH)

    def sends_q(f):
        return (x == 1) & (c == MOVED[f][0] // 2)

    wq_copy.wait()
    def q_copy(t):
        half = pl.ds(t * 3, 3)
        return pltpu.make_async_remote_copy(src_ref=q_buf.at[1 - c, half], dst_ref=q_buf.at[2, half], send_sem=send_sem.at[6 + t], recv_sem=recv_sem.at[6 + t],
                                            device_id={"sp": partner}, device_id_type=MESH)

    for t in range(2):
        q_rows(t)
        q_copy(t).start()
    for f in range(FOREIGN):
        @pl.when(sends_q(f))
        def _():
            foreign_q(f, c, cross).start()
            foreign_q(f, 1 - c, diag).start()

    def flip(src):
        vt[src] = kv[src, c, 1].T

    def cache_copy(src, i):
        rows = pl.ds(pl.multiple_of(src * ROWS, ROWS), ROWS)
        return (pltpu.make_async_copy(kv.at[src, x, 0], kc_ref.at[rows, :], cache_sem.at[i, 0]),
                pltpu.make_async_copy(kv.at[src, x, 1], vc_ref.at[rows, :], cache_sem.at[i, 1]))

    for cp in cache_copy(me, 0):
        cp.start()
    flip(me)
    m_s[...] = jnp.full_like(m_s, NEG)
    l_s[...] = jnp.zeros_like(l_s)
    for cp in to_partner:
        cp.wait_recv()
    for cp in cache_copy(partner, 1):
        cp.start()
    flip(partner)
    for t in range(2):
        q_copy(t).wait_recv()

    def by_chip(a, b):
        return jnp.where(x == 0, a, b)

    def flash(a_groups, a_words, a_start, b_run, biased):
        b_words = packed([b_run])

        def words_fn(j):
            return [by_chip(lookup(j + a_start, a), lookup(j, b)) for a, b in zip(a_words, b_words)]

        flash_run(by_chip(a_groups, len(b_run) // 4), words_fn, biased, c, q_buf, kv, vt, acc, m_s, l_s, s_buf, p_buf, top_s, decay_s, bias)

    flash(len(a_masked) // 4, packed([a_masked]), 0, b_masked, True)
    flash(len(a_plain) // 4, packed([a_plain]), 0, b_plain, False)

    def o_place(t, col):
        return out_ref.at[pl.ds(pl.multiple_of(t * QB, QB), QB), pl.ds(pl.multiple_of(col * 256, 256), 256)]

    def o_send(st, t, col, peer):
        return pltpu.make_async_remote_copy(src_ref=o_buf.at[st], dst_ref=o_place(t, col), send_sem=osend_sem.at[st], recv_sem=orecv_sem.at[t, col],
                                            device_id={"sp": peer}, device_id_type=MESH)

    def o_keep(st, t, col):
        return pltpu.make_async_copy(o_buf.at[st], o_place(t, col), ocopy_sem.at[t, lax.rem(col, 3)])

    def finish(st):
        q_idx = lax.broadcasted_iota(jnp.int32, (1, QB), 1) + (x * 2 * ROWS + (st // 3) * QB)
        for u in range(2):
            inv = jnp.where(q_idx >= pad, 1.0 / l_s[st, u], 0.0)
            o_buf[st, :, u * 128:(u + 1) * 128] = (acc[st, u] * inv).T.astype(jnp.bfloat16)

    def here(tb, pair):
        moved = [(tb == m_tb) & (pair == m_pair) for m_tb, m_pair in MOVED]
        return (x == 0) | jnp.logical_not(functools.reduce(jnp.logical_or, moved))

    def finish_own(j, _):
        half = jnp.where(j < 6, 1 - c, c)
        t = lax.rem(j, 6) // 3
        pair = lax.rem(j, 3)
        tb = 2 * half + t
        st = 3 * tb + pair

        @pl.when(here(tb, pair))
        def _():
            finish(st)

            @pl.when(j < 6)
            def _():
                o_send(st, t, 3 * c + pair, partner).start()

            @pl.when(j >= 6)
            def _():
                o_keep(st, t, 3 * c + pair).start()

        return 0

    @pl.when(x == 0)
    def _():
        lax.fori_loop(0, 12, finish_own, 0)

    def arrived(src, i):
        kv_copy(src, c, i, cross).wait_recv()
        kv_copy(src, c, 4 + i, partner).start()
        flip(src)

    @pl.when(gets_cross)
    def _():
        arrived(cross, 0)

    arrived(diag, 1)

    f_len = [len(run) // 4 for run in foreign]
    f_start = [sum(f_len[:k]) for k in range(FOREIGN)]

    def far_round(j, _):
        for r, f in ((0, 0), (0, 1), (1, 2)):
            @pl.when((x == 0) & (j == r))
            def _():
                foreign_q(f, 0, cross).wait_recv()

        flash(lookup(j, f_len), packed(foreign), lookup(j, f_start), b_real, True)

        @pl.when(x == 0)
        def _():
            finish(12 + j)
            tb = lookup(j, [m[0] for m in MOVED])
            o_send(12 + j, lax.rem(tb, 2), 3 * c + lookup(j, [m[1] for m in MOVED]), 2 + lax.div(tb, 2)).start()

        return 0

    lax.fori_loop(0, by_chip(FOREIGN, 1), far_round, 0)
    for sem, src, i in ((4, diag, 3), (5, cross, 2)):
        def forwarded():
            kv_copy(src, 1 - c, sem, partner).wait_recv()

        if sem == 4:
            pl.when(me != 0)(forwarded)
        else:
            forwarded()
        for cp in cache_copy(src, i):
            cp.start()
    flash(0, packed([b_far]), 0, b_far, False)

    @pl.when(x == 1)
    def _():
        lax.fori_loop(0, 12, finish_own, 0)

    pl.when(sends_cross)(lambda: to_cross.wait_send())
    to_diag.wait_send()
    for cp in to_partner:
        cp.wait_send()
    pl.when(gets_cross)(lambda: kv_copy(cross, c, 4, partner).wait_send())
    kv_copy(diag, c, 5, partner).wait_send()
    for t in range(2):
        q_copy(t).wait_send()
    for i, src in enumerate((me, partner, cross, diag)):
        for cp in cache_copy(src, i):
            cp.wait()
    for f in range(FOREIGN):
        @pl.when(sends_q(f))
        def _():
            foreign_q(f, c, cross).wait_send()
            foreign_q(f, 1 - c, diag).wait_send()

    for t in range(2):
        for pair in range(3):
            mine = here(2 * c + t, pair)
            theirs = here(2 * (1 - c) + t, pair)

            @pl.when(mine)
            def _():
                o_keep(0, t, 3 * c + pair).wait()

            @pl.when(jnp.logical_not(mine))
            def _():
                o_send(0, t, 3 * c + pair, cross).wait_recv()

            o_send(0, t, 3 * (1 - c) + pair, partner).wait_recv()

            @pl.when(theirs)
            def _():
                o_send(3 * (2 * (1 - c) + t) + pair, t, 3 * c + pair, partner).wait_send()

    @pl.when(x == 0)
    def _():
        for f, (tb, p) in enumerate(MOVED):
            o_send(12 + f, tb % 2, 3 * c + p, 2 + tb // 2).wait_send()


def attn_call(positions, freq, x, gain, w_query, w_key, w_value):
    vm = pl.BlockSpec(memory_space=pltpu.VMEM)
    hbm = pl.BlockSpec(memory_space=pl.ANY)
    flops = 2 * ROWS * DIM * 2048 + 4 * 128 * 3 * 4096 * 2048
    bf, f32 = jnp.bfloat16, jnp.float32
    dma = pltpu.SemaphoreType.DMA
    return pl.pallas_call(
        attn_kernel,
        out_shape=(jax.ShapeDtypeStruct((ROWS, DIM), bf), jax.ShapeDtypeStruct((4 * ROWS, 128), bf), jax.ShapeDtypeStruct((4 * ROWS, 128), bf)),
        in_specs=[pl.BlockSpec(memory_space=pltpu.SMEM)] + [vm] * 2 + [hbm] * 4,
        out_specs=(hbm, hbm, hbm),
        scratch_shapes=[
            pltpu.VMEM((ROWS, DIM), bf),
            pltpu.VMEM((DIM, 256), bf),
            pltpu.VMEM((DIM, 256), bf),
            pltpu.VMEM((DIM, DIM), bf),
            pltpu.VMEM((ROWS, 128), f32),
            pltpu.VMEM((ROWS, 128), f32),
            pltpu.VMEM((ROWS, DIM), bf),
            pltpu.VMEM((4, 6, 2, QB, 128), bf),
            pltpu.VMEM((4, 2, 2, ROWS, 128), bf),
            pltpu.VMEM((4, 128, ROWS), bf),
            pltpu.VMEM((12 + FOREIGN, 2, 128, QB), f32),
            pltpu.VMEM((12 + FOREIGN, 2, 1, QB), f32),
            pltpu.VMEM((12 + FOREIGN, 2, 1, QB), f32),
            pltpu.VMEM((4, 2, QB, QB), f32),
            pltpu.VMEM((2, 2, QB, QB), bf),
            pltpu.VMEM((4, 2, 8, QB), f32),
            pltpu.VMEM((2, 2, 1, QB), f32),
            pltpu.VMEM((5, QB, QB), f32),
            pltpu.VMEM((12 + FOREIGN, QB, 256), bf),
            dma((8,)), dma((8,)), dma((FOREIGN, 2)), dma((FOREIGN,)), dma((12 + FOREIGN,)), dma((2, 6)), dma((4, 2)), dma((2, 3)), dma((7,)),
        ],
        compiler_params=pltpu.CompilerParams(vmem_limit_bytes=62 << 20, collective_id=0, has_side_effects=True),
        cost_estimate=pl.CostEstimate(flops=flops, bytes_accessed=20 << 20, transcendentals=3 * 4096 * 2048),
        name="attn_block",
    )(positions, freq, gain, x, w_key, w_value, w_query)


def solution(mesh):
    freq = 1.0 / (ROPE_THETA ** (np.arange(0, HEAD_DIM, 2, dtype=np.float64) / HEAD_DIM))
    freq = np.concatenate([freq, freq]).astype(np.float32).reshape(1, HEAD_DIM)

    def layer_shard(hidden, positions, attn_gain, w_query, w_key, w_value, w_out, mlp_gain, w_gate, w_up, w_down):
        attn, k_all, v_all = attn_call(positions, jnp.asarray(freq), hidden, attn_gain, w_query, w_key, w_value)
        hidden_out, k_cache, v_cache = mlp_call(attn, hidden, w_out, mlp_gain, w_gate, w_up, w_down, k_all, v_all)
        return hidden_out, k_cache.reshape(4 * ROWS, 1, HEAD_DIM), v_cache.reshape(4 * ROWS, 1, HEAD_DIM)

    row_spec = P(("dp", "sp"), None)
    cache_spec = P("dp", "sp", None)
    return jax.shard_map(layer_shard, mesh=mesh, in_specs=(row_spec, P(("dp", "sp")), P(), P(), P(), P(), P(), P(), P(), P(), P()), out_specs=(row_spec, cache_spec, cache_spec), check_vma=False)
```
